8 devices in a mesh: dp: 8 (over z, y, x, core).
Axes of the slice: x: 2, y: 2, z: 1, core: 2. Of those that a mesh axis runs over, the one named last changes fastest.
Arguments:
- grad_rows: bfloat16 [8, 25530368], P('dp')
- master: float32 [25530368], P('dp')
- mom_first: float32 [25530368], P('dp')
- mom_second: float32 [25530368], P('dp')
- decay_mask: int32 [25530368], P('dp')
- learn_rate: float32 [1], replicated
Outputs:
- output 1: bfloat16 [25530368], replicated
- output 2: float32 [25530368], P('dp')
- output 3: float32 [25530368], P('dp')
- output 4: float32 [25530368], P('dp')
- output 5: float32 [1], replicated
All inputs are finite; a program needn't handle non-finite values.
Results may differ from the reference program's by a relative error of at most 0.001.
Values are sent between devices in bfloat16 or wider.
A program may use at most 1 GiB of HBM per device.

```python
import jax
import jax.numpy as jnp
from jax import lax

NUM_DEV = 8
MODEL_WIDTH = 1024
MLP_HIDDEN = 2752
VOCAB_ROWS = 12576
PADDED = 25530368
ADAM_STEP = 10

BETA_FIRST = 0.9
BETA_SECOND = 0.95
ADAM_EPS = 1e-8
CLIP_EPS = 1e-6
WEIGHT_DECAY = 0.1


def decay_layout(mask_key):
    seg_lens = [VOCAB_ROWS * MODEL_WIDTH, MODEL_WIDTH * MODEL_WIDTH, MODEL_WIDTH * MODEL_WIDTH, MODEL_WIDTH * MODEL_WIDTH, MODEL_WIDTH * MODEL_WIDTH, MODEL_WIDTH * MLP_HIDDEN, MODEL_WIDTH * MLP_HIDDEN, MLP_HIDDEN * MODEL_WIDTH, MODEL_WIDTH, MODEL_WIDTH, MODEL_WIDTH, MODEL_WIDTH]
    seg_flags = [0, 1, 1, 1, 1, 1, 1, 1, 0, 0, 0, 0]
    tensor_order = jax.random.permutation(mask_key, len(seg_lens))
    lens_perm = jnp.array(seg_lens, dtype=jnp.int32)[tensor_order]
    flags_perm = jnp.concatenate([jnp.array(seg_flags, dtype=jnp.int32)[tensor_order], jnp.zeros((1,), jnp.int32)])
    seg_ends = jnp.cumsum(lens_perm)
    seg_pos = jnp.searchsorted(seg_ends, jnp.arange(PADDED, dtype=jnp.int32), side='right')
    return flags_perm[seg_pos]


def setup_inputs(seed: int = 0) -> dict:
    key_list = jax.random.split(jax.random.key(seed), 8)
    dev_scale = 2.0 ** jax.random.uniform(key_list[0], (NUM_DEV,), jnp.float32, -1.5, 1.5)
    norm_aim = jax.random.uniform(key_list[1], (), jnp.float32, 3.0, 8.0)
    grad_scale = norm_aim * NUM_DEV / jnp.sqrt(jnp.sum(dev_scale * dev_scale) * PADDED)
    row_keys = jax.random.split(key_list[2], NUM_DEV)

    def draw_row(row_args):
        row_key, row_scale = row_args
        row_vals = jax.random.normal(row_key, (PADDED,), jnp.float32) * (grad_scale * row_scale)
        return row_vals.astype(jnp.bfloat16)

    grad_rows = lax.map(draw_row, (row_keys, dev_scale))
    unit_scale = PADDED ** -0.5
    master = jax.random.normal(key_list[3], (PADDED,), jnp.float32)
    mom_first = 0.15 * unit_scale * jax.random.normal(key_list[4], (PADDED,), jnp.float32)
    mom_second = 0.05 * unit_scale * unit_scale * (0.5 + jax.random.uniform(key_list[5], (PADDED,), jnp.float32))
    decay_mask = decay_layout(key_list[6])
    learn_rate = jax.random.uniform(key_list[7], (1,), jnp.float32, 0.5, 1.0)
    return {'grad_rows': grad_rows, 'master': master, 'mom_first': mom_first, 'mom_second': mom_second, 'decay_mask': decay_mask, 'learn_rate': learn_rate}


def reference(grad_rows, master, mom_first, mom_second, decay_mask, learn_rate):
    grad_mean = jnp.sum(grad_rows, axis=0, dtype=jnp.float32) / NUM_DEV
    grad_norm = jnp.sqrt(jnp.sum(grad_mean * grad_mean))
    clip_coef = jnp.minimum(1.0, 1.0 / (grad_norm + CLIP_EPS))
    clipped = grad_mean * clip_coef
    new_first = BETA_FIRST * mom_first + (1.0 - BETA_FIRST) * clipped
    new_second = BETA_SECOND * mom_second + (1.0 - BETA_SECOND) * clipped * clipped
    step_dir = (new_first / (1.0 - BETA_FIRST ** ADAM_STEP)) / (jnp.sqrt(new_second / (1.0 - BETA_SECOND ** ADAM_STEP)) + ADAM_EPS)
    decay_flag = decay_mask.astype(jnp.float32)
    new_master = master - learn_rate[0] * (step_dir + WEIGHT_DECAY * decay_flag * master)
    params = new_master.astype(jnp.bfloat16)
    return params, new_master, new_first, new_second, grad_norm.reshape(1)
```

```python
import functools

import jax
import jax.numpy as jnp
from jax import lax
from jax.experimental import pallas as pl
from jax.experimental.pallas import tpu as pltpu
from jax.sharding import PartitionSpec as P

BETA_FIRST = 0.9
BETA_SECOND = 0.95
ADAM_EPS = 1e-8
CLIP_EPS = 1e-6
WEIGHT_DECAY = 0.1
ADAM_STEP = 10

MESH = pl.DeviceIdType.MESH
LANES = 128
CHUNK_ROWS = 784
HALF_ROWS = CHUNK_ROWS // 2
SLOTS = 4
GATHER_CHUNKS = 23
ADAM_ROWS = 512


def places():
    me = lax.axis_index("dp")
    core = me % 2
    part = me + 1 - 2 * core
    along_x = me + 2 - 4 * ((me // 2) % 2)
    along_y = me + 4 - 8 * (me // 4)
    return me, part, along_x, along_y


def meet(peers):
    barrier = pltpu.get_barrier_semaphore()
    for peer in peers:
        pl.semaphore_signal(barrier, inc=1, device_id=(peer,), device_id_type=MESH)
    pl.semaphore_wait(barrier, len(peers))


def remote(src, dst, send_sem, recv_sem, device):
    return pltpu.make_async_remote_copy(
        src_ref=src, dst_ref=dst, send_sem=send_sem, recv_sem=recv_sem,
        device_id=(device,), device_id_type=MESH)


def reduce_kernel(shard_rows, grad, g_out, norm_out,
                  own, other, x_send, y_send, x_keep, y_keep, mine, x_recv, y_recv,
                  x_fin, y_fin, x_last, y_last, g_buf, acc, norm_send, norm_recv,
                  own_sem, part_ssem, part_rsem, x_ssem, x_rsem, y_ssem, y_rsem,
                  xf_ssem, xf_rsem, yf_ssem, yf_rsem, g_sem, n_ssem, n_rsem):
    me, part, along_x, along_y = places()
    diag = along_x + along_y - me
    shift = part - me
    blocks = (me, along_x, along_y, diag)
    shard_len = shard_rows * LANES
    full = CHUNK_ROWS * LANES
    chunks = -(-shard_rows // CHUNK_ROWS)
    tail_rows = shard_rows - (chunks - 1) * CHUNK_ROWS
    tail = tail_rows * LANES

    meet((part, along_x, along_y))
    acc[...] = jnp.zeros_like(acc)

    def loads(i, size):
        slot = i % SLOTS
        out = []
        for b, block in enumerate(blocks):
            src = pl.multiple_of(block * shard_len + i * full, LANES)
            out.append(pltpu.make_async_copy(
                grad.at[:, pl.ds(src, size)], own.at[slot, b, :, pl.ds(0, size)], own_sem.at[slot, b]))
        return out

    def swaps(i, size):
        slot = i % SLOTS
        out = []
        for b, block in enumerate(blocks):
            src = pl.multiple_of((block + shift) * shard_len + i * full, LANES)
            out.append(remote(
                grad.at[:, pl.ds(src, size)], other.at[slot, b, :, pl.ds(0, size)],
                part_ssem.at[slot, b], part_rsem.at[slot, b], part))
        return out

    def first_hops(j):
        slot = j % SLOTS
        return (remote(x_send.at[slot], x_recv.at[slot], x_ssem.at[slot], x_rsem.at[slot], along_x),
                remote(y_send.at[slot], y_recv.at[slot], y_ssem.at[slot], y_rsem.at[slot], along_y))

    def last_hops(j):
        slot = j % SLOTS
        return (remote(x_fin.at[slot], x_last.at[slot], xf_ssem.at[slot], xf_rsem.at[slot], along_x),
                remote(y_fin.at[slot], y_last.at[slot], yf_ssem.at[slot], yf_rsem.at[slot], along_y))

    def store_g(j):
        slot = j % 2
        row = pl.multiple_of(j * CHUNK_ROWS, 8)
        return pltpu.make_async_copy(g_buf.at[slot], g_out.at[pl.ds(row, CHUNK_ROWS)], g_sem.at[slot])

    def for_size(i, do):
        @pl.when(i < chunks - 1)
        def _():
            do(full)

        @pl.when(i == chunks - 1)
        def _():
            do(tail)

    def begin(i):
        def do(size):
            for cp in loads(i, size) + swaps(i, size):
                cp.start()
        for_size(i, do)

    def pair_sums(j):
        def do(size):
            for cp in loads(j, size) + swaps(j, size):
                cp.wait()
        for_size(j, do)
        slot = j % SLOTS

        def tile(t, carry):
            for half in range(2):
                row = pl.multiple_of(t * 8, 8)
                col = pl.multiple_of((t + half * (HALF_ROWS // 8)) * 8 * LANES, 8 * LANES)

                def pair(b):
                    a = own[slot, b, :, pl.ds(col, 8 * LANES)].astype(jnp.float32)
                    o = other[slot, b, :, pl.ds(col, 8 * LANES)].astype(jnp.float32)
                    return (a + o).reshape(8, LANES)

                mine[slot, half, pl.ds(row, 8)] = pair(0)
                if half == 0:
                    x_send[slot, 0, pl.ds(row, 8)] = pair(1)
                    y_keep[slot, pl.ds(row, 8)] = pair(2)
                    x_send[slot, 1, pl.ds(row, 8)] = pair(3)
                else:
                    x_keep[slot, pl.ds(row, 8)] = pair(1)
                    y_send[slot, 0, pl.ds(row, 8)] = pair(2)
                    y_send[slot, 1, pl.ds(row, 8)] = pair(3)
            return carry

        lax.fori_loop(0, HALF_ROWS // 8, tile, 0)
        for cp in first_hops(j):
            cp.start()

    def relay(j):
        for cp in first_hops(j):
            cp.wait()
        slot = j % SLOTS
        x_fin[slot] = x_keep[slot] + y_recv[slot, 1]
        y_fin[slot] = y_keep[slot] + x_recv[slot, 1]
        for cp in last_hops(j):
            cp.start()
        mine[slot, 0] = mine[slot, 0] + x_recv[slot, 0]
        mine[slot, 1] = mine[slot, 1] + y_recv[slot, 0]

    def finish(j):
        for cp in last_hops(j):
            cp.wait()
        slot = j % SLOTS
        out = j % 2

        @pl.when(j >= 2)
        def _():
            store_g(j - 2).wait()

        left = shard_rows - j * CHUNK_ROWS
        rows = lax.broadcasted_iota(jnp.int32, (8, LANES), 0)

        def tile(t, total):
            row = pl.multiple_of(t * 8, 8)
            top = (mine[slot, 0, pl.ds(row, 8)] + y_last[slot, pl.ds(row, 8)]) * 0.125
            low = (mine[slot, 1, pl.ds(row, 8)] + x_last[slot, pl.ds(row, 8)]) * 0.125
            g_buf[out, pl.ds(row, 8)] = top
            g_buf[out, pl.ds(pl.multiple_of(HALF_ROWS + t * 8, 8), 8)] = low
            total = total + jnp.where(rows + t * 8 < left, top * top, 0.0)
            return total + jnp.where(rows + (HALF_ROWS + t * 8) < left, low * low, 0.0)

        acc[...] += lax.fori_loop(0, HALF_ROWS // 8, tile, jnp.zeros((8, LANES), jnp.float32))
        store_g(j).start()

    def step(i, carry):
        @pl.when(i < chunks)
        def _():
            begin(i)

        @pl.when((i >= 1) & (i < chunks + 1))
        def _():
            pair_sums(i - 1)

        @pl.when((i >= 2) & (i < chunks + 2))
        def _():
            relay(i - 2)

        @pl.when(i >= 3)
        def _():
            finish(i - 3)

        return carry

    lax.fori_loop(0, chunks + 3, step, 0)
    for k, peer in enumerate((part, along_x, along_y)):
        norm_send[k] = acc[...]
        cp = remote(norm_send.at[k], norm_recv.at[k], n_ssem.at[k], n_rsem.at[k], peer)
        cp.start()
        cp.wait()
        acc[...] = acc[...] + norm_recv[k]
    norm_out[...] = jnp.broadcast_to(jnp.sqrt(jnp.sum(acc[...], keepdims=True)), norm_out.shape)
    store_g(chunks - 2).wait()
    store_g(chunks - 1).wait()


def reduce_scatter(grad_row, shard_rows):
    f32, bf16 = jnp.float32, jnp.bfloat16
    chunks = -(-shard_rows // CHUNK_ROWS)
    vm, dma = pltpu.VMEM, pltpu.SemaphoreType.DMA
    pair = (SLOTS, 2, HALF_ROWS, LANES)
    one = (SLOTS, HALF_ROWS, LANES)
    raw = (SLOTS, 4, 1, CHUNK_ROWS * LANES)
    return pl.pallas_call(
        functools.partial(reduce_kernel, shard_rows),
        out_shape=(jax.ShapeDtypeStruct((chunks * CHUNK_ROWS, LANES), f32),
                   jax.ShapeDtypeStruct((8, LANES), f32)),
        in_specs=[pl.BlockSpec(memory_space=pl.ANY)],
        out_specs=(pl.BlockSpec(memory_space=pl.ANY), pl.BlockSpec(memory_space=pltpu.VMEM)),
        scratch_shapes=[
            vm(raw, bf16), vm(raw, bf16), vm(pair, f32), vm(pair, f32), vm(one, f32), vm(one, f32),
            vm(pair, f32), vm(pair, f32), vm(pair, f32), vm(one, f32), vm(one, f32), vm(one, f32),
            vm(one, f32), vm((2, CHUNK_ROWS, LANES), f32), vm((8, LANES), f32), vm((3, 8, LANES), f32),
            vm((3, 8, LANES), f32),
            dma((SLOTS, 4)), dma((SLOTS, 4)), dma((SLOTS, 4)),
            dma((SLOTS,)), dma((SLOTS,)), dma((SLOTS,)), dma((SLOTS,)),
            dma((SLOTS,)), dma((SLOTS,)), dma((SLOTS,)), dma((SLOTS,)),
            dma((2,)), dma((3,)), dma((3,))],
        compiler_params=pltpu.CompilerParams(collective_id=0, has_side_effects=True,
                                             vmem_limit_bytes=48 << 20),
    )(grad_row)


def adamw_kernel(lr, norm, g, w, m, v, mask, w_out, m_out, v_out, packed):
    coef = jnp.minimum(1.0, 1.0 / (norm[...] + CLIP_EPS))[0:1]
    h = g[...] * coef
    first = BETA_FIRST * m[...] + (1.0 - BETA_FIRST) * h
    second = BETA_SECOND * v[...] + (1.0 - BETA_SECOND) * h * h
    step_dir = (first / (1.0 - BETA_FIRST ** ADAM_STEP)) / (
        jnp.sqrt(second / (1.0 - BETA_SECOND ** ADAM_STEP)) + ADAM_EPS)
    old = w[...]
    new = old - lr[0] * (step_dir + WEIGHT_DECAY * mask[...].astype(jnp.float32) * old)
    w_out[...] = new
    m_out[...] = first
    v_out[...] = second
    packed[...] = new.reshape(packed.shape).astype(packed.dtype)


def adamw(lr, norm, g, w, m, v, mask):
    rows = w.shape[0]
    block = pl.BlockSpec((ADAM_ROWS, LANES), lambda i: (i, 0))
    state = jax.ShapeDtypeStruct((rows, LANES), jnp.float32)
    return pl.pallas_call(
        adamw_kernel,
        grid=(-(-rows // ADAM_ROWS),),
        out_shape=(state, state, state, jax.ShapeDtypeStruct((rows // 4, 4, LANES), jnp.bfloat16)),
        in_specs=[pl.BlockSpec(memory_space=pltpu.SMEM),
                  pl.BlockSpec((8, LANES), lambda i: (0, 0)),
                  block, block, block, block, block],
        out_specs=(block, block, block, pl.BlockSpec((ADAM_ROWS // 4, 4, LANES), lambda i: (i, 0, 0))),
    )(lr, norm, g, w, m, v, mask)


def gather_kernel(new, whole, own, load_sem, keep_sem, x_ssem, y_ssem, xr_ssem, yr_ssem, part_ssem,
                  x_rsem, y_rsem, d_rsem, part_rsem):
    me, part, along_x, along_y = places()
    diag = along_x + along_y - me
    grains = own.shape[0]
    size = grains // GATHER_CHUNKS

    def at(block, q):
        return whole.at[pl.ds(block * grains + q * size, size)]

    def block_at(block):
        return whole.at[pl.ds(block * grains, grains)]

    def to_part(src, block, q, k):
        return remote(src, at(block, q), part_ssem.at[k], part_rsem.at[k], part)

    load = pltpu.make_async_copy(new, own, load_sem)
    load.start()
    meet((part, along_x, along_y))
    load.wait()
    keep = pltpu.make_async_copy(own, block_at(me), keep_sem)
    keep.start()

    def mine(q):
        src = own.at[pl.ds(q * size, size)]
        return (remote(src, at(me, q), x_ssem, x_rsem.at[q], along_x),
                remote(src, at(me, q), y_ssem, y_rsem.at[q], along_y),
                to_part(src, me, q, 0))

    def send(q, carry):
        for cp in mine(q):
            cp.start()
        return carry

    lax.fori_loop(0, GATHER_CHUNKS, send, 0)

    def pass_on(q, carry):
        got = at(along_x, q)
        remote(got, got, x_ssem, x_rsem.at[q], along_x).wait_recv()
        to_part(got, along_x, q, 1).start()

        @pl.when(q % 2 == 0)
        def _():
            remote(got, got, yr_ssem, d_rsem.at[q], along_y).start()

        got = at(along_y, q)
        remote(got, got, y_ssem, y_rsem.at[q], along_y).wait_recv()
        to_part(got, along_y, q, 2).start()

        @pl.when(q % 2 == 1)
        def _():
            remote(got, got, xr_ssem, d_rsem.at[q], along_x).start()

        return carry

    lax.fori_loop(0, GATHER_CHUNKS, pass_on, 0)

    def last(q, carry):
        got = at(diag, q)
        remote(got, got, xr_ssem, d_rsem.at[q], along_x).wait_recv()
        to_part(got, diag, q, 3).start()
        return carry

    lax.fori_loop(0, GATHER_CHUNKS, last, 0)

    evens = size * ((GATHER_CHUNKS + 1) // 2)
    odds = size * (GATHER_CHUNKS // 2)
    remote(own, block_at(me), x_ssem, x_rsem.at[0], along_x).wait_send()
    remote(own, block_at(me), y_ssem, y_rsem.at[0], along_y).wait_send()
    some = whole.at[pl.ds(0, evens)]
    remote(some, some, yr_ssem, d_rsem.at[0], along_y).wait_send()
    some = whole.at[pl.ds(0, odds)]
    remote(some, some, xr_ssem, d_rsem.at[0], along_x).wait_send()
    shift = part - me
    for k, block in enumerate((me, along_x, along_y, diag)):
        cp = remote(block_at(block), block_at(block + shift), part_ssem.at[k], part_rsem.at[k], part)
        cp.wait_send()
        cp.wait_recv()
    keep.wait()


def all_gather(new, num_dev):
    grains = new.shape[0]
    vm, dma = pltpu.VMEM, pltpu.SemaphoreType.DMA
    return pl.pallas_call(
        gather_kernel,
        out_shape=jax.ShapeDtypeStruct((num_dev * grains, 4, LANES), jnp.bfloat16),
        in_specs=[pl.BlockSpec(memory_space=pl.ANY)],
        out_specs=pl.BlockSpec(memory_space=pl.ANY),
        scratch_shapes=[vm((grains, 4, LANES), jnp.bfloat16), dma, dma, dma, dma, dma, dma, dma((4,)),
                        dma((GATHER_CHUNKS,)), dma((GATHER_CHUNKS,)), dma((GATHER_CHUNKS,)), dma((4,))],
        compiler_params=pltpu.CompilerParams(collective_id=1, has_side_effects=True),
    )(new)


def solution(mesh):
    num_dev = mesh.shape["dp"]

    def local_step(grad_row, master, mom_first, mom_second, decay_mask, learn_rate):
        shard_len = master.shape[0]
        rows = shard_len // LANES
        flat = lambda a: a.reshape(rows, LANES)
        g, norm = reduce_scatter(grad_row, rows)
        new_w, new_m, new_v, packed = adamw(
            learn_rate, norm, g, flat(master), flat(mom_first), flat(mom_second), flat(decay_mask))
        params = all_gather(packed, num_dev).reshape(num_dev * shard_len)
        return (params, new_w.reshape(shard_len), new_m.reshape(shard_len), new_v.reshape(shard_len),
                norm[0, 0:1])

    return jax.shard_map(
        local_step, mesh=mesh,
        in_specs=(P("dp", None), P("dp"), P("dp"), P("dp"), P("dp"), P()),
        out_specs=(P(), P("dp"), P("dp"), P("dp"), P()), check_vma=False)
```

```python
import functools

import jax
import jax.numpy as jnp
from jax import lax
from jax.experimental import pallas as pl
from jax.experimental.pallas import tpu as pltpu
from jax.sharding import PartitionSpec as P

BETA_FIRST = 0.9
BETA_SECOND = 0.95
ADAM_EPS = 1e-8
CLIP_EPS = 1e-6
WEIGHT_DECAY = 0.1
ADAM_STEP = 10

MESH = pl.DeviceIdType.MESH
LANES = 128
CHUNK_ROWS = 384
HALF_ROWS = CHUNK_ROWS // 2
SLOTS = 4
VMEM_LIMIT = 20 << 20
GATHER_CHUNKS = 23
ADAM_ROWS = 5 * CHUNK_ROWS


def places():
    me = lax.axis_index("dp")
    core = me % 2
    part = me + 1 - 2 * core
    along_x = me + 2 - 4 * ((me // 2) % 2)
    along_y = me + 4 - 8 * (me // 4)
    return me, part, along_x, along_y


def meet(peers):
    barrier = pltpu.get_barrier_semaphore()
    for peer in peers:
        pl.semaphore_signal(barrier, inc=1, device_id=(peer,), device_id_type=MESH)
    pl.semaphore_wait(barrier, len(peers))


def stay(array):
    return pltpu.with_memory_space_constraint(array, pltpu.VMEM)


def remote(src, dst, send_sem, recv_sem, device):
    return pltpu.make_async_remote_copy(
        src_ref=src, dst_ref=dst, send_sem=send_sem, recv_sem=recv_sem,
        device_id=(device,), device_id_type=MESH)


def reduce_kernel(shard_rows, grad, w, m, g_out, w_out, m_out, norm_out,
                  own, other, x_send, y_send, x_keep, y_keep, mine, x_recv, y_recv,
                  x_fin, y_fin, x_last, y_last, acc, norm_recv,
                  own_sem, part_ssem, part_rsem, x_ssem, x_rsem, y_ssem, y_rsem,
                  xf_ssem, xf_rsem, yf_ssem, yf_rsem, n_ssem, n_rsem, w_sem, m_sem):
    me, part, along_x, along_y = places()
    diag = along_x + along_y - me
    shift = part - me
    blocks = (me, along_x, along_y, diag)
    shard_len = shard_rows * LANES
    full = CHUNK_ROWS * LANES
    chunks = -(-shard_rows // CHUNK_ROWS)
    tail_rows = shard_rows - (chunks - 1) * CHUNK_ROWS
    tail = tail_rows * LANES

    num_dev = grad.shape[1] // shard_len
    others = [(me + k) % num_dev for k in range(1, num_dev)]
    fetches = (pltpu.make_async_copy(w, w_out.at[pl.ds(0, shard_rows)], w_sem),
               pltpu.make_async_copy(m, m_out.at[pl.ds(0, shard_rows)], m_sem))

    meet(others)
    acc[...] = jnp.zeros_like(acc)

    def loads(i, size):
        slot = i % SLOTS
        out = []
        for b, block in enumerate(blocks):
            src = pl.multiple_of(block * shard_len + i * full, LANES)
            out.append(pltpu.make_async_copy(
                grad.at[:, pl.ds(src, size)], own.at[slot, b, :, pl.ds(0, size)], own_sem.at[slot, b]))
        return out

    def swaps(i, size):
        slot = i % SLOTS
        out = []
        for b, block in enumerate(blocks):
            src = pl.multiple_of((block + shift) * shard_len + i * full, LANES)
            out.append(remote(
                grad.at[:, pl.ds(src, size)], other.at[slot, b, :, pl.ds(0, size)],
                part_ssem.at[slot, b], part_rsem.at[slot, b], part))
        return out

    def first_hops(j):
        slot = j % SLOTS
        return (remote(x_send.at[slot], x_recv.at[slot], x_ssem.at[slot], x_rsem.at[slot], along_x),
                remote(y_send.at[slot], y_recv.at[slot], y_ssem.at[slot], y_rsem.at[slot], along_y))

    def last_hops(j):
        slot = j % SLOTS
        return (remote(x_fin.at[slot], x_last.at[slot], xf_ssem.at[slot], xf_rsem.at[slot], along_x),
                remote(y_fin.at[slot], y_last.at[slot], yf_ssem.at[slot], yf_rsem.at[slot], along_y))

    def for_size(i, do):
        @pl.when(i < chunks - 1)
        def _():
            do(full)

        @pl.when(i == chunks - 1)
        def _():
            do(tail)

    def begin(i):
        def do(size):
            for cp in loads(i, size) + swaps(i, size):
                cp.start()
        for_size(i, do)

    def pair_sums(j):
        def do(size):
            for cp in loads(j, size) + swaps(j, size):
                cp.wait()
        for_size(j, do)
        slot = j % SLOTS

        def tile(t, carry):
            for half in range(2):
                row = pl.multiple_of(t * 8, 8)
                col = pl.multiple_of((t + half * (HALF_ROWS // 8)) * 8 * LANES, 8 * LANES)

                def pair(b):
                    a = own[slot, b, :, pl.ds(col, 8 * LANES)].astype(jnp.float32)
                    o = other[slot, b, :, pl.ds(col, 8 * LANES)].astype(jnp.float32)
                    return (a + o).reshape(8, LANES)

                mine[slot, half, pl.ds(row, 8)] = pair(0)
                if half == 0:
                    x_send[slot, 0, pl.ds(row, 8)] = pair(1)
                    y_keep[slot, pl.ds(row, 8)] = pair(2)
                    x_send[slot, 1, pl.ds(row, 8)] = pair(3)
                else:
                    x_keep[slot, pl.ds(row, 8)] = pair(1)
                    y_send[slot, 0, pl.ds(row, 8)] = pair(2)
                    y_send[slot, 1, pl.ds(row, 8)] = pair(3)
            return carry

        lax.fori_loop(0, HALF_ROWS // 8, tile, 0)
        for cp in first_hops(j):
            cp.start()

    def relay(j):
        for cp in first_hops(j):
            cp.wait()
        slot = j % SLOTS
        x_fin[slot] = x_keep[slot] + y_recv[slot, 1]
        y_fin[slot] = y_keep[slot] + x_recv[slot, 1]
        for cp in last_hops(j):
            cp.start()
        mine[slot, 0] = mine[slot, 0] + x_recv[slot, 0]
        mine[slot, 1] = mine[slot, 1] + y_recv[slot, 0]

    def finish(j):
        for cp in last_hops(j):
            cp.wait()
        slot = j % SLOTS
        base = j * CHUNK_ROWS
        left = shard_rows - j * CHUNK_ROWS
        rows = lax.broadcasted_iota(jnp.int32, (8, LANES), 0)

        def tile(t, total):
            row = pl.multiple_of(t * 8, 8)
            top = (mine[slot, 0, pl.ds(row, 8)] + y_last[slot, pl.ds(row, 8)]) * 0.125
            low = (mine[slot, 1, pl.ds(row, 8)] + x_last[slot, pl.ds(row, 8)]) * 0.125
            g_out[pl.ds(pl.multiple_of(base + t * 8, 8), 8)] = top
            g_out[pl.ds(pl.multiple_of(base + HALF_ROWS + t * 8, 8), 8)] = low
            total = total + jnp.where(rows + t * 8 < left, top * top, 0.0)
            return total + jnp.where(rows + (HALF_ROWS + t * 8) < left, low * low, 0.0)

        acc[...] += lax.fori_loop(0, HALF_ROWS // 8, tile, jnp.zeros((8, LANES), jnp.float32))

    def step(i, carry):
        @pl.when(i < chunks)
        def _():
            begin(i)

        @pl.when((i >= 1) & (i < chunks + 1))
        def _():
            pair_sums(i - 1)

        @pl.when((i >= 2) & (i < chunks + 2))
        def _():
            relay(i - 2)

        @pl.when(i == 4)
        def _():
            for cp in fetches:
                cp.start()

        @pl.when(i >= 4)
        def _():
            finish(i - 4)

        return carry

    lax.fori_loop(0, chunks + 4, step, 0)
    norm_recv[me] = acc[...]

    def shares(peer, k):
        return remote(acc, norm_recv.at[me], n_ssem.at[k], n_rsem.at[me], peer)

    for k, peer in enumerate(others):
        shares(peer, k).start()
    for k, peer in enumerate(others):
        shares(peer, k).wait_send()
        remote(acc, norm_recv.at[peer], n_ssem.at[k], n_rsem.at[peer], peer).wait_recv()
    total = norm_recv[0]
    for k in range(1, num_dev):
        total = total + norm_recv[k]
    for cp in fetches:
        cp.wait()
    norm_out[...] = jnp.broadcast_to(jnp.sqrt(jnp.sum(total, keepdims=True)), norm_out.shape)


def reduce_scatter(grad_row, w, m, shard_rows, num_dev):
    f32, bf16 = jnp.float32, jnp.bfloat16
    chunks = -(-shard_rows // CHUNK_ROWS)
    vm, dma = pltpu.VMEM, pltpu.SemaphoreType.DMA
    pair = (SLOTS, 2, HALF_ROWS, LANES)
    one = (SLOTS, HALF_ROWS, LANES)
    raw = (SLOTS, 4, 1, CHUNK_ROWS * LANES)
    state = vm((chunks * CHUNK_ROWS, LANES), f32)
    return pl.pallas_call(
        functools.partial(reduce_kernel, shard_rows),
        out_shape=(state, state, state, jax.ShapeDtypeStruct((8, LANES), f32)),
        in_specs=[pl.BlockSpec(memory_space=pltpu.HBM)] * 3,
        out_specs=(pl.BlockSpec(memory_space=vm),) * 4,
        scratch_shapes=[
            vm(raw, bf16), vm(raw, bf16), vm(pair, f32), vm(pair, f32), vm(one, f32), vm(one, f32),
            vm(pair, f32), vm(pair, f32), vm(pair, f32), vm(one, f32), vm(one, f32), vm(one, f32),
            vm(one, f32), vm((8, LANES), f32),
            vm((num_dev, 8, LANES), f32),
            dma((SLOTS, 4)), dma((SLOTS, 4)), dma((SLOTS, 4)),
            dma((SLOTS,)), dma((SLOTS,)), dma((SLOTS,)), dma((SLOTS,)),
            dma((SLOTS,)), dma((SLOTS,)), dma((SLOTS,)), dma((SLOTS,)),
            dma((num_dev - 1,)), dma((num_dev,)), dma, dma],
        compiler_params=pltpu.CompilerParams(collective_id=0, has_side_effects=True,
                                             vmem_limit_bytes=VMEM_LIMIT),
    )(grad_row, w, m)


def adamw_kernel(lr, norm, g, w, m, v, mask, w_out, m_out, v_out, packed, norm_out):
    norm_out[0] = norm[0, 0]
    coef = jnp.minimum(1.0, 1.0 / (norm[...] + CLIP_EPS))[0:1]
    h = g[...] * coef
    first = BETA_FIRST * m[...] + (1.0 - BETA_FIRST) * h
    second = BETA_SECOND * v[...] + (1.0 - BETA_SECOND) * h * h
    step_dir = (first / (1.0 - BETA_FIRST ** ADAM_STEP)) / (
        jnp.sqrt(second / (1.0 - BETA_SECOND ** ADAM_STEP)) + ADAM_EPS)
    old = w[...]
    new = old - lr[0] * (step_dir + WEIGHT_DECAY * mask[...].astype(jnp.float32) * old)
    w_out[...] = new
    m_out[...] = first
    v_out[...] = second
    packed[...] = new.reshape(packed.shape).astype(packed.dtype)


def adamw(lr, norm, g, w, m, v, mask):
    rows = v.shape[0]
    block = pl.BlockSpec((ADAM_ROWS, LANES), lambda i: (i, 0))
    state = jax.ShapeDtypeStruct((rows, LANES), jnp.float32)
    return pl.pallas_call(
        adamw_kernel,
        grid=(-(-rows // ADAM_ROWS),),
        out_shape=(state, state, state, pltpu.VMEM((g.shape[0] // 4, 4, LANES), jnp.bfloat16),
                   jax.ShapeDtypeStruct((1,), jnp.float32)),
        in_specs=[pl.BlockSpec(memory_space=pltpu.SMEM),
                  pl.BlockSpec((8, LANES), lambda i: (0, 0)),
                  block, block, block, block, block],
        out_specs=(block, block, block, pl.BlockSpec((ADAM_ROWS // 4, 4, LANES), lambda i: (i, 0, 0)),
                   pl.BlockSpec(memory_space=pltpu.SMEM)),
        compiler_params=pltpu.CompilerParams(vmem_limit_bytes=VMEM_LIMIT),
    )(lr, norm, stay(g), stay(w), stay(m), v, mask)


def gather_kernel(grains, own, whole, x_ssem, y_ssem, xr_ssem, yr_ssem, part_ssem,
                  x_rsem, y_rsem, d_rsem, part_rsem):
    me, part, along_x, along_y = places()
    diag = along_x + along_y - me
    size = grains // GATHER_CHUNKS

    def at(block, q):
        return whole.at[pl.ds(block * grains + q * size, size)]

    def block_at(block):
        return whole.at[pl.ds(block * grains, grains)]

    def to_part(src, block, q, k):
        return remote(src, at(block, q), part_ssem.at[k], part_rsem.at[k], part)

    meet((part, along_x, along_y))

    def mine(q):
        src = own.at[pl.ds(q * size, size)]
        return (remote(src, at(me, q), x_ssem, x_rsem.at[q], along_x),
                remote(src, at(me, q), y_ssem, y_rsem.at[q], along_y),
                to_part(src, me, q, 0))

    def send(q, carry):
        for cp in mine(q):
            cp.start()
        return carry

    lax.fori_loop(0, GATHER_CHUNKS, send, 0)

    def pass_on(q, carry):
        got = at(along_x, q)
        remote(got, got, x_ssem, x_rsem.at[q], along_x).wait_recv()
        to_part(got, along_x, q, 1).start()

        @pl.when(q % 2 == 0)
        def _():
            remote(got, got, yr_ssem, d_rsem.at[q], along_y).start()

        got = at(along_y, q)
        remote(got, got, y_ssem, y_rsem.at[q], along_y).wait_recv()
        to_part(got, along_y, q, 2).start()

        @pl.when(q % 2 == 1)
        def _():
            remote(got, got, xr_ssem, d_rsem.at[q], along_x).start()

        return carry

    lax.fori_loop(0, GATHER_CHUNKS, pass_on, 0)

    def last(q, carry):
        got = at(diag, q)
        remote(got, got, xr_ssem, d_rsem.at[q], along_x).wait_recv()
        to_part(got, diag, q, 3).start()
        return carry

    lax.fori_loop(0, GATHER_CHUNKS, last, 0)

    evens = size * ((GATHER_CHUNKS + 1) // 2)
    odds = size * (GATHER_CHUNKS // 2)
    remote(block_at(me), block_at(me), x_ssem, x_rsem.at[0], along_x).wait_send()
    remote(block_at(me), block_at(me), y_ssem, y_rsem.at[0], along_y).wait_send()
    some = whole.at[pl.ds(0, evens)]
    remote(some, some, yr_ssem, d_rsem.at[0], along_y).wait_send()
    some = whole.at[pl.ds(0, odds)]
    remote(some, some, xr_ssem, d_rsem.at[0], along_x).wait_send()
    shift = part - me
    for k, block in enumerate((me, along_x, along_y, diag)):
        cp = remote(block_at(block), block_at(block + shift), part_ssem.at[k], part_rsem.at[k], part)
        cp.wait_send()
        cp.wait_recv()


def all_gather(packed, grains, num_dev):
    vm, dma = pltpu.VMEM, pltpu.SemaphoreType.DMA
    return pl.pallas_call(
        functools.partial(gather_kernel, grains),
        out_shape=vm((num_dev * grains, 4, LANES), jnp.bfloat16),
        in_specs=[pl.BlockSpec(memory_space=vm)],
        out_specs=pl.BlockSpec(memory_space=vm),
        scratch_shapes=[dma, dma, dma, dma, dma((4,)),
                        dma((GATHER_CHUNKS,)), dma((GATHER_CHUNKS,)), dma((GATHER_CHUNKS,)), dma((4,))],
        compiler_params=pltpu.CompilerParams(collective_id=1, has_side_effects=True,
                                             vmem_limit_bytes=1 << 20),
    )(stay(packed))


def store_kernel(grains, own, whole, params, sem):
    me = lax.axis_index("dp")
    num_dev = whole.shape[0] // grains
    copies = []
    for k in range(num_dev):
        block = (me + k) % num_dev
        dst = params.at[pl.ds(block * grains, grains)]
        src = own.at[pl.ds(0, grains)] if k == 0 else whole.at[pl.ds(block * grains, grains)]
        copies.append(pltpu.make_async_copy(src, dst, sem.at[k]))
    for cp in copies:
        cp.start()
    for cp in copies:
        cp.wait()


def store(packed, whole, grains, num_dev):
    return pl.pallas_call(
        functools.partial(store_kernel, grains),
        out_shape=jax.ShapeDtypeStruct(whole.shape, whole.dtype),
        in_specs=[pl.BlockSpec(memory_space=pltpu.VMEM)] * 2,
        out_specs=pl.BlockSpec(memory_space=pl.ANY),
        scratch_shapes=[pltpu.SemaphoreType.DMA((num_dev,))],
        compiler_params=pltpu.CompilerParams(vmem_limit_bytes=1 << 20),
    )(stay(packed), stay(whole))


def solution(mesh):
    num_dev = mesh.shape["dp"]

    def local_step(grad_row, master, mom_first, mom_second, decay_mask, learn_rate):
        shard_len = master.shape[0]
        rows = shard_len // LANES
        flat = lambda a: a.reshape(rows, LANES)
        g, w, m, norm = reduce_scatter(grad_row, flat(master), flat(mom_first), rows, num_dev)
        new_w, new_m, new_v, packed, grad_norm = adamw(
            learn_rate, norm, g, w, m, flat(mom_second), flat(decay_mask))
        whole = all_gather(packed, rows // 4, num_dev)
        params = store(packed, whole, rows // 4, num_dev).reshape(num_dev * shard_len)
        return (params, new_w.reshape(shard_len), new_m.reshape(shard_len), new_v.reshape(shard_len),
                grad_norm)

    return jax.shard_map(
        local_step, mesh=mesh,
        in_specs=(P("dp", None), P("dp"), P("dp"), P("dp"), P("dp"), P()),
        out_specs=(P(), P("dp"), P("dp"), P("dp"), P()), check_vma=False)
```

```python
import functools

import jax
import jax.numpy as jnp
from jax import lax
from jax.experimental import pallas as pl
from jax.experimental.pallas import tpu as pltpu
from jax.sharding import PartitionSpec as P

BETA_FIRST = 0.9
BETA_SECOND = 0.95
ADAM_EPS = 1e-8
CLIP_EPS = 1e-6
WEIGHT_DECAY = 0.1
ADAM_STEP = 10

MESH = pl.DeviceIdType.MESH
LANES = 128
CHUNK_ROWS = 384
HALF_ROWS = CHUNK_ROWS // 2
SLOTS = 4
VMEM_LIMIT = 20 << 20
GATHER_CHUNKS = 23
ADAM_ROWS = 5 * CHUNK_ROWS
TILE_ROWS = 128


def places():
    me = lax.axis_index("dp")
    core = me % 2
    part = me + 1 - 2 * core
    along_x = me + 2 - 4 * ((me // 2) % 2)
    along_y = me + 4 - 8 * (me // 4)
    return me, part, along_x, along_y


def meet(peers):
    barrier = pltpu.get_barrier_semaphore()
    for peer in peers:
        pl.semaphore_signal(barrier, inc=1, device_id=(peer,), device_id_type=MESH)
    pl.semaphore_wait(barrier, len(peers))


def stay(array):
    return pltpu.with_memory_space_constraint(array, pltpu.VMEM)


def remote(src, dst, send_sem, recv_sem, device):
    return pltpu.make_async_remote_copy(
        src_ref=src, dst_ref=dst, send_sem=send_sem, recv_sem=recv_sem,
        device_id=(device,), device_id_type=MESH)


def reduce_kernel(shard_rows, grad, w, m, g_out, w_out, m_out, norm_out,
                  own, other, x_send, y_send, x_keep, y_keep, mine, x_recv, y_recv,
                  x_fin, y_fin, x_last, y_last, acc, norm_recv,
                  own_sem, part_ssem, part_rsem, x_ssem, x_rsem, y_ssem, y_rsem,
                  xf_ssem, xf_rsem, yf_ssem, yf_rsem, n_ssem, n_rsem, w_sem, m_sem):
    me, part, along_x, along_y = places()
    diag = along_x + along_y - me
    shift = part - me
    blocks = (me, along_x, along_y, diag)
    shard_len = shard_rows * LANES
    full = CHUNK_ROWS * LANES
    chunks = -(-shard_rows // CHUNK_ROWS)
    tail_rows = shard_rows - (chunks - 1) * CHUNK_ROWS
    tail = tail_rows * LANES

    num_dev = grad.shape[1] // shard_len
    others = [(me + k) % num_dev for k in range(1, num_dev)]
    fetches = (pltpu.make_async_copy(w, w_out.at[pl.ds(0, shard_rows)], w_sem),
               pltpu.make_async_copy(m, m_out.at[pl.ds(0, shard_rows)], m_sem))

    meet(others)
    acc[...] = jnp.zeros_like(acc)

    def loads(i, size):
        slot = i % SLOTS
        out = []
        for b, block in enumerate(blocks):
            src = pl.multiple_of(block * shard_len + i * full, LANES)
            out.append(pltpu.make_async_copy(
                grad.at[:, pl.ds(src, size)], own.at[slot, b, :, pl.ds(0, size)], own_sem.at[slot, b]))
        return out

    def swaps(i, size):
        slot = i % SLOTS
        out = []
        for b, block in enumerate(blocks):
            src = pl.multiple_of((block + shift) * shard_len + i * full, LANES)
            out.append(remote(
                grad.at[:, pl.ds(src, size)], other.at[slot, b, :, pl.ds(0, size)],
                part_ssem.at[slot, b], part_rsem.at[slot, b], part))
        return out

    def first_hops(j):
        slot = j % SLOTS
        return (remote(x_send.at[slot], x_recv.at[slot], x_ssem.at[slot], x_rsem.at[slot], along_x),
                remote(y_send.at[slot], y_recv.at[slot], y_ssem.at[slot], y_rsem.at[slot], along_y))

    def last_hops(j):
        slot = j % SLOTS
        return (remote(x_fin.at[slot], x_last.at[slot], xf_ssem.at[slot], xf_rsem.at[slot], along_x),
                remote(y_fin.at[slot], y_last.at[slot], yf_ssem.at[slot], yf_rsem.at[slot], along_y))

    def for_size(i, do):
        @pl.when(i < chunks - 1)
        def _():
            do(full)

        @pl.when(i == chunks - 1)
        def _():
            do(tail)

    def begin(i):
        def do(size):
            for cp in loads(i, size) + swaps(i, size):
                cp.start()
        for_size(i, do)

    def pair_sums(j):
        def do(size):
            for cp in loads(j, size) + swaps(j, size):
                cp.wait()
        for_size(j, do)
        slot = j % SLOTS

        def tile(t, carry):
            for half in range(2):
                row = pl.multiple_of(t * 8, 8)
                col = pl.multiple_of((t + half * (HALF_ROWS // 8)) * 8 * LANES, 8 * LANES)

                def pair(b):
                    a = own[slot, b, :, pl.ds(col, 8 * LANES)].astype(jnp.float32)
                    o = other[slot, b, :, pl.ds(col, 8 * LANES)].astype(jnp.float32)
                    return (a + o).reshape(8, LANES)

                mine[slot, half, pl.ds(row, 8)] = pair(0)
                if half == 0:
                    x_send[slot, 0, pl.ds(row, 8)] = pair(1)
                    y_keep[slot, pl.ds(row, 8)] = pair(2)
                    x_send[slot, 1, pl.ds(row, 8)] = pair(3)
                else:
                    x_keep[slot, pl.ds(row, 8)] = pair(1)
                    y_send[slot, 0, pl.ds(row, 8)] = pair(2)
                    y_send[slot, 1, pl.ds(row, 8)] = pair(3)
            return carry

        lax.fori_loop(0, HALF_ROWS // 8, tile, 0)
        for cp in first_hops(j):
            cp.start()

    def relay(j):
        for cp in first_hops(j):
            cp.wait()
        slot = j % SLOTS
        x_fin[slot] = x_keep[slot] + y_recv[slot, 1]
        y_fin[slot] = y_keep[slot] + x_recv[slot, 1]
        for cp in last_hops(j):
            cp.start()
        mine[slot, 0] = mine[slot, 0] + x_recv[slot, 0]
        mine[slot, 1] = mine[slot, 1] + y_recv[slot, 0]

    def finish(j):
        for cp in last_hops(j):
            cp.wait()
        slot = j % SLOTS
        base = j * CHUNK_ROWS
        left = shard_rows - j * CHUNK_ROWS
        rows = lax.broadcasted_iota(jnp.int32, (8, LANES), 0)

        def tile(t, total):
            row = pl.multiple_of(t * 8, 8)
            top = (mine[slot, 0, pl.ds(row, 8)] + y_last[slot, pl.ds(row, 8)]) * 0.125
            low = (mine[slot, 1, pl.ds(row, 8)] + x_last[slot, pl.ds(row, 8)]) * 0.125
            g_out[pl.ds(pl.multiple_of(base + t * 8, 8), 8)] = top
            g_out[pl.ds(pl.multiple_of(base + HALF_ROWS + t * 8, 8), 8)] = low
            total = total + jnp.where(rows + t * 8 < left, top * top, 0.0)
            return total + jnp.where(rows + (HALF_ROWS + t * 8) < left, low * low, 0.0)

        acc[...] += lax.fori_loop(0, HALF_ROWS // 8, tile, jnp.zeros((8, LANES), jnp.float32))

    def step(i, carry):
        @pl.when(i < chunks)
        def _():
            begin(i)

        @pl.when((i >= 1) & (i < chunks + 1))
        def _():
            pair_sums(i - 1)

        @pl.when((i >= 2) & (i < chunks + 2))
        def _():
            relay(i - 2)

        @pl.when(i == 4)
        def _():
            for cp in fetches:
                cp.start()

        @pl.when(i >= 4)
        def _():
            finish(i - 4)

        return carry

    lax.fori_loop(0, chunks + 4, step, 0)
    norm_recv[me] = acc[...]

    def shares(peer, k):
        return remote(acc, norm_recv.at[me], n_ssem.at[k], n_rsem.at[me], peer)

    for k, peer in enumerate(others):
        shares(peer, k).start()
    for k, peer in enumerate(others):
        shares(peer, k).wait_send()
        remote(acc, norm_recv.at[peer], n_ssem.at[k], n_rsem.at[peer], peer).wait_recv()
    total = norm_recv[0]
    for k in range(1, num_dev):
        total = total + norm_recv[k]
    for cp in fetches:
        cp.wait()
    norm_out[...] = jnp.broadcast_to(jnp.sqrt(jnp.sum(total, keepdims=True)), norm_out.shape)


def reduce_scatter(grad_row, w, m, shard_rows, num_dev):
    f32, bf16 = jnp.float32, jnp.bfloat16
    chunks = -(-shard_rows // CHUNK_ROWS)
    vm, dma = pltpu.VMEM, pltpu.SemaphoreType.DMA
    pair = (SLOTS, 2, HALF_ROWS, LANES)
    one = (SLOTS, HALF_ROWS, LANES)
    raw = (SLOTS, 4, 1, CHUNK_ROWS * LANES)
    state = vm((chunks * CHUNK_ROWS, LANES), f32)
    return pl.pallas_call(
        functools.partial(reduce_kernel, shard_rows),
        out_shape=(state, state, state, jax.ShapeDtypeStruct((8, LANES), f32)),
        in_specs=[pl.BlockSpec(memory_space=pltpu.HBM)] * 3,
        out_specs=(pl.BlockSpec(memory_space=vm),) * 4,
        scratch_shapes=[
            vm(raw, bf16), vm(raw, bf16), vm(pair, f32), vm(pair, f32), vm(one, f32), vm(one, f32),
            vm(pair, f32), vm(pair, f32), vm(pair, f32), vm(one, f32), vm(one, f32), vm(one, f32),
            vm(one, f32), vm((8, LANES), f32),
            vm((num_dev, 8, LANES), f32),
            dma((SLOTS, 4)), dma((SLOTS, 4)), dma((SLOTS, 4)),
            dma((SLOTS,)), dma((SLOTS,)), dma((SLOTS,)), dma((SLOTS,)),
            dma((SLOTS,)), dma((SLOTS,)), dma((SLOTS,)), dma((SLOTS,)),
            dma((num_dev - 1,)), dma((num_dev,)), dma, dma],
        compiler_params=pltpu.CompilerParams(collective_id=0, has_side_effects=True,
                                             vmem_limit_bytes=VMEM_LIMIT),
    )(grad_row, w, m)


def adamw_kernel(lr, norm, g, w, m, v, mask, w_out, m_out, v_out, packed, norm_out):
    norm_out[0] = norm[0, 0]
    coef = jnp.minimum(1.0, 1.0 / (norm[0:1] + CLIP_EPS))
    rate = lr[0]

    def tile(t, carry):
        at = pl.ds(pl.multiple_of(t * TILE_ROWS, TILE_ROWS), TILE_ROWS)
        h = g[at] * coef
        first = BETA_FIRST * m[at] + (1.0 - BETA_FIRST) * h
        second = BETA_SECOND * v[at] + (1.0 - BETA_SECOND) * h * h
        step_dir = (first * (1.0 / (1.0 - BETA_FIRST ** ADAM_STEP))) / (
            jnp.sqrt(second * (1.0 / (1.0 - BETA_SECOND ** ADAM_STEP))) + ADAM_EPS)
        old = w[at]
        new = old - rate * (step_dir + WEIGHT_DECAY * mask[at].astype(jnp.float32) * old)
        w_out[at] = new
        m_out[at] = first
        v_out[at] = second
        grains = TILE_ROWS // 4
        packed[pl.ds(pl.multiple_of(t * grains, grains), grains)] = new.reshape(grains, 4, LANES).astype(packed.dtype)
        return carry

    lax.fori_loop(0, ADAM_ROWS // TILE_ROWS, tile, 0)


def adamw(lr, norm, g, w, m, v, mask):
    rows = v.shape[0]
    block = pl.BlockSpec((ADAM_ROWS, LANES), lambda i: (i, 0))
    state = jax.ShapeDtypeStruct((rows, LANES), jnp.float32)
    return pl.pallas_call(
        adamw_kernel,
        grid=(-(-rows // ADAM_ROWS),),
        out_shape=(state, state, state, pltpu.VMEM((g.shape[0] // 4, 4, LANES), jnp.bfloat16),
                   jax.ShapeDtypeStruct((1,), jnp.float32)),
        in_specs=[pl.BlockSpec(memory_space=pltpu.SMEM),
                  pl.BlockSpec((8, LANES), lambda i: (0, 0)),
                  block, block, block, block, block],
        out_specs=(block, block, block, pl.BlockSpec((ADAM_ROWS // 4, 4, LANES), lambda i: (i, 0, 0)),
                   pl.BlockSpec(memory_space=pltpu.SMEM)),
        compiler_params=pltpu.CompilerParams(vmem_limit_bytes=VMEM_LIMIT),
    )(lr, norm, stay(g), stay(w), stay(m), v, mask)


def gather_kernel(grains, own, whole, x_ssem, y_ssem, xr_ssem, yr_ssem, part_ssem,
                  x_rsem, y_rsem, d_rsem, part_rsem):
    me, part, along_x, along_y = places()
    diag = along_x + along_y - me
    size = grains // GATHER_CHUNKS

    def at(block, q):
        return whole.at[pl.ds(block * grains + q * size, size)]

    def block_at(block):
        return whole.at[pl.ds(block * grains, grains)]

    def to_part(src, block, q, k):
        return remote(src, at(block, q), part_ssem.at[k], part_rsem.at[k], part)

    meet((part, along_x, along_y))

    def mine(q):
        src = own.at[pl.ds(q * size, size)]
        return (remote(src, at(me, q), x_ssem, x_rsem.at[q], along_x),
                remote(src, at(me, q), y_ssem, y_rsem.at[q], along_y),
                to_part(src, me, q, 0))

    def send(q, carry):
        for cp in mine(q):
            cp.start()
        return carry

    lax.fori_loop(0, GATHER_CHUNKS, send, 0)

    def pass_on(q, carry):
        got = at(along_x, q)
        remote(got, got, x_ssem, x_rsem.at[q], along_x).wait_recv()
        to_part(got, along_x, q, 1).start()

        @pl.when(q % 2 == 0)
        def _():
            remote(got, got, yr_ssem, d_rsem.at[q], along_y).start()

        got = at(along_y, q)
        remote(got, got, y_ssem, y_rsem.at[q], along_y).wait_recv()
        to_part(got, along_y, q, 2).start()

        @pl.when(q % 2 == 1)
        def _():
            remote(got, got, xr_ssem, d_rsem.at[q], along_x).start()

        return carry

    lax.fori_loop(0, GATHER_CHUNKS, pass_on, 0)

    def last(q, carry):
        got = at(diag, q)
        remote(got, got, xr_ssem, d_rsem.at[q], along_x).wait_recv()
        to_part(got, diag, q, 3).start()
        return carry

    lax.fori_loop(0, GATHER_CHUNKS, last, 0)

    evens = size * ((GATHER_CHUNKS + 1) // 2)
    odds = size * (GATHER_CHUNKS // 2)
    remote(block_at(me), block_at(me), x_ssem, x_rsem.at[0], along_x).wait_send()
    remote(block_at(me), block_at(me), y_ssem, y_rsem.at[0], along_y).wait_send()
    some = whole.at[pl.ds(0, evens)]
    remote(some, some, yr_ssem, d_rsem.at[0], along_y).wait_send()
    some = whole.at[pl.ds(0, odds)]
    remote(some, some, xr_ssem, d_rsem.at[0], along_x).wait_send()
    shift = part - me
    for k, block in enumerate((me, along_x, along_y, diag)):
        cp = remote(block_at(block), block_at(block + shift), part_ssem.at[k], part_rsem.at[k], part)
        cp.wait_send()
        cp.wait_recv()


def all_gather(packed, grains, num_dev):
    vm, dma = pltpu.VMEM, pltpu.SemaphoreType.DMA
    return pl.pallas_call(
        functools.partial(gather_kernel, grains),
        out_shape=vm((num_dev * grains, 4, LANES), jnp.bfloat16),
        in_specs=[pl.BlockSpec(memory_space=vm)],
        out_specs=pl.BlockSpec(memory_space=vm),
        scratch_shapes=[dma, dma, dma, dma, dma((4,)),
                        dma((GATHER_CHUNKS,)), dma((GATHER_CHUNKS,)), dma((GATHER_CHUNKS,)), dma((4,))],
        compiler_params=pltpu.CompilerParams(collective_id=1, has_side_effects=True,
                                             vmem_limit_bytes=1 << 20),
    )(stay(packed))


def store_kernel(grains, own, whole, params, sem):
    me = lax.axis_index("dp")
    num_dev = whole.shape[0] // grains
    copies = []
    for k in range(num_dev):
        block = (me + k) % num_dev
        dst = params.at[pl.ds(block * grains, grains)]
        src = own.at[pl.ds(0, grains)] if k == 0 else whole.at[pl.ds(block * grains, grains)]
        copies.append(pltpu.make_async_copy(src, dst, sem.at[k]))
    for cp in copies:
        cp.start()
    for cp in copies:
        cp.wait()


def store(packed, whole, grains, num_dev):
    return pl.pallas_call(
        functools.partial(store_kernel, grains),
        out_shape=jax.ShapeDtypeStruct(whole.shape, whole.dtype),
        in_specs=[pl.BlockSpec(memory_space=pltpu.VMEM)] * 2,
        out_specs=pl.BlockSpec(memory_space=pl.ANY),
        scratch_shapes=[pltpu.SemaphoreType.DMA((num_dev,))],
        compiler_params=pltpu.CompilerParams(vmem_limit_bytes=1 << 20),
    )(stay(packed), stay(whole))


def solution(mesh):
    num_dev = mesh.shape["dp"]

    def local_step(grad_row, master, mom_first, mom_second, decay_mask, learn_rate):
        shard_len = master.shape[0]
        rows = shard_len // LANES
        flat = lambda a: a.reshape(rows, LANES)
        g, w, m, norm = reduce_scatter(grad_row, flat(master), flat(mom_first), rows, num_dev)
        new_w, new_m, new_v, packed, grad_norm = adamw(
            learn_rate, norm, g, w, m, flat(mom_second), flat(decay_mask))
        whole = all_gather(packed, rows // 4, num_dev)
        params = store(packed, whole, rows // 4, num_dev).reshape(num_dev * shard_len)
        return (params, new_w.reshape(shard_len), new_m.reshape(shard_len), new_v.reshape(shard_len),
                grad_norm)

    return jax.shard_map(
        local_step, mesh=mesh,
        in_specs=(P("dp", None), P("dp"), P("dp"), P("dp"), P("dp"), P()),
        out_specs=(P(), P("dp"), P("dp"), P("dp"), P()), check_vma=False)
```

```python
import functools

import jax
import jax.numpy as jnp
from jax import lax
from jax.experimental import pallas as pl
from jax.experimental.pallas import tpu as pltpu
from jax.sharding import PartitionSpec as P

BETA_FIRST = 0.9
BETA_SECOND = 0.95
ADAM_EPS = 1e-8
CLIP_EPS = 1e-6
WEIGHT_DECAY = 0.1
ADAM_STEP = 10

MESH = pl.DeviceIdType.MESH
LANES = 128
CHUNK_ROWS = 384
HALF_ROWS = CHUNK_ROWS // 2
SLOTS = 4
VMEM_LIMIT = 20 << 20
PARTS = 4
ADAM_ROWS = 1560
TILE_ROWS = 120


def places():
    me = lax.axis_index("dp")
    core = me % 2
    part = me + 1 - 2 * core
    along_x = me + 2 - 4 * ((me // 2) % 2)
    along_y = me + 4 - 8 * (me // 4)
    return me, part, along_x, along_y


def meet(peers):
    barrier = pltpu.get_barrier_semaphore()
    for peer in peers:
        pl.semaphore_signal(barrier, inc=1, device_id=(peer,), device_id_type=MESH)
    pl.semaphore_wait(barrier, len(peers))


def stay(array):
    return pltpu.with_memory_space_constraint(array, pltpu.VMEM)


def remote(src, dst, send_sem, recv_sem, device):
    return pltpu.make_async_remote_copy(
        src_ref=src, dst_ref=dst, send_sem=send_sem, recv_sem=recv_sem,
        device_id=(device,), device_id_type=MESH)


def reduce_kernel(shard_rows, grad, w, m, g_out, w_out, m_out, norm_out,
                  own, other, x_send, y_send, x_keep, y_keep, mine, x_recv, y_recv,
                  x_fin, y_fin, x_last, y_last, acc, norm_recv,
                  own_sem, part_ssem, part_rsem, x_ssem, x_rsem, y_ssem, y_rsem,
                  xf_ssem, xf_rsem, yf_ssem, yf_rsem, n_ssem, n_rsem, w_sem, m_sem):
    me, part, along_x, along_y = places()
    diag = along_x + along_y - me
    shift = part - me
    blocks = (me, along_x, along_y, diag)
    shard_len = shard_rows * LANES
    full = CHUNK_ROWS * LANES
    chunks = -(-shard_rows // CHUNK_ROWS)
    tail_rows = shard_rows - (chunks - 1) * CHUNK_ROWS
    tail = tail_rows * LANES

    num_dev = grad.shape[1] // shard_len
    others = [(me + k) % num_dev for k in range(1, num_dev)]
    fetches = (pltpu.make_async_copy(w, w_out.at[pl.ds(0, shard_rows)], w_sem),
               pltpu.make_async_copy(m, m_out.at[pl.ds(0, shard_rows)], m_sem))

    meet(others)
    acc[...] = jnp.zeros_like(acc)

    def loads(i, size):
        slot = i % SLOTS
        out = []
        for b, block in enumerate(blocks):
            src = pl.multiple_of(block * shard_len + i * full, LANES)
            out.append(pltpu.make_async_copy(
                grad.at[:, pl.ds(src, size)], own.at[slot, b, :, pl.ds(0, size)], own_sem.at[slot, b]))
        return out

    def swaps(i, size):
        slot = i % SLOTS
        out = []
        for b, block in enumerate(blocks):
            src = pl.multiple_of((block + shift) * shard_len + i * full, LANES)
            out.append(remote(
                grad.at[:, pl.ds(src, size)], other.at[slot, b, :, pl.ds(0, size)],
                part_ssem.at[slot, b], part_rsem.at[slot, b], part))
        return out

    def first_hops(j):
        slot = j % SLOTS
        return (remote(x_send.at[slot], x_recv.at[slot], x_ssem.at[slot], x_rsem.at[slot], along_x),
                remote(y_send.at[slot], y_recv.at[slot], y_ssem.at[slot], y_rsem.at[slot], along_y))

    def last_hops(j):
        slot = j % SLOTS
        return (remote(x_fin.at[slot], x_last.at[slot], xf_ssem.at[slot], xf_rsem.at[slot], along_x),
                remote(y_fin.at[slot], y_last.at[slot], yf_ssem.at[slot], yf_rsem.at[slot], along_y))

    def for_size(i, do):
        @pl.when(i < chunks - 1)
        def _():
            do(full)

        @pl.when(i == chunks - 1)
        def _():
            do(tail)

    def begin(i):
        def do(size):
            for cp in loads(i, size) + swaps(i, size):
                cp.start()
        for_size(i, do)

    def pair_sums(j):
        def do(size):
            for cp in loads(j, size) + swaps(j, size):
                cp.wait()
        for_size(j, do)
        slot = j % SLOTS

        def tile(t, carry):
            for half in range(2):
                row = pl.multiple_of(t * 8, 8)
                col = pl.multiple_of((t + half * (HALF_ROWS // 8)) * 8 * LANES, 8 * LANES)

                def pair(b):
                    a = own[slot, b, :, pl.ds(col, 8 * LANES)].astype(jnp.float32)
                    o = other[slot, b, :, pl.ds(col, 8 * LANES)].astype(jnp.float32)
                    return (a + o).reshape(8, LANES)

                mine[slot, half, pl.ds(row, 8)] = pair(0)
                if half == 0:
                    x_send[slot, 0, pl.ds(row, 8)] = pair(1)
                    y_keep[slot, pl.ds(row, 8)] = pair(2)
                    x_send[slot, 1, pl.ds(row, 8)] = pair(3)
                else:
                    x_keep[slot, pl.ds(row, 8)] = pair(1)
                    y_send[slot, 0, pl.ds(row, 8)] = pair(2)
                    y_send[slot, 1, pl.ds(row, 8)] = pair(3)
            return carry

        lax.fori_loop(0, HALF_ROWS // 8, tile, 0)
        for cp in first_hops(j):
            cp.start()

    def relay(j):
        for cp in first_hops(j):
            cp.wait()
        slot = j % SLOTS
        x_fin[slot] = x_keep[slot] + y_recv[slot, 1]
        y_fin[slot] = y_keep[slot] + x_recv[slot, 1]
        for cp in last_hops(j):
            cp.start()
        mine[slot, 0] = mine[slot, 0] + x_recv[slot, 0]
        mine[slot, 1] = mine[slot, 1] + y_recv[slot, 0]

    def finish(j):
        for cp in last_hops(j):
            cp.wait()
        slot = j % SLOTS
        base = j * CHUNK_ROWS
        left = shard_rows - j * CHUNK_ROWS
        rows = lax.broadcasted_iota(jnp.int32, (8, LANES), 0)

        def tile(t, total):
            row = pl.multiple_of(t * 8, 8)
            top = (mine[slot, 0, pl.ds(row, 8)] + y_last[slot, pl.ds(row, 8)]) * 0.125
            low = (mine[slot, 1, pl.ds(row, 8)] + x_last[slot, pl.ds(row, 8)]) * 0.125
            g_out[pl.ds(pl.multiple_of(base + t * 8, 8), 8)] = top
            g_out[pl.ds(pl.multiple_of(base + HALF_ROWS + t * 8, 8), 8)] = low
            total = total + jnp.where(rows + t * 8 < left, top * top, 0.0)
            return total + jnp.where(rows + (HALF_ROWS + t * 8) < left, low * low, 0.0)

        acc[...] += lax.fori_loop(0, HALF_ROWS // 8, tile, jnp.zeros((8, LANES), jnp.float32))

    def step(i, carry):
        @pl.when(i < chunks)
        def _():
            begin(i)

        @pl.when((i >= 1) & (i < chunks + 1))
        def _():
            pair_sums(i - 1)

        @pl.when((i >= 2) & (i < chunks + 2))
        def _():
            relay(i - 2)

        @pl.when(i == 4)
        def _():
            for cp in fetches:
                cp.start()

        @pl.when(i >= 4)
        def _():
            finish(i - 4)

        return carry

    lax.fori_loop(0, chunks + 4, step, 0)
    norm_recv[me] = acc[...]

    def shares(peer, k):
        return remote(acc, norm_recv.at[me], n_ssem.at[k], n_rsem.at[me], peer)

    for k, peer in enumerate(others):
        shares(peer, k).start()
    for k, peer in enumerate(others):
        shares(peer, k).wait_send()
        remote(acc, norm_recv.at[peer], n_ssem.at[k], n_rsem.at[peer], peer).wait_recv()
    total = norm_recv[0]
    for k in range(1, num_dev):
        total = total + norm_recv[k]
    for cp in fetches:
        cp.wait()
    norm_out[...] = jnp.broadcast_to(jnp.sqrt(jnp.sum(total, keepdims=True)), norm_out.shape)


def reduce_scatter(grad_row, w, m, shard_rows, num_dev):
    f32, bf16 = jnp.float32, jnp.bfloat16
    chunks = -(-shard_rows // CHUNK_ROWS)
    vm, dma = pltpu.VMEM, pltpu.SemaphoreType.DMA
    pair = (SLOTS, 2, HALF_ROWS, LANES)
    one = (SLOTS, HALF_ROWS, LANES)
    raw = (SLOTS, 4, 1, CHUNK_ROWS * LANES)
    state = vm((chunks * CHUNK_ROWS, LANES), f32)
    return pl.pallas_call(
        functools.partial(reduce_kernel, shard_rows),
        out_shape=(state, state, state, jax.ShapeDtypeStruct((8, LANES), f32)),
        in_specs=[pl.BlockSpec(memory_space=pltpu.HBM)] * 3,
        out_specs=(pl.BlockSpec(memory_space=vm),) * 4,
        scratch_shapes=[
            vm(raw, bf16), vm(raw, bf16), vm(pair, f32), vm(pair, f32), vm(one, f32), vm(one, f32),
            vm(pair, f32), vm(pair, f32), vm(pair, f32), vm(one, f32), vm(one, f32), vm(one, f32),
            vm(one, f32), vm((8, LANES), f32),
            vm((num_dev, 8, LANES), f32),
            dma((SLOTS, 4)), dma((SLOTS, 4)), dma((SLOTS, 4)),
            dma((SLOTS,)), dma((SLOTS,)), dma((SLOTS,)), dma((SLOTS,)),
            dma((SLOTS,)), dma((SLOTS,)), dma((SLOTS,)), dma((SLOTS,)),
            dma((num_dev - 1,)), dma((num_dev,)), dma, dma],
        compiler_params=pltpu.CompilerParams(collective_id=0, has_side_effects=True,
                                             vmem_limit_bytes=VMEM_LIMIT),
    )(grad_row, w, m)


def adamw_kernel(lr, norm, g, w, m, v, mask, *rest):
    w_out, m_out, v_out, packed, norm_out = rest[-5:]
    norm_out[0] = norm[0, 0]
    coef = jnp.minimum(1.0, 1.0 / (norm[0:1] + CLIP_EPS))
    rate = lr[0]

    def tile(t, carry):
        at = pl.ds(pl.multiple_of(t * TILE_ROWS, 8), TILE_ROWS)
        h = g[at] * coef
        first = BETA_FIRST * m[at] + (1.0 - BETA_FIRST) * h
        second = BETA_SECOND * v[at] + (1.0 - BETA_SECOND) * h * h
        step_dir = (first * (1.0 / (1.0 - BETA_FIRST ** ADAM_STEP))) / (
            jnp.sqrt(second * (1.0 / (1.0 - BETA_SECOND ** ADAM_STEP))) + ADAM_EPS)
        old = w[at]
        new = old - rate * (step_dir + WEIGHT_DECAY * mask[at].astype(jnp.float32) * old)
        w_out[at] = new
        m_out[at] = first
        v_out[at] = second
        grains = TILE_ROWS // 4
        packed[pl.ds(pl.multiple_of(t * grains, 2), grains)] = new.reshape(grains, 4, LANES).astype(packed.dtype)
        return carry

    lax.fori_loop(0, ADAM_ROWS // TILE_ROWS, tile, 0)


def adamw(part, lr, norm, g, w, m, v, mask, before):
    rows = v.shape[0]
    part_rows = g.shape[0] // PARTS
    steps = part_rows // ADAM_ROWS
    block = pl.BlockSpec((ADAM_ROWS, LANES), lambda i: (i + part * steps, 0))
    state = jax.ShapeDtypeStruct((rows, LANES), jnp.float32)
    blind = [pl.BlockSpec(memory_space=pl.ANY)] * len(before)
    return pl.pallas_call(
        adamw_kernel,
        grid=(steps,),
        out_shape=(state, state, state, jax.ShapeDtypeStruct((part_rows // 4, 4, LANES), jnp.bfloat16),
                   jax.ShapeDtypeStruct((1,), jnp.float32)),
        in_specs=[pl.BlockSpec(memory_space=pltpu.SMEM),
                  pl.BlockSpec((8, LANES), lambda i: (0, 0)),
                  block, block, block, block, block] + blind,
        out_specs=(block, block, block, pl.BlockSpec((ADAM_ROWS // 4, 4, LANES), lambda i: (i, 0, 0)),
                   pl.BlockSpec(memory_space=pltpu.SMEM)),
        input_output_aliases={7 + k: k for k in range(len(before))},
        compiler_params=pltpu.CompilerParams(vmem_limit_bytes=VMEM_LIMIT),
        cost_estimate=pl.CostEstimate(flops=30 * part_rows * LANES * 40, bytes_accessed=20 * part_rows * LANES, transcendentals=0),
    )(lr, norm, stay(g), stay(w), stay(m), v, mask, *before)


def store_kernel(spots, *refs):
    count = len(spots)
    pieces = refs[:count]
    params, buf, in_sem, out_sem = refs[-4:]
    me, part, along_x, along_y = places()
    diag = along_x + along_y - me
    shift = part - me
    blocks = (me, along_x, along_y, diag, me + shift, along_x + shift, along_y + shift, diag + shift)
    loads, stores = [], []
    for k, (which, start, size, grains) in enumerate(spots):
        dst = params.at[pl.ds(blocks[which] * grains + start, size)]
        loads.append(pltpu.make_async_copy(pieces[k].at[pl.ds(0, size)], buf.at[k, pl.ds(0, size)], in_sem.at[k]))
        stores.append(pltpu.make_async_copy(buf.at[k, pl.ds(0, size)], dst, out_sem.at[k]))
    for cp in loads:
        cp.start()
    for cp, out in zip(loads, stores):
        cp.wait()
        out.start()
    for out in stores:
        out.wait()


def store(pieces, spots, before, num_dev, grains):
    count = len(pieces)
    hbm = pl.BlockSpec(memory_space=pltpu.HBM)
    size = pieces[0].shape[0]
    moved = sum(p.size for p in pieces)
    return pl.pallas_call(
        functools.partial(store_kernel, [(which, start, min(size, grains - start), grains) for which, start in spots]),
        out_shape=jax.ShapeDtypeStruct((num_dev * grains, 4, LANES), jnp.bfloat16),
        in_specs=[hbm] * (count + len(before)),
        out_specs=hbm,
        input_output_aliases={count: 0} if before else {},
        scratch_shapes=[pltpu.VMEM((count,) + pieces[0].shape, jnp.bfloat16),
                        pltpu.SemaphoreType.DMA((count,)), pltpu.SemaphoreType.DMA((count,))],
        compiler_params=pltpu.CompilerParams(vmem_limit_bytes=VMEM_LIMIT),
        cost_estimate=pl.CostEstimate(flops=40 * moved, bytes_accessed=4 * moved, transcendentals=0),
    )(*pieces, *before)


def solution(mesh):
    num_dev = mesh.shape["dp"]
    hop = {"core": [(i, i ^ 1) for i in range(num_dev)], "x": [(i, i ^ 2) for i in range(num_dev)],
           "y": [(i, i ^ 4) for i in range(num_dev)]}

    def local_step(grad_row, master, mom_first, mom_second, decay_mask, learn_rate):
        shard_len = master.shape[0]
        rows = shard_len // LANES
        grains = rows // 4
        flat = lambda a: a.reshape(rows, LANES)
        send = lambda a, along: lax.ppermute(a, "dp", hop[along])
        g, w, m, norm = reduce_scatter(grad_row, flat(master), flat(mom_first), rows, num_dev)
        state = ()
        whole = ()
        arrived = []
        for p in range(PARTS):
            *state, packed, grad_norm = adamw(p, learn_rate, norm, g, w, m, flat(mom_second), flat(decay_mask), state)
            arrived.append((packed, send(packed, "x"), send(packed, "y")))
        for p, (packed, from_x, from_y) in enumerate(arrived):
            start = p * packed.shape[0]
            pieces = [packed, from_x, from_y]
            pieces = pieces + [send(a, "core") for a in pieces]
            whole = (store(pieces, [(k, start) for k in (0, 1, 2, 4, 5, 6)], whole, num_dev, grains),)
        for p, (packed, from_x, from_y) in enumerate(arrived):
            start = p * packed.shape[0]
            far = send(from_x, "y") if p % 2 == 0 else send(from_y, "x")
            whole = (store([far, send(far, "core")], [(3, start), (7, start)], whole, num_dev, grains),)
        new_w, new_m, new_v = state
        params = whole[0].reshape(num_dev * shard_len)
        return (params, new_w.reshape(shard_len), new_m.reshape(shard_len), new_v.reshape(shard_len),
                grad_norm)

    return jax.shard_map(
        local_step, mesh=mesh,
        in_specs=(P("dp", None), P("dp"), P("dp"), P("dp"), P("dp"), P()),
        out_specs=(P(), P("dp"), P("dp"), P("dp"), P()), check_vma=False)
```

```python
import functools

import jax
import jax.numpy as jnp
from jax import lax
from jax.experimental import pallas as pl
from jax.experimental.pallas import tpu as pltpu
from jax.sharding import PartitionSpec as P


BETA_FIRST = 0.9
BETA_SECOND = 0.95
ADAM_EPS = 1e-8
CLIP_EPS = 1e-6
WEIGHT_DECAY = 0.1
ADAM_STEP = 10

MESH = pl.DeviceIdType.MESH
LANES = 128
CHUNK_ROWS = 384
HALF_ROWS = CHUNK_ROWS // 2
SLOTS = 4
VMEM_LIMIT = 20 << 20
PARTS = 8
ADAM_ROWS = 1560
TILE_ROWS = 120


def places():
    me = lax.axis_index("dp")
    core = me % 2
    part = me + 1 - 2 * core
    along_x = me + 2 - 4 * ((me // 2) % 2)
    along_y = me + 4 - 8 * (me // 4)
    return me, part, along_x, along_y


def meet(peers):
    barrier = pltpu.get_barrier_semaphore()
    for peer in peers:
        pl.semaphore_signal(barrier, inc=1, device_id=(peer,), device_id_type=MESH)
    pl.semaphore_wait(barrier, len(peers))


def stay(array):
    return pltpu.with_memory_space_constraint(array, pltpu.VMEM)


def remote(src, dst, send_sem, recv_sem, device):
    return pltpu.make_async_remote_copy(
        src_ref=src, dst_ref=dst, send_sem=send_sem, recv_sem=recv_sem,
        device_id=(device,), device_id_type=MESH)


def reduce_kernel(shard_rows, grad, w, m, g_out, w_out, m_out, norm_out,
                  own, other, x_send, y_send, x_keep, y_keep, mine, x_recv, y_recv,
                  x_fin, y_fin, x_last, y_last, acc, norm_recv,
                  own_sem, part_ssem, part_rsem, x_ssem, x_rsem, y_ssem, y_rsem,
                  xf_ssem, xf_rsem, yf_ssem, yf_rsem, n_ssem, n_rsem, w_sem, m_sem):
    me, part, along_x, along_y = places()
    diag = along_x + along_y - me
    shift = part - me
    blocks = (me, along_x, along_y, diag)
    shard_len = shard_rows * LANES
    full = CHUNK_ROWS * LANES
    chunks = -(-shard_rows // CHUNK_ROWS)
    tail_rows = shard_rows - (chunks - 1) * CHUNK_ROWS
    tail = tail_rows * LANES

    num_dev = grad.shape[1] // shard_len
    others = [(me + k) % num_dev for k in range(1, num_dev)]
    fetches = (pltpu.make_async_copy(w, w_out.at[pl.ds(0, shard_rows)], w_sem),
               pltpu.make_async_copy(m, m_out.at[pl.ds(0, shard_rows)], m_sem))

    meet(others)
    acc[...] = jnp.zeros_like(acc)

    def loads(i, size):
        slot = i % SLOTS
        out = []
        for b, block in enumerate(blocks):
            src = pl.multiple_of(block * shard_len + i * full, LANES)
            out.append(pltpu.make_async_copy(
                grad.at[:, pl.ds(src, size)], own.at[slot, b, :, pl.ds(0, size)], own_sem.at[slot, b]))
        return out

    def swaps(i, size):
        slot = i % SLOTS
        out = []
        for b, block in enumerate(blocks):
            src = pl.multiple_of((block + shift) * shard_len + i * full, LANES)
            out.append(remote(
                grad.at[:, pl.ds(src, size)], other.at[slot, b, :, pl.ds(0, size)],
                part_ssem.at[slot, b], part_rsem.at[slot, b], part))
        return out

    def first_hops(j):
        slot = j % SLOTS
        return (remote(x_send.at[slot], x_recv.at[slot], x_ssem.at[slot], x_rsem.at[slot], along_x),
                remote(y_send.at[slot], y_recv.at[slot], y_ssem.at[slot], y_rsem.at[slot], along_y))

    def last_hops(j):
        slot = j % SLOTS
        return (remote(x_fin.at[slot], x_last.at[slot], xf_ssem.at[slot], xf_rsem.at[slot], along_x),
                remote(y_fin.at[slot], y_last.at[slot], yf_ssem.at[slot], yf_rsem.at[slot], along_y))

    def for_size(i, do):
        @pl.when(i < chunks - 1)
        def _():
            do(full)

        @pl.when(i == chunks - 1)
        def _():
            do(tail)

    def begin(i):
        def do(size):
            for cp in loads(i, size) + swaps(i, size):
                cp.start()

        for_size(i, do)

    def pair_sums(j):
        def do(size):
            for cp in loads(j, size) + swaps(j, size):
                cp.wait()

        for_size(j, do)
        slot = j % SLOTS

        def tile(t, carry):
            for half in range(2):
                row = pl.multiple_of(t * 8, 8)
                col = pl.multiple_of((t + half * (HALF_ROWS // 8)) * 8 * LANES, 8 * LANES)

                def pair(b):
                    a = own[slot, b, :, pl.ds(col, 8 * LANES)].astype(jnp.float32)
                    o = other[slot, b, :, pl.ds(col, 8 * LANES)].astype(jnp.float32)
                    return (a + o).reshape(8, LANES)

                mine[slot, half, pl.ds(row, 8)] = pair(0)
                if half == 0:
                    x_send[slot, 0, pl.ds(row, 8)] = pair(1)
                    y_keep[slot, pl.ds(row, 8)] = pair(2)
                    x_send[slot, 1, pl.ds(row, 8)] = pair(3)
                else:
                    x_keep[slot, pl.ds(row, 8)] = pair(1)
                    y_send[slot, 0, pl.ds(row, 8)] = pair(2)
                    y_send[slot, 1, pl.ds(row, 8)] = pair(3)
            return carry

        lax.fori_loop(0, HALF_ROWS // 8, tile, 0)
        for cp in first_hops(j):
            cp.start()

    def relay(j):
        for cp in first_hops(j):
            cp.wait()
        slot = j % SLOTS
        x_fin[slot] = x_keep[slot] + y_recv[slot, 1]
        y_fin[slot] = y_keep[slot] + x_recv[slot, 1]
        for cp in last_hops(j):
            cp.start()
        mine[slot, 0] = mine[slot, 0] + x_recv[slot, 0]
        mine[slot, 1] = mine[slot, 1] + y_recv[slot, 0]

    def finish(j):
        for cp in last_hops(j):
            cp.wait()
        slot = j % SLOTS
        base = j * CHUNK_ROWS
        left = shard_rows - j * CHUNK_ROWS
        rows = lax.broadcasted_iota(jnp.int32, (8, LANES), 0)

        def tile(t, total):
            row = pl.multiple_of(t * 8, 8)
            top = (mine[slot, 0, pl.ds(row, 8)] + y_last[slot, pl.ds(row, 8)]) * 0.125
            low = (mine[slot, 1, pl.ds(row, 8)] + x_last[slot, pl.ds(row, 8)]) * 0.125
            g_out[pl.ds(pl.multiple_of(base + t * 8, 8), 8)] = top
            g_out[pl.ds(pl.multiple_of(base + HALF_ROWS + t * 8, 8), 8)] = low
            total = total + jnp.where(rows + t * 8 < left, top * top, 0.0)
            return total + jnp.where(rows + (HALF_ROWS + t * 8) < left, low * low, 0.0)

        acc[...] += lax.fori_loop(0, HALF_ROWS // 8, tile, jnp.zeros((8, LANES), jnp.float32))

    def step(i, carry):
        @pl.when(i < chunks)
        def _():
            begin(i)

        @pl.when((i >= 1) & (i < chunks + 1))
        def _():
            pair_sums(i - 1)

        @pl.when((i >= 2) & (i < chunks + 2))
        def _():
            relay(i - 2)

        @pl.when(i == 4)
        def _():
            for cp in fetches:
                cp.start()

        @pl.when(i >= 4)
        def _():
            finish(i - 4)

        return carry

    lax.fori_loop(0, chunks + 4, step, 0)
    norm_recv[me] = acc[...]

    def shares(peer, k):
        return remote(acc, norm_recv.at[me], n_ssem.at[k], n_rsem.at[me], peer)

    for k, peer in enumerate(others):
        shares(peer, k).start()
    for k, peer in enumerate(others):
        shares(peer, k).wait_send()
        remote(acc, norm_recv.at[peer], n_ssem.at[k], n_rsem.at[peer], peer).wait_recv()
    total = norm_recv[0]
    for k in range(1, num_dev):
        total = total + norm_recv[k]
    for cp in fetches:
        cp.wait()
    norm_out[...] = jnp.broadcast_to(jnp.sqrt(jnp.sum(total, keepdims=True)), norm_out.shape)


def reduce_scatter(grad_row, w, m, shard_rows, num_dev):
    f32, bf16 = jnp.float32, jnp.bfloat16
    chunks = -(-shard_rows // CHUNK_ROWS)
    vm, dma = pltpu.VMEM, pltpu.SemaphoreType.DMA
    pair = (SLOTS, 2, HALF_ROWS, LANES)
    one = (SLOTS, HALF_ROWS, LANES)
    raw = (SLOTS, 4, 1, CHUNK_ROWS * LANES)
    state = vm((chunks * CHUNK_ROWS, LANES), f32)
    return pl.pallas_call(
        functools.partial(reduce_kernel, shard_rows),
        out_shape=(state, state, state, jax.ShapeDtypeStruct((8, LANES), f32)),
        in_specs=[pl.BlockSpec(memory_space=pltpu.HBM)] * 3,
        out_specs=(pl.BlockSpec(memory_space=vm),) * 4,
        scratch_shapes=[
            vm(raw, bf16), vm(raw, bf16), vm(pair, f32), vm(pair, f32), vm(one, f32), vm(one, f32),
            vm(pair, f32), vm(pair, f32), vm(pair, f32), vm(one, f32), vm(one, f32), vm(one, f32),
            vm(one, f32), vm((8, LANES), f32),
            vm((num_dev, 8, LANES), f32),
            dma((SLOTS, 4)), dma((SLOTS, 4)), dma((SLOTS, 4)),
            dma((SLOTS,)), dma((SLOTS,)), dma((SLOTS,)), dma((SLOTS,)),
            dma((SLOTS,)), dma((SLOTS,)), dma((SLOTS,)), dma((SLOTS,)),
            dma((num_dev - 1,)), dma((num_dev,)), dma, dma],
        compiler_params=pltpu.CompilerParams(collective_id=0, has_side_effects=True,
                                             vmem_limit_bytes=VMEM_LIMIT),
    )(grad_row, w, m)


def adamw_kernel(lr, norm, g, w, m, v, mask, *rest):
    w_out, m_out, v_out, packed, norm_out = rest[-5:]
    norm_out[0] = norm[0, 0]
    coef = jnp.minimum(1.0, 1.0 / (norm[0:1] + CLIP_EPS))
    rate = lr[0]

    def tile(t, carry):
        at = pl.ds(pl.multiple_of(t * TILE_ROWS, 8), TILE_ROWS)
        h = g[at] * coef
        first = BETA_FIRST * m[at] + (1.0 - BETA_FIRST) * h
        second = BETA_SECOND * v[at] + (1.0 - BETA_SECOND) * h * h
        step_dir = (first * (1.0 / (1.0 - BETA_FIRST ** ADAM_STEP))) / (
            jnp.sqrt(second * (1.0 / (1.0 - BETA_SECOND ** ADAM_STEP))) + ADAM_EPS)
        old = w[at]
        new = old - rate * (step_dir + WEIGHT_DECAY * mask[at].astype(jnp.float32) * old)
        w_out[at] = new
        m_out[at] = first
        v_out[at] = second
        grains = TILE_ROWS // 4
        packed[pl.ds(pl.multiple_of(t * grains, 2), grains)] = new.reshape(grains, 4, LANES).astype(packed.dtype)
        return carry

    lax.fori_loop(0, ADAM_ROWS // TILE_ROWS, tile, 0)


def adamw(part, lr, norm, g, w, m, v, mask, before):
    rows = v.shape[0]
    part_rows = g.shape[0] // PARTS
    steps = part_rows // ADAM_ROWS
    block = pl.BlockSpec((ADAM_ROWS, LANES), lambda i: (i + part * steps, 0))
    state = jax.ShapeDtypeStruct((rows, LANES), jnp.float32)
    blind = [pl.BlockSpec(memory_space=pl.ANY)] * len(before)
    return pl.pallas_call(
        adamw_kernel,
        grid=(steps,),
        out_shape=(state, state, state, jax.ShapeDtypeStruct((part_rows // 4, 4, LANES), jnp.bfloat16),
                   jax.ShapeDtypeStruct((1,), jnp.float32)),
        in_specs=[pl.BlockSpec(memory_space=pltpu.SMEM),
                  pl.BlockSpec((8, LANES), lambda i: (0, 0)),
                  block, block, block, block, block] + blind,
        out_specs=(block, block, block, pl.BlockSpec((ADAM_ROWS // 4, 4, LANES), lambda i: (i, 0, 0)),
                   pl.BlockSpec(memory_space=pltpu.SMEM)),
        input_output_aliases={7 + k: k for k in range(len(before))},
        compiler_params=pltpu.CompilerParams(vmem_limit_bytes=VMEM_LIMIT),
        cost_estimate=pl.CostEstimate(flops=30 * part_rows * LANES * 40, bytes_accessed=20 * part_rows * LANES, transcendentals=0),
    )(lr, norm, stay(g), stay(w), stay(m), v, mask, *before)


def store_kernel(spots, *refs):
    count = len(spots)
    pieces = refs[:count]
    params, buf, in_sem, out_sem = refs[-4:]
    me, part, along_x, along_y = places()
    diag = along_x + along_y - me
    shift = part - me
    blocks = (me, along_x, along_y, diag, me + shift, along_x + shift, along_y + shift, diag + shift)
    loads, stores = [], []
    for k, (which, start, size, grains) in enumerate(spots):
        dst = params.at[pl.ds(blocks[which] * grains + start, size)]
        loads.append(pltpu.make_async_copy(pieces[k].at[pl.ds(0, size)], buf.at[k, pl.ds(0, size)], in_sem.at[k]))
        stores.append(pltpu.make_async_copy(buf.at[k, pl.ds(0, size)], dst, out_sem.at[k]))
    for cp in loads:
        cp.start()
    for cp, out in zip(loads, stores):
        cp.wait()
        out.start()
    for out in stores:
        out.wait()


def store(pieces, spots, before, num_dev, grains):
    count = len(pieces)
    hbm = pl.BlockSpec(memory_space=pltpu.HBM)
    size = pieces[0].shape[0]
    moved = sum(p.size for p in pieces)
    return pl.pallas_call(
        functools.partial(store_kernel, [(which, start, min(size, grains - start), grains) for which, start in spots]),
        out_shape=jax.ShapeDtypeStruct((num_dev * grains, 4, LANES), jnp.bfloat16),
        in_specs=[hbm] * (count + len(before)),
        out_specs=hbm,
        input_output_aliases={count: 0} if before else {},
        scratch_shapes=[pltpu.VMEM((count,) + pieces[0].shape, jnp.bfloat16),
                        pltpu.SemaphoreType.DMA((count,)), pltpu.SemaphoreType.DMA((count,))],
        compiler_params=pltpu.CompilerParams(vmem_limit_bytes=VMEM_LIMIT),
        cost_estimate=pl.CostEstimate(flops=40 * moved, bytes_accessed=4 * moved, transcendentals=0),
    )(*pieces, *before)


def solution(mesh):
    num_dev = mesh.shape["dp"]
    hop = {"core": [(i, i ^ 1) for i in range(num_dev)], "x": [(i, i ^ 2) for i in range(num_dev)],
           "y": [(i, i ^ 4) for i in range(num_dev)]}

    def local_step(grad_row, master, mom_first, mom_second, decay_mask, learn_rate):
        shard_len = master.shape[0]
        rows = shard_len // LANES
        grains = rows // 4
        flat = lambda a: a.reshape(rows, LANES)

        def send(a, along):
            return lax.ppermute(a, "dp", hop[along])

        def put(pieces, spots, whole):
            return (store(pieces, spots, whole, num_dev, grains),)

        g, w, m, norm = reduce_scatter(grad_row, flat(master), flat(mom_first), rows, num_dev)
        state = ()
        whole = ()
        arrived = []
        for p in range(PARTS):
            *state, packed, grad_norm = adamw(
                p, learn_rate, norm, g, w, m, flat(mom_second), flat(decay_mask), state)
            arrived.append((packed, send(packed, "x"), send(packed, "y"),
                            send(packed, "core")))
        size = packed.shape[0]
        far = []
        for p, (packed, from_x, from_y, from_core) in enumerate(arrived):
            far.append(send(from_x, "y") if p % 2 == 0 else send(from_y, "x"))
            pieces = [packed, from_x, from_y, from_core, send(from_x, "core"), send(from_y, "core")]
            whole = put(pieces, [(k, p * size) for k in (0, 1, 2, 4, 5, 6)], whole)
        for p in range(0, PARTS, 2):
            pieces, spots = [], []
            for q in (p, p + 1):
                pieces += [far[q], send(far[q], "core")]
                spots += [(3, q * size), (7, q * size)]
            whole = put(pieces, spots, whole)
        new_w, new_m, new_v = state
        params = whole[0].reshape(num_dev * shard_len)
        return (params, new_w.reshape(shard_len), new_m.reshape(shard_len), new_v.reshape(shard_len),
                grad_norm)

    return jax.shard_map(
        local_step, mesh=mesh,
        in_specs=(P("dp", None), P("dp"), P("dp"), P("dp"), P("dp"), P()),
        out_specs=(P(), P("dp"), P("dp"), P("dp"), P()), check_vma=False)
```

```python
import functools

import jax
import jax.numpy as jnp
from jax import lax
from jax.experimental import pallas as pl
from jax.experimental.pallas import tpu as pltpu
from jax.sharding import PartitionSpec as P


BETA_FIRST = 0.9
BETA_SECOND = 0.95
ADAM_EPS = 1e-8
CLIP_EPS = 1e-6
WEIGHT_DECAY = 0.1
ADAM_STEP = 10

MESH = pl.DeviceIdType.MESH
LANES = 128
CHUNK_ROWS = 240
HALF_ROWS = CHUNK_ROWS // 2
SLOTS = 4
VMEM_LIMIT = 20 << 20
ADAM_ROWS = 960
PARTS = (1, 2, 4, 4, 4, 4, 3, 2, 1, 1)
TILE_ROWS = 120


def places():
    me = lax.axis_index("dp")
    core = me % 2
    part = me + 1 - 2 * core
    along_x = me + 2 - 4 * ((me // 2) % 2)
    along_y = me + 4 - 8 * (me // 4)
    return me, part, along_x, along_y


def meet(peers):
    barrier = pltpu.get_barrier_semaphore()
    for peer in peers:
        pl.semaphore_signal(barrier, inc=1, device_id=(peer,), device_id_type=MESH)
    pl.semaphore_wait(barrier, len(peers))


def stay(array):
    return pltpu.with_memory_space_constraint(array, pltpu.VMEM)


def remote(src, dst, send_sem, recv_sem, device):
    return pltpu.make_async_remote_copy(
        src_ref=src, dst_ref=dst, send_sem=send_sem, recv_sem=recv_sem,
        device_id=(device,), device_id_type=MESH)


def reduce_kernel(shard_rows, grad, w, m, g_out, w_out, m_out, norm_out,
                  own, other, x_send, y_send, x_keep, y_keep, mine, x_recv, y_recv,
                  x_fin, y_fin, x_last, y_last, acc, norm_recv,
                  own_sem, part_ssem, part_rsem, x_ssem, x_rsem, y_ssem, y_rsem,
                  xf_ssem, xf_rsem, yf_ssem, yf_rsem, n_ssem, n_rsem, w_sem, m_sem):
    me, part, along_x, along_y = places()
    diag = along_x + along_y - me
    shift = part - me
    blocks = (me, along_x, along_y, diag)
    shard_len = shard_rows * LANES
    full = CHUNK_ROWS * LANES
    chunks = -(-shard_rows // CHUNK_ROWS)
    tail_rows = shard_rows - (chunks - 1) * CHUNK_ROWS
    tail = tail_rows * LANES

    num_dev = grad.shape[1] // shard_len
    others = [(me + k) % num_dev for k in range(1, num_dev)]
    fetches = (pltpu.make_async_copy(w, w_out.at[pl.ds(0, shard_rows)], w_sem),
               pltpu.make_async_copy(m, m_out.at[pl.ds(0, shard_rows)], m_sem))

    acc[...] = jnp.zeros_like(acc)

    def loads(i, size):
        slot = i % SLOTS
        out = []
        for b, block in enumerate(blocks):
            src = pl.multiple_of(block * shard_len + i * full, LANES)
            out.append(pltpu.make_async_copy(
                grad.at[:, pl.ds(src, size)], own.at[slot, b, :, pl.ds(0, size)], own_sem.at[slot, b]))
        return out

    def swaps(i, size):
        slot = i % SLOTS
        out = []
        for b, block in enumerate(blocks):
            src = pl.multiple_of((block + shift) * shard_len + i * full, LANES)
            out.append(remote(
                grad.at[:, pl.ds(src, size)], other.at[slot, b, :, pl.ds(0, size)],
                part_ssem.at[slot, b], part_rsem.at[slot, b], part))
        return out

    def first_hops(j):
        slot = j % SLOTS
        return (remote(x_send.at[slot], x_recv.at[slot], x_ssem.at[slot], x_rsem.at[slot], along_x),
                remote(y_send.at[slot], y_recv.at[slot], y_ssem.at[slot], y_rsem.at[slot], along_y))

    def last_hops(j):
        slot = j % SLOTS
        return (remote(x_fin.at[slot], x_last.at[slot], xf_ssem.at[slot], xf_rsem.at[slot], along_x),
                remote(y_fin.at[slot], y_last.at[slot], yf_ssem.at[slot], yf_rsem.at[slot], along_y))

    def for_size(i, do):
        @pl.when(i < chunks - 1)
        def _():
            do(full)

        @pl.when(i == chunks - 1)
        def _():
            do(tail)

    for cp in loads(0, full):
        cp.start()
    meet(others)
    for cp in swaps(0, full):
        cp.start()

    def begin(i):
        def do(size):
            for cp in swaps(i, size) + loads(i, size):
                cp.start()

        for_size(i, do)

    def pair_sums(j):
        def do(size):
            for cp in loads(j, size) + swaps(j, size):
                cp.wait()

        for_size(j, do)
        slot = j % SLOTS

        def tile(t, carry):
            for half in range(2):
                row = pl.multiple_of(t * 8, 8)
                col = pl.multiple_of((t + half * (HALF_ROWS // 8)) * 8 * LANES, 8 * LANES)

                def pair(b):
                    a = own[slot, b, :, pl.ds(col, 8 * LANES)].astype(jnp.float32)
                    o = other[slot, b, :, pl.ds(col, 8 * LANES)].astype(jnp.float32)
                    return (a + o).reshape(8, LANES)

                mine[slot, half, pl.ds(row, 8)] = pair(0)
                if half == 0:
                    x_send[slot, 0, pl.ds(row, 8)] = pair(1)
                    y_keep[slot, pl.ds(row, 8)] = pair(2)
                    x_send[slot, 1, pl.ds(row, 8)] = pair(3)
                else:
                    x_keep[slot, pl.ds(row, 8)] = pair(1)
                    y_send[slot, 0, pl.ds(row, 8)] = pair(2)
                    y_send[slot, 1, pl.ds(row, 8)] = pair(3)
            return carry

        lax.fori_loop(0, HALF_ROWS // 8, tile, 0)
        for cp in first_hops(j):
            cp.start()

    def relay(j):
        for cp in first_hops(j):
            cp.wait()
        slot = j % SLOTS
        x_fin[slot] = x_keep[slot] + y_recv[slot, 1]
        y_fin[slot] = y_keep[slot] + x_recv[slot, 1]
        for cp in last_hops(j):
            cp.start()
        mine[slot, 0] = mine[slot, 0] + x_recv[slot, 0]
        mine[slot, 1] = mine[slot, 1] + y_recv[slot, 0]

    def finish(j):
        for cp in last_hops(j):
            cp.wait()
        slot = j % SLOTS
        base = j * CHUNK_ROWS
        left = shard_rows - j * CHUNK_ROWS
        rows = lax.broadcasted_iota(jnp.int32, (8, LANES), 0)

        def tile(t, total):
            row = pl.multiple_of(t * 8, 8)
            top = (mine[slot, 0, pl.ds(row, 8)] + y_last[slot, pl.ds(row, 8)]) * 0.125
            low = (mine[slot, 1, pl.ds(row, 8)] + x_last[slot, pl.ds(row, 8)]) * 0.125
            g_out[pl.ds(pl.multiple_of(base + t * 8, 8), 8)] = top
            g_out[pl.ds(pl.multiple_of(base + HALF_ROWS + t * 8, 8), 8)] = low
            total = total + jnp.where(rows + t * 8 < left, top * top, 0.0)
            return total + jnp.where(rows + (HALF_ROWS + t * 8) < left, low * low, 0.0)

        acc[...] += lax.fori_loop(0, HALF_ROWS // 8, tile, jnp.zeros((8, LANES), jnp.float32))

    def step(i, carry):
        @pl.when((i >= 1) & (i < chunks))
        def _():
            begin(i)

        @pl.when((i >= 1) & (i < chunks + 1))
        def _():
            pair_sums(i - 1)

        @pl.when((i >= 2) & (i < chunks + 2))
        def _():
            relay(i - 2)

        @pl.when(i == 4)
        def _():
            for cp in fetches:
                cp.start()

        @pl.when(i >= 4)
        def _():
            finish(i - 4)

        return carry

    lax.fori_loop(0, chunks + 4, step, 0)
    norm_recv[me] = acc[...]

    def shares(peer, k):
        return remote(acc, norm_recv.at[me], n_ssem.at[k], n_rsem.at[me], peer)

    for k, peer in enumerate(others):
        shares(peer, k).start()
    for k, peer in enumerate(others):
        shares(peer, k).wait_send()
        remote(acc, norm_recv.at[peer], n_ssem.at[k], n_rsem.at[peer], peer).wait_recv()
    total = norm_recv[0]
    for k in range(1, num_dev):
        total = total + norm_recv[k]
    for cp in fetches:
        cp.wait()
    norm_out[...] = jnp.broadcast_to(jnp.sqrt(jnp.sum(total, keepdims=True)), norm_out.shape)


def reduce_scatter(grad_row, w, m, shard_rows, num_dev):
    f32, bf16 = jnp.float32, jnp.bfloat16
    chunks = -(-shard_rows // CHUNK_ROWS)
    vm, dma = pltpu.VMEM, pltpu.SemaphoreType.DMA
    pair = (SLOTS, 2, HALF_ROWS, LANES)
    one = (SLOTS, HALF_ROWS, LANES)
    raw = (SLOTS, 4, 1, CHUNK_ROWS * LANES)
    state = vm((chunks * CHUNK_ROWS, LANES), f32)
    return pl.pallas_call(
        functools.partial(reduce_kernel, shard_rows),
        out_shape=(state, state, state, jax.ShapeDtypeStruct((8, LANES), f32)),
        in_specs=[pl.BlockSpec(memory_space=pltpu.HBM)] * 3,
        out_specs=(pl.BlockSpec(memory_space=vm),) * 4,
        scratch_shapes=[
            vm(raw, bf16), vm(raw, bf16), vm(pair, f32), vm(pair, f32), vm(one, f32), vm(one, f32),
            vm(pair, f32), vm(pair, f32), vm(pair, f32), vm(one, f32), vm(one, f32), vm(one, f32),
            vm(one, f32), vm((8, LANES), f32),
            vm((num_dev, 8, LANES), f32),
            dma((SLOTS, 4)), dma((SLOTS, 4)), dma((SLOTS, 4)),
            dma((SLOTS,)), dma((SLOTS,)), dma((SLOTS,)), dma((SLOTS,)),
            dma((SLOTS,)), dma((SLOTS,)), dma((SLOTS,)), dma((SLOTS,)),
            dma((num_dev - 1,)), dma((num_dev,)), dma, dma],
        compiler_params=pltpu.CompilerParams(collective_id=0, has_side_effects=True,
                                             vmem_limit_bytes=VMEM_LIMIT),
    )(grad_row, w, m)


def adamw_kernel(lr, norm, g, w, m, v, mask, *rest):
    w_out, m_out, v_out, packed, norm_out = rest[-5:]
    norm_out[0] = norm[0, 0]
    coef = jnp.minimum(1.0, 1.0 / (norm[0:1] + CLIP_EPS))
    rate = lr[0]

    def tile(t, carry):
        at = pl.ds(pl.multiple_of(t * TILE_ROWS, 8), TILE_ROWS)
        h = g[at] * coef
        first = BETA_FIRST * m[at] + (1.0 - BETA_FIRST) * h
        second = BETA_SECOND * v[at] + (1.0 - BETA_SECOND) * h * h
        step_dir = (first * (1.0 / (1.0 - BETA_FIRST ** ADAM_STEP))) / (
            jnp.sqrt(second * (1.0 / (1.0 - BETA_SECOND ** ADAM_STEP))) + ADAM_EPS)
        old = w[at]
        new = old - rate * (step_dir + WEIGHT_DECAY * mask[at].astype(jnp.float32) * old)
        w_out[at] = new
        m_out[at] = first
        v_out[at] = second
        grains = TILE_ROWS // 4
        packed[pl.ds(pl.multiple_of(t * grains, 2), grains)] = new.reshape(grains, 4, LANES).astype(packed.dtype)
        return carry

    lax.fori_loop(0, ADAM_ROWS // TILE_ROWS, tile, 0)


def adamw(first, steps, lr, norm, g, w, m, v, mask, before):
    rows = v.shape[0]
    part_rows = steps * ADAM_ROWS
    block = pl.BlockSpec((ADAM_ROWS, LANES), lambda i: (i + first, 0))
    state = jax.ShapeDtypeStruct((rows, LANES), jnp.float32)
    blind = [pl.BlockSpec(memory_space=pl.ANY)] * len(before)
    return pl.pallas_call(
        adamw_kernel,
        grid=(steps,),
        out_shape=(state, state, state, jax.ShapeDtypeStruct((part_rows // 4, 4, LANES), jnp.bfloat16),
                   jax.ShapeDtypeStruct((1,), jnp.float32)),
        in_specs=[pl.BlockSpec(memory_space=pltpu.SMEM),
                  pl.BlockSpec((8, LANES), lambda i: (0, 0)),
                  block, block, block, block, block] + blind,
        out_specs=(block, block, block, pl.BlockSpec((ADAM_ROWS // 4, 4, LANES), lambda i: (i, 0, 0)),
                   pl.BlockSpec(memory_space=pltpu.SMEM)),
        input_output_aliases={7 + k: k for k in range(len(before))},
        compiler_params=pltpu.CompilerParams(vmem_limit_bytes=VMEM_LIMIT),
        cost_estimate=pl.CostEstimate(flops=30 * part_rows * LANES * 40, bytes_accessed=20 * part_rows * LANES, transcendentals=0),
    )(lr, norm, stay(g), stay(w), stay(m), v, mask, *before)


def store_kernel(spots, *refs):
    count = len(spots)
    pieces = refs[:count]
    params, buf, in_sem, out_sem = refs[-4:]
    me, part, along_x, along_y = places()
    diag = along_x + along_y - me
    shift = part - me
    blocks = (me, along_x, along_y, diag, me + shift, along_x + shift, along_y + shift, diag + shift)
    loads, stores = [], []
    for k, (which, start, size, grains) in enumerate(spots):
        dst = params.at[pl.ds(blocks[which] * grains + start, size)]
        loads.append(pltpu.make_async_copy(pieces[k].at[pl.ds(0, size)], buf.at[k, pl.ds(0, size)], in_sem.at[k]))
        stores.append(pltpu.make_async_copy(buf.at[k, pl.ds(0, size)], dst, out_sem.at[k]))
    for cp in loads:
        cp.start()
    for cp, out in zip(loads, stores):
        cp.wait()
        out.start()
    for out in stores:
        out.wait()


def store(pieces, spots, before, num_dev, grains):
    count = len(pieces)
    hbm = pl.BlockSpec(memory_space=pltpu.HBM)
    room = max(p.shape[0] for p in pieces)
    moved = sum(p.size for p in pieces)
    return pl.pallas_call(
        functools.partial(store_kernel, [(which, start, min(p.shape[0], grains - start), grains)
                                         for p, (which, start) in zip(pieces, spots)]),
        out_shape=jax.ShapeDtypeStruct((num_dev * grains, 4, LANES), jnp.bfloat16),
        in_specs=[hbm] * (count + len(before)),
        out_specs=hbm,
        input_output_aliases={count: 0} if before else {},
        scratch_shapes=[pltpu.VMEM((count, room, 4, LANES), jnp.bfloat16),
                        pltpu.SemaphoreType.DMA((count,)), pltpu.SemaphoreType.DMA((count,))],
        compiler_params=pltpu.CompilerParams(vmem_limit_bytes=VMEM_LIMIT),
        cost_estimate=pl.CostEstimate(flops=40 * moved, bytes_accessed=4 * moved, transcendentals=0),
    )(*pieces, *before)


def solution(mesh):
    num_dev = mesh.shape["dp"]
    hop = {"core": [(i, i ^ 1) for i in range(num_dev)], "x": [(i, i ^ 2) for i in range(num_dev)],
           "y": [(i, i ^ 4) for i in range(num_dev)]}

    def local_step(grad_row, master, mom_first, mom_second, decay_mask, learn_rate):
        shard_len = master.shape[0]
        rows = shard_len // LANES
        grains = rows // 4
        flat = lambda a: a.reshape(rows, LANES)

        def send(a, along):
            return lax.ppermute(a, "dp", hop[along])

        def put(pieces, spots, whole):
            return (store(pieces, spots, whole, num_dev, grains),)

        g, w, m, norm = reduce_scatter(grad_row, flat(master), flat(mom_first), rows, num_dev)
        state = ()
        whole = ()
        arrived = []
        firsts = [sum(PARTS[:p]) for p in range(len(PARTS))]
        for p, steps in enumerate(PARTS):
            *state, packed, grad_norm = adamw(
                firsts[p], steps, learn_rate, norm, g, w, m, flat(mom_second), flat(decay_mask), state)
            arrived.append((packed, send(packed, "x"), send(packed, "y"),
                            send(packed, "core")))
        starts = [first * ADAM_ROWS // 4 for first in firsts]
        far = []
        for p, (packed, from_x, from_y, from_core) in enumerate(arrived):
            far.append(send(from_x, "y") if p % 2 == 0 else send(from_y, "x"))
            pieces = [packed, from_x, from_y, from_core, send(from_x, "core"), send(from_y, "core")]
            whole = put(pieces, [(k, starts[p]) for k in (0, 1, 2, 4, 5, 6)], whole)
        for p in range(0, len(PARTS), 2):
            pieces, spots = [], []
            for q in (p, p + 1):
                pieces += [far[q], send(far[q], "core")]
                spots += [(3, starts[q]), (7, starts[q])]
            whole = put(pieces, spots, whole)
        new_w, new_m, new_v = state
        params = whole[0].reshape(num_dev * shard_len)
        return (params, new_w.reshape(shard_len), new_m.reshape(shard_len), new_v.reshape(shard_len),
                grad_norm)

    return jax.shard_map(
        local_step, mesh=mesh,
        in_specs=(P("dp", None), P("dp"), P("dp"), P("dp"), P("dp"), P()),
        out_specs=(P(), P("dp"), P("dp"), P("dp"), P()), check_vma=False)
```

```python
import functools

import jax
import jax.numpy as jnp
from jax import lax
from jax.experimental import pallas as pl
from jax.experimental.pallas import tpu as pltpu
from jax.sharding import PartitionSpec as P


BETA_FIRST = 0.9
BETA_SECOND = 0.95
ADAM_EPS = 1e-8
CLIP_EPS = 1e-6
WEIGHT_DECAY = 0.1
ADAM_STEP = 10

MESH = pl.DeviceIdType.MESH
LANES = 128
CHUNK_ROWS = 384
HALF_ROWS = CHUNK_ROWS // 2
SLOTS = 4
VMEM_LIMIT = 20 << 20
ADAM_ROWS = 960
PARTS = (1, 2, 4, 4, 4, 4, 3, 2, 1, 1)
TILE_ROWS = 120


def places():
    me = lax.axis_index("dp")
    core = me % 2
    part = me + 1 - 2 * core
    along_x = me + 2 - 4 * ((me // 2) % 2)
    along_y = me + 4 - 8 * (me // 4)
    return me, part, along_x, along_y


def meet(peers):
    barrier = pltpu.get_barrier_semaphore()
    for peer in peers:
        pl.semaphore_signal(barrier, inc=1, device_id=(peer,), device_id_type=MESH)
    pl.semaphore_wait(barrier, len(peers))


def stay(array):
    return pltpu.with_memory_space_constraint(array, pltpu.VMEM)


def remote(src, dst, send_sem, recv_sem, device):
    return pltpu.make_async_remote_copy(
        src_ref=src, dst_ref=dst, send_sem=send_sem, recv_sem=recv_sem,
        device_id=(device,), device_id_type=MESH)


def reduce_kernel(shard_rows, grad, w, m, g_out, w_out, m_out, norm_out,
                  own, other, x_send, y_send, x_keep, y_keep, mine, x_recv, y_recv,
                  x_fin, y_fin, x_last, y_last, acc, norm_recv,
                  own_sem, part_ssem, part_rsem, x_ssem, x_rsem, y_ssem, y_rsem,
                  xf_ssem, xf_rsem, yf_ssem, yf_rsem, n_ssem, n_rsem, w_sem, m_sem):
    me, part, along_x, along_y = places()
    diag = along_x + along_y - me
    shift = part - me
    blocks = (me, along_x, along_y, diag)
    shard_len = shard_rows * LANES
    full = CHUNK_ROWS * LANES
    chunks = -(-shard_rows // CHUNK_ROWS)
    tail_rows = shard_rows - (chunks - 1) * CHUNK_ROWS
    tail = tail_rows * LANES

    num_dev = grad.shape[1] // shard_len
    others = [(me + k) % num_dev for k in range(1, num_dev)]
    fetches = (pltpu.make_async_copy(w, w_out.at[pl.ds(0, shard_rows)], w_sem),
               pltpu.make_async_copy(m, m_out.at[pl.ds(0, shard_rows)], m_sem))

    acc[...] = jnp.zeros_like(acc)

    def loads(i, size):
        slot = i % SLOTS
        out = []
        for b, block in enumerate(blocks):
            src = pl.multiple_of(block * shard_len + i * full, LANES)
            out.append(pltpu.make_async_copy(
                grad.at[:, pl.ds(src, size)], own.at[slot, b, :, pl.ds(0, size)], own_sem.at[slot, b]))
        return out

    def swaps(i, size):
        slot = i % SLOTS
        out = []
        for b, block in enumerate(blocks):
            src = pl.multiple_of((block + shift) * shard_len + i * full, LANES)
            out.append(remote(
                grad.at[:, pl.ds(src, size)], other.at[slot, b, :, pl.ds(0, size)],
                part_ssem.at[slot, b], part_rsem.at[slot, b], part))
        return out

    def first_hops(j):
        slot = j % SLOTS
        return (remote(x_send.at[slot], x_recv.at[slot], x_ssem.at[slot], x_rsem.at[slot], along_x),
                remote(y_send.at[slot], y_recv.at[slot], y_ssem.at[slot], y_rsem.at[slot], along_y))

    def last_hops(j):
        slot = j % SLOTS
        return (remote(x_fin.at[slot], x_last.at[slot], xf_ssem.at[slot], xf_rsem.at[slot], along_x),
                remote(y_fin.at[slot], y_last.at[slot], yf_ssem.at[slot], yf_rsem.at[slot], along_y))

    def for_size(i, do):
        @pl.when(i < chunks - 1)
        def _():
            do(full)

        @pl.when(i == chunks - 1)
        def _():
            do(tail)

    for cp in loads(0, full):
        cp.start()
    meet(others)
    for cp in swaps(0, full):
        cp.start()

    def begin(i):
        def do(size):
            for cp in swaps(i, size) + loads(i, size):
                cp.start()

        for_size(i, do)

    def pair_sums(j):
        def do(size):
            for cp in loads(j, size) + swaps(j, size):
                cp.wait()

        for_size(j, do)
        slot = j % SLOTS

        def tile(t, carry):
            for half in range(2):
                row = pl.multiple_of(t * 8, 8)
                col = pl.multiple_of((t + half * (HALF_ROWS // 8)) * 8 * LANES, 8 * LANES)

                def pair(b):
                    a = own[slot, b, :, pl.ds(col, 8 * LANES)].astype(jnp.float32)
                    o = other[slot, b, :, pl.ds(col, 8 * LANES)].astype(jnp.float32)
                    return (a + o).reshape(8, LANES)

                mine[slot, half, pl.ds(row, 8)] = pair(0)
                if half == 0:
                    x_send[slot, 0, pl.ds(row, 8)] = pair(1)
                    y_keep[slot, pl.ds(row, 8)] = pair(2)
                    x_send[slot, 1, pl.ds(row, 8)] = pair(3)
                else:
                    x_keep[slot, pl.ds(row, 8)] = pair(1)
                    y_send[slot, 0, pl.ds(row, 8)] = pair(2)
                    y_send[slot, 1, pl.ds(row, 8)] = pair(3)
            return carry

        lax.fori_loop(0, HALF_ROWS // 8, tile, 0)
        for cp in first_hops(j):
            cp.start()

    def relay(j):
        for cp in first_hops(j):
            cp.wait()
        slot = j % SLOTS
        x_fin[slot] = x_keep[slot] + y_recv[slot, 1]
        y_fin[slot] = y_keep[slot] + x_recv[slot, 1]
        for cp in last_hops(j):
            cp.start()
        mine[slot, 0] = mine[slot, 0] + x_recv[slot, 0]
        mine[slot, 1] = mine[slot, 1] + y_recv[slot, 0]

    def finish(j):
        for cp in last_hops(j):
            cp.wait()
        slot = j % SLOTS
        base = j * CHUNK_ROWS
        left = shard_rows - j * CHUNK_ROWS
        rows = lax.broadcasted_iota(jnp.int32, (8, LANES), 0)

        def tile(t, total):
            row = pl.multiple_of(t * 8, 8)
            top = (mine[slot, 0, pl.ds(row, 8)] + y_last[slot, pl.ds(row, 8)]) * 0.125
            low = (mine[slot, 1, pl.ds(row, 8)] + x_last[slot, pl.ds(row, 8)]) * 0.125
            g_out[pl.ds(pl.multiple_of(base + t * 8, 8), 8)] = top
            g_out[pl.ds(pl.multiple_of(base + HALF_ROWS + t * 8, 8), 8)] = low
            total = total + jnp.where(rows + t * 8 < left, top * top, 0.0)
            return total + jnp.where(rows + (HALF_ROWS + t * 8) < left, low * low, 0.0)

        acc[...] += lax.fori_loop(0, HALF_ROWS // 8, tile, jnp.zeros((8, LANES), jnp.float32))

    def step(i, carry):
        @pl.when((i >= 1) & (i < chunks))
        def _():
            begin(i)

        @pl.when((i >= 1) & (i < chunks + 1))
        def _():
            pair_sums(i - 1)

        @pl.when((i >= 2) & (i < chunks + 2))
        def _():
            relay(i - 2)

        @pl.when(i == 4)
        def _():
            for cp in fetches:
                cp.start()

        @pl.when(i >= 4)
        def _():
            finish(i - 4)

        return carry

    lax.fori_loop(0, chunks + 4, step, 0)
    norm_recv[me] = acc[...]

    def shares(peer, k):
        return remote(acc, norm_recv.at[me], n_ssem.at[k], n_rsem.at[me], peer)

    for k, peer in enumerate(others):
        shares(peer, k).start()
    for k, peer in enumerate(others):
        shares(peer, k).wait_send()
        remote(acc, norm_recv.at[peer], n_ssem.at[k], n_rsem.at[peer], peer).wait_recv()
    total = norm_recv[0]
    for k in range(1, num_dev):
        total = total + norm_recv[k]
    for cp in fetches:
        cp.wait()
    norm_out[...] = jnp.broadcast_to(jnp.sqrt(jnp.sum(total, keepdims=True)), norm_out.shape)


def reduce_scatter(grad_row, w, m, shard_rows, num_dev):
    f32, bf16 = jnp.float32, jnp.bfloat16
    chunks = -(-shard_rows // CHUNK_ROWS)
    vm, dma = pltpu.VMEM, pltpu.SemaphoreType.DMA
    pair = (SLOTS, 2, HALF_ROWS, LANES)
    one = (SLOTS, HALF_ROWS, LANES)
    raw = (SLOTS, 4, 1, CHUNK_ROWS * LANES)
    state = vm((chunks * CHUNK_ROWS, LANES), f32)
    return pl.pallas_call(
        functools.partial(reduce_kernel, shard_rows),
        out_shape=(state, state, state, jax.ShapeDtypeStruct((8, LANES), f32)),
        in_specs=[pl.BlockSpec(memory_space=pltpu.HBM)] * 3,
        out_specs=(pl.BlockSpec(memory_space=vm),) * 4,
        scratch_shapes=[
            vm(raw, bf16), vm(raw, bf16), vm(pair, f32), vm(pair, f32), vm(one, f32), vm(one, f32),
            vm(pair, f32), vm(pair, f32), vm(pair, f32), vm(one, f32), vm(one, f32), vm(one, f32),
            vm(one, f32), vm((8, LANES), f32),
            vm((num_dev, 8, LANES), f32),
            dma((SLOTS, 4)), dma((SLOTS, 4)), dma((SLOTS, 4)),
            dma((SLOTS,)), dma((SLOTS,)), dma((SLOTS,)), dma((SLOTS,)),
            dma((SLOTS,)), dma((SLOTS,)), dma((SLOTS,)), dma((SLOTS,)),
            dma((num_dev - 1,)), dma((num_dev,)), dma, dma],
        compiler_params=pltpu.CompilerParams(collective_id=0, has_side_effects=True,
                                             vmem_limit_bytes=VMEM_LIMIT),
    )(grad_row, w, m)


def adamw_kernel(lr, norm, g, w, m, v, mask, *rest):
    w_out, m_out, v_out, packed, norm_out = rest[-5:]
    norm_out[0] = norm[0, 0]
    coef = jnp.minimum(1.0, 1.0 / (norm[0:1] + CLIP_EPS))
    rate = lr[0]

    def tile(t, carry):
        at = pl.ds(pl.multiple_of(t * TILE_ROWS, 8), TILE_ROWS)
        h = g[at] * coef
        first = BETA_FIRST * m[at] + (1.0 - BETA_FIRST) * h
        second = BETA_SECOND * v[at] + (1.0 - BETA_SECOND) * h * h
        step_dir = (first * (1.0 / (1.0 - BETA_FIRST ** ADAM_STEP))) / (
            jnp.sqrt(second * (1.0 / (1.0 - BETA_SECOND ** ADAM_STEP))) + ADAM_EPS)
        old = w[at]
        new = old - rate * (step_dir + WEIGHT_DECAY * mask[at].astype(jnp.float32) * old)
        w_out[at] = new
        m_out[at] = first
        v_out[at] = second
        grains = TILE_ROWS // 4
        packed[pl.ds(pl.multiple_of(t * grains, 2), grains)] = new.reshape(grains, 4, LANES).astype(packed.dtype)
        return carry

    lax.fori_loop(0, ADAM_ROWS // TILE_ROWS, tile, 0)


def adamw(first, steps, lr, norm, g, w, m, v, mask, before):
    rows = v.shape[0]
    part_rows = steps * ADAM_ROWS
    block = pl.BlockSpec((ADAM_ROWS, LANES), lambda i: (i + first, 0))
    state = jax.ShapeDtypeStruct((rows, LANES), jnp.float32)
    blind = [pl.BlockSpec(memory_space=pl.ANY)] * len(before)
    return pl.pallas_call(
        adamw_kernel,
        grid=(steps,),
        out_shape=(state, state, state, jax.ShapeDtypeStruct((part_rows // 4, 4, LANES), jnp.bfloat16),
                   jax.ShapeDtypeStruct((1,), jnp.float32)),
        in_specs=[pl.BlockSpec(memory_space=pltpu.SMEM),
                  pl.BlockSpec((8, LANES), lambda i: (0, 0)),
                  block, block, block, block, block] + blind,
        out_specs=(block, block, block, pl.BlockSpec((ADAM_ROWS // 4, 4, LANES), lambda i: (i, 0, 0)),
                   pl.BlockSpec(memory_space=pltpu.SMEM)),
        input_output_aliases={7 + k: k for k in range(len(before))},
        compiler_params=pltpu.CompilerParams(vmem_limit_bytes=VMEM_LIMIT),
        cost_estimate=pl.CostEstimate(flops=30 * part_rows * LANES * 40, bytes_accessed=20 * part_rows * LANES, transcendentals=0),
    )(lr, norm, stay(g), stay(w), stay(m), v, mask, *before)


def store_kernel(spots, direct, *refs):
    count = len(spots)
    pieces = refs[:count]
    params, buf, in_sem, out_sem = refs[-4:]
    me, part, along_x, along_y = places()
    diag = along_x + along_y - me
    shift = part - me
    blocks = (me, along_x, along_y, diag, me + shift, along_x + shift, along_y + shift, diag + shift)
    loads, stores = [], []
    for k, (which, start, size, grains) in enumerate(spots):
        dst = params.at[pl.ds(blocks[which] * grains + start, size)]
        src = pieces[k].at[pl.ds(0, size)]
        if not direct:
            loads.append(pltpu.make_async_copy(src, buf.at[k, pl.ds(0, size)], in_sem.at[k]))
            src = buf.at[k, pl.ds(0, size)]
        stores.append(pltpu.make_async_copy(src, dst, out_sem.at[k]))
    for cp in loads:
        cp.start()
    for k, out in enumerate(stores):
        if not direct:
            loads[k].wait()
        out.start()
    for out in stores:
        out.wait()


def store(pieces, spots, before, num_dev, grains, direct):
    count = len(pieces)
    if direct:
        pieces = [stay(p) for p in pieces]
    hbm = pl.BlockSpec(memory_space=pltpu.HBM)
    room = max(p.shape[0] for p in pieces)
    moved = sum(p.size for p in pieces)
    return pl.pallas_call(
        functools.partial(store_kernel, [(which, start, min(p.shape[0], grains - start), grains)
                                         for p, (which, start) in zip(pieces, spots)], direct),
        out_shape=jax.ShapeDtypeStruct((num_dev * grains, 4, LANES), jnp.bfloat16),
        in_specs=[pl.BlockSpec(memory_space=pltpu.VMEM) if direct else hbm] * count + [hbm] * len(before),
        out_specs=hbm,
        input_output_aliases={count: 0} if before else {},
        scratch_shapes=[pltpu.VMEM((1, 2, 4, LANES) if direct else (count, room, 4, LANES), jnp.bfloat16),
                        pltpu.SemaphoreType.DMA((count,)), pltpu.SemaphoreType.DMA((count,))],
        compiler_params=pltpu.CompilerParams(vmem_limit_bytes=VMEM_LIMIT),
        cost_estimate=pl.CostEstimate(flops=40 * moved, bytes_accessed=4 * moved, transcendentals=0),
    )(*pieces, *before)


def solution(mesh):
    num_dev = mesh.shape["dp"]
    hop = {"core": [(i, i ^ 1) for i in range(num_dev)], "x": [(i, i ^ 2) for i in range(num_dev)],
           "y": [(i, i ^ 4) for i in range(num_dev)]}

    def local_step(grad_row, master, mom_first, mom_second, decay_mask, learn_rate):
        shard_len = master.shape[0]
        rows = shard_len // LANES
        grains = rows // 4
        flat = lambda a: a.reshape(rows, LANES)

        def send(a, along):
            return lax.ppermute(a, "dp", hop[along])

        def put(pieces, spots, whole, direct=False):
            return (store(pieces, spots, whole, num_dev, grains, direct),)

        g, w, m, norm = reduce_scatter(grad_row, flat(master), flat(mom_first), rows, num_dev)
        state = ()
        whole = ()
        arrived = []
        firsts = [sum(PARTS[:p]) for p in range(len(PARTS))]
        for p, steps in enumerate(PARTS):
            *state, packed, grad_norm = adamw(
                firsts[p], steps, learn_rate, norm, g, w, m, flat(mom_second), flat(decay_mask), state)
            arrived.append((packed, send(packed, "x"), send(packed, "y"),
                            send(packed, "core")))
        starts = [first * ADAM_ROWS // 4 for first in firsts]
        far = []
        for p, (packed, from_x, from_y, from_core) in enumerate(arrived):
            far.append(send(from_x, "y") if p % 2 == 0 else send(from_y, "x"))
            pieces = [packed, from_x, from_y, from_core, send(from_x, "core"), send(from_y, "core")]
            whole = put(pieces, [(k, starts[p]) for k in (0, 1, 2, 4, 5, 6)], whole)
        for p in range(0, len(PARTS), 2):
            pieces, spots = [], []
            for q in (p, p + 1):
                pieces += [far[q], send(far[q], "core")]
                spots += [(3, starts[q]), (7, starts[q])]
            whole = put(pieces, spots, whole, p + 2 == len(PARTS))
        new_w, new_m, new_v = state
        params = whole[0].reshape(num_dev * shard_len)
        return (params, new_w.reshape(shard_len), new_m.reshape(shard_len), new_v.reshape(shard_len),
                grad_norm)

    return jax.shard_map(
        local_step, mesh=mesh,
        in_specs=(P("dp", None), P("dp"), P("dp"), P("dp"), P("dp"), P()),
        out_specs=(P(), P("dp"), P("dp"), P("dp"), P()), check_vma=False)
```

```python
import functools

import jax
import jax.numpy as jnp
from jax import lax
from jax.experimental import pallas as pl
from jax.experimental.pallas import tpu as pltpu
from jax.sharding import PartitionSpec as P


BETA_FIRST = 0.9
BETA_SECOND = 0.95
ADAM_EPS = 1e-8
CLIP_EPS = 1e-6
WEIGHT_DECAY = 0.1
ADAM_STEP = 10

MESH = pl.DeviceIdType.MESH
LANES = 128
CHUNK_ROWS = 384
HALF_ROWS = CHUNK_ROWS // 2
SLOTS = 4
VMEM_LIMIT = 20 << 20
ADAM_ROWS = 960
PARTS = (2, 3, 4, 4, 4, 4, 2, 1, 1, 1)
TILE_ROWS = 120


def places():
    me = lax.axis_index("dp")
    core = me % 2
    part = me + 1 - 2 * core
    along_x = me + 2 - 4 * ((me // 2) % 2)
    along_y = me + 4 - 8 * (me // 4)
    return me, part, along_x, along_y


def meet(peers):
    barrier = pltpu.get_barrier_semaphore()
    for peer in peers:
        pl.semaphore_signal(barrier, inc=1, device_id=(peer,), device_id_type=MESH)
    pl.semaphore_wait(barrier, len(peers))


def stay(array):
    return pltpu.with_memory_space_constraint(array, pltpu.VMEM)


def remote(src, dst, send_sem, recv_sem, device):
    return pltpu.make_async_remote_copy(
        src_ref=src, dst_ref=dst, send_sem=send_sem, recv_sem=recv_sem,
        device_id=(device,), device_id_type=MESH)


def adamw_tile(g, w, m, v, mask, coef, rate):
    h = g * coef
    first = BETA_FIRST * m + (1.0 - BETA_FIRST) * h
    second = BETA_SECOND * v + (1.0 - BETA_SECOND) * h * h
    step_dir = (first * (1.0 / (1.0 - BETA_FIRST ** ADAM_STEP))) / (
        jnp.sqrt(second * (1.0 / (1.0 - BETA_SECOND ** ADAM_STEP))) + ADAM_EPS)
    new = w - rate * (step_dir + WEIGHT_DECAY * mask.astype(jnp.float32) * w)
    return new, first, second


def pack_tile(packed, t, new):
    grains = TILE_ROWS // 4
    packed[pl.ds(pl.multiple_of(t * grains, 2), grains)] = new.reshape(grains, 4, LANES).astype(packed.dtype)


def reduce_kernel(shard_rows, lr, grad, w, m, v, mask, g_out, w_out, m_out, packed, norm_out,
                  own, other, x_send, y_send, x_keep, y_keep, mine, x_recv, y_recv, acc, norm_recv,
                  own_sem, part_ssem, part_rsem, x_ssem, x_rsem, y_ssem, y_rsem, n_ssem, n_rsem,
                  v_part, mask_part, fetch_sem):
    me, part, along_x, along_y = places()
    diag = along_x + along_y - me
    shift = part - me
    blocks = (me, along_x, along_y, diag)
    shard_len = shard_rows * LANES
    full = CHUNK_ROWS * LANES
    chunks = -(-shard_rows // CHUNK_ROWS)
    tail = (shard_rows - (chunks - 1) * CHUNK_ROWS) * LANES
    num_dev = grad.shape[1] // shard_len
    others = [(me + k) % num_dev for k in range(1, num_dev)]
    ahead = v_part.shape[0]
    fetches = [pltpu.make_async_copy(src, dst, fetch_sem.at[k]) for k, (src, dst) in enumerate((
        (w, w_out.at[pl.ds(0, shard_rows)]), (m, m_out.at[pl.ds(0, shard_rows)]),
        (v.at[pl.ds(0, ahead)], v_part), (mask.at[pl.ds(0, ahead)], mask_part)))]

    acc[...] = jnp.zeros_like(acc)

    def loads(i, size):
        slot = i % SLOTS
        out = []
        for b, block in enumerate(blocks):
            src = pl.multiple_of(block * shard_len + i * full, LANES)
            out.append(pltpu.make_async_copy(
                grad.at[:, pl.ds(src, size)], own.at[slot, b, :, pl.ds(0, size)], own_sem.at[slot, b]))
        return out

    def swaps(i, size):
        slot = i % SLOTS
        out = []
        for b, block in enumerate(blocks):
            src = pl.multiple_of((block + shift) * shard_len + i * full, LANES)
            out.append(remote(
                grad.at[:, pl.ds(src, size)], other.at[slot, b, :, pl.ds(0, size)],
                part_ssem.at[slot, b], part_rsem.at[slot, b], part))
        return out

    def for_size(i, do):
        @pl.when(i < chunks - 1)
        def _():
            do(full)

        @pl.when(i == chunks - 1)
        def _():
            do(tail)

    def hops(q, planes):
        slot = q % SLOTS
        return (remote(x_send.at[slot, planes], x_recv.at[slot, planes], x_ssem.at[slot], x_rsem.at[slot], along_x),
                remote(y_send.at[slot, planes], y_recv.at[slot, planes], y_ssem.at[slot], y_rsem.at[slot], along_y))

    def for_planes(q, do):
        @pl.when((q >= 1) & (q < 3))
        def _():
            do(pl.ds(0, 2))

        @pl.when((q >= 3) & (q <= chunks))
        def _():
            do(pl.ds(0, 3))

        @pl.when((q > chunks) & (q <= chunks + 2))
        def _():
            do(pl.ds(2, 1))

    for cp in loads(0, full):
        cp.start()
    meet(others)
    for cp in swaps(0, full):
        cp.start()

    def begin(i):
        def do(size):
            for cp in swaps(i, size) + loads(i, size):
                cp.start()

        for_size(i, do)

    def pair_sums(j):
        def do(size):
            for cp in loads(j, size) + swaps(j, size):
                cp.wait()

        for_size(j, do)
        slot = j % SLOTS
        out = (j + 1) % SLOTS
        kept = j % (SLOTS + 1)

        def tile(t, carry):
            for half in range(2):
                row = pl.multiple_of(t * 8, 8)
                col = pl.multiple_of((t + half * (HALF_ROWS // 8)) * 8 * LANES, 8 * LANES)

                def pair(b):
                    a = own[slot, b, :, pl.ds(col, 8 * LANES)].astype(jnp.float32)
                    o = other[slot, b, :, pl.ds(col, 8 * LANES)].astype(jnp.float32)
                    return (a + o).reshape(8, LANES)

                mine[kept, half, pl.ds(row, 8)] = pair(0)
                if half == 0:
                    x_send[out, 0, pl.ds(row, 8)] = pair(1)
                    y_keep[slot, pl.ds(row, 8)] = pair(2)
                    x_send[out, 1, pl.ds(row, 8)] = pair(3)
                else:
                    x_keep[slot, pl.ds(row, 8)] = pair(1)
                    y_send[out, 0, pl.ds(row, 8)] = pair(2)
                    y_send[out, 1, pl.ds(row, 8)] = pair(3)
            return carry

        lax.fori_loop(0, HALF_ROWS // 8, tile, 0)

    def wait_for(q):
        def do(planes):
            for cp in hops(q, planes):
                cp.wait()

        for_planes(q, do)

    def relay(j):
        slot = j % SLOTS
        got = (j + 1) % SLOTS
        out = (j + 3) % SLOTS
        kept = j % (SLOTS + 1)
        x_send[out, 2] = x_keep[slot] + y_recv[got, 1]
        y_send[out, 2] = y_keep[slot] + x_recv[got, 1]
        mine[kept, 0] = mine[kept, 0] + x_recv[got, 0]
        mine[kept, 1] = mine[kept, 1] + y_recv[got, 0]

    def finish(j):
        got = (j + 3) % SLOTS
        kept = j % (SLOTS + 1)
        base = j * CHUNK_ROWS
        left = shard_rows - j * CHUNK_ROWS
        rows = lax.broadcasted_iota(jnp.int32, (8, LANES), 0)

        def tile(t, total):
            row = pl.multiple_of(t * 8, 8)
            top = (mine[kept, 0, pl.ds(row, 8)] + y_recv[got, 2, pl.ds(row, 8)]) * 0.125
            low = (mine[kept, 1, pl.ds(row, 8)] + x_recv[got, 2, pl.ds(row, 8)]) * 0.125
            g_out[pl.ds(pl.multiple_of(base + t * 8, 8), 8)] = top
            g_out[pl.ds(pl.multiple_of(base + HALF_ROWS + t * 8, 8), 8)] = low
            total = total + jnp.where(rows + t * 8 < left, top * top, 0.0)
            return total + jnp.where(rows + (HALF_ROWS + t * 8) < left, low * low, 0.0)

        acc[...] += lax.fori_loop(0, HALF_ROWS // 8, tile, jnp.zeros((8, LANES), jnp.float32))

    def step(i, carry):
        @pl.when((i >= 1) & (i < chunks))
        def _():
            begin(i)

        @pl.when((i >= 1) & (i <= chunks))
        def _():
            pair_sums(i - 1)

        wait_for(i - 2)

        @pl.when((i >= 3) & (i <= chunks + 2))
        def _():
            relay(i - 3)

        @pl.when(i >= 5)
        def _():
            finish(i - 5)

        def go(planes):
            for cp in hops(i, planes):
                cp.start()

        for_planes(i, go)

        @pl.when(i == 4)
        def _():
            for cp in fetches:
                cp.start()

        return carry

    lax.fori_loop(0, chunks + 5, step, 0)
    norm_recv[me] = acc[...]

    def shares(peer, k):
        return remote(acc, norm_recv.at[me], n_ssem.at[k], n_rsem.at[me], peer)

    for k, peer in enumerate(others):
        shares(peer, k).start()
    for cp in fetches:
        cp.wait()
    for k, peer in enumerate(others):
        shares(peer, k).wait_send()
        remote(acc, norm_recv.at[peer], n_ssem.at[k], n_rsem.at[peer], peer).wait_recv()
    total = norm_recv[0]
    for k in range(1, num_dev):
        total = total + norm_recv[k]
    norm = jnp.broadcast_to(jnp.sqrt(jnp.sum(total, keepdims=True)), norm_out.shape)
    norm_out[...] = norm
    coef = jnp.minimum(1.0, 1.0 / (norm[0:1] + CLIP_EPS))
    rate = lr[0]

    def part_tile(t, carry):
        at = pl.ds(pl.multiple_of(t * TILE_ROWS, 8), TILE_ROWS)
        new, _, _ = adamw_tile(g_out[at], w_out[at], m_out[at], v_part[at], mask_part[at], coef, rate)
        pack_tile(packed, t, new)
        return carry

    lax.fori_loop(0, ahead // TILE_ROWS, part_tile, 0)


def reduce_scatter(lr, grad_row, w, m, v, mask, num_dev):
    f32, bf16 = jnp.float32, jnp.bfloat16
    shard_rows = w.shape[0]
    chunks = -(-shard_rows // CHUNK_ROWS)
    ahead = PARTS[0] * ADAM_ROWS
    vm, dma = pltpu.VMEM, pltpu.SemaphoreType.DMA
    three = (SLOTS, 3, HALF_ROWS, LANES)
    one = (SLOTS, HALF_ROWS, LANES)
    raw = (SLOTS, 4, 1, CHUNK_ROWS * LANES)
    state = vm((chunks * CHUNK_ROWS, LANES), f32)
    return pl.pallas_call(
        functools.partial(reduce_kernel, shard_rows),
        out_shape=(state, state, state, vm((ahead // 4, 4, LANES), bf16), jax.ShapeDtypeStruct((8, LANES), f32)),
        in_specs=[pl.BlockSpec(memory_space=pltpu.SMEM)] + [pl.BlockSpec(memory_space=pltpu.HBM)] * 5,
        out_specs=(pl.BlockSpec(memory_space=vm),) * 5,
        scratch_shapes=[
            vm(raw, bf16), vm(raw, bf16), vm(three, f32), vm(three, f32), vm(one, f32), vm(one, f32),
            vm((SLOTS + 1, 2, HALF_ROWS, LANES), f32), vm(three, f32), vm(three, f32), vm((8, LANES), f32),
            vm((num_dev, 8, LANES), f32),
            dma((SLOTS, 4)), dma((SLOTS, 4)), dma((SLOTS, 4)),
            dma((SLOTS,)), dma((SLOTS,)), dma((SLOTS,)), dma((SLOTS,)),
            dma((num_dev - 1,)), dma((num_dev,)),
            vm((ahead, LANES), f32), vm((ahead, LANES), jnp.int32), dma((4,))],
        compiler_params=pltpu.CompilerParams(collective_id=0, has_side_effects=True,
                                             vmem_limit_bytes=VMEM_LIMIT),
    )(lr, grad_row, w, m, v, mask)


def adamw_kernel(lr, norm, g, w, m, v, mask, *rest):
    w_out, m_out, v_out, packed, norm_out = rest[-5:]
    norm_out[0] = norm[0, 0]
    coef = jnp.minimum(1.0, 1.0 / (norm[0:1] + CLIP_EPS))
    rate = lr[0]

    def tile(t, carry):
        at = pl.ds(pl.multiple_of(t * TILE_ROWS, 8), TILE_ROWS)
        w_out[at], m_out[at], v_out[at] = new, first, second = adamw_tile(
            g[at], w[at], m[at], v[at], mask[at], coef, rate)
        pack_tile(packed, t, new)
        return carry

    lax.fori_loop(0, ADAM_ROWS // TILE_ROWS, tile, 0)


def adamw(first, steps, lr, norm, g, w, m, v, mask, before):
    rows = v.shape[0]
    part_rows = steps * ADAM_ROWS
    block = pl.BlockSpec((ADAM_ROWS, LANES), lambda i: (i + first, 0))
    state = jax.ShapeDtypeStruct((rows, LANES), jnp.float32)
    blind = [pl.BlockSpec(memory_space=pl.ANY)] * len(before)
    return pl.pallas_call(
        adamw_kernel,
        grid=(steps,),
        out_shape=(state, state, state, jax.ShapeDtypeStruct((part_rows // 4, 4, LANES), jnp.bfloat16),
                   jax.ShapeDtypeStruct((1,), jnp.float32)),
        in_specs=[pl.BlockSpec(memory_space=pltpu.SMEM),
                  pl.BlockSpec((8, LANES), lambda i: (0, 0)),
                  block, block, block, block, block] + blind,
        out_specs=(block, block, block, pl.BlockSpec((ADAM_ROWS // 4, 4, LANES), lambda i: (i, 0, 0)),
                   pl.BlockSpec(memory_space=pltpu.SMEM)),
        input_output_aliases={7 + k: k for k in range(len(before))},
        compiler_params=pltpu.CompilerParams(vmem_limit_bytes=VMEM_LIMIT),
        cost_estimate=pl.CostEstimate(flops=30 * part_rows * LANES * 40, bytes_accessed=20 * part_rows * LANES, transcendentals=0),
    )(lr, norm, stay(g), stay(w), stay(m), v, mask, *before)


def store_kernel(spots, direct, *refs):
    count = len(spots)
    pieces = refs[:count]
    params, buf, in_sem, out_sem = refs[-4:]
    me, part, along_x, along_y = places()
    diag = along_x + along_y - me
    shift = part - me
    blocks = (me, along_x, along_y, diag, me + shift, along_x + shift, along_y + shift, diag + shift)
    loads, stores = [], []
    for k, (which, start, size, grains) in enumerate(spots):
        dst = params.at[pl.ds(blocks[which] * grains + start, size)]
        src = pieces[k].at[pl.ds(0, size)]
        if not direct:
            loads.append(pltpu.make_async_copy(src, buf.at[k, pl.ds(0, size)], in_sem.at[k]))
            src = buf.at[k, pl.ds(0, size)]
        stores.append(pltpu.make_async_copy(src, dst, out_sem.at[k]))
    for cp in loads:
        cp.start()
    for k, out in enumerate(stores):
        if not direct:
            loads[k].wait()
        out.start()
    for out in stores:
        out.wait()


def store(pieces, spots, before, num_dev, grains, direct):
    count = len(pieces)
    if direct:
        pieces = [stay(p) for p in pieces]
    hbm = pl.BlockSpec(memory_space=pltpu.HBM)
    room = max(p.shape[0] for p in pieces)
    moved = sum(p.size for p in pieces)
    return pl.pallas_call(
        functools.partial(store_kernel, [(which, start, min(p.shape[0], grains - start), grains)
                                         for p, (which, start) in zip(pieces, spots)], direct),
        out_shape=jax.ShapeDtypeStruct((num_dev * grains, 4, LANES), jnp.bfloat16),
        in_specs=[pl.BlockSpec(memory_space=pltpu.VMEM) if direct else hbm] * count + [hbm] * len(before),
        out_specs=hbm,
        input_output_aliases={count: 0} if before else {},
        scratch_shapes=[pltpu.VMEM((1, 2, 4, LANES) if direct else (count, room, 4, LANES), jnp.bfloat16),
                        pltpu.SemaphoreType.DMA((count,)), pltpu.SemaphoreType.DMA((count,))],
        compiler_params=pltpu.CompilerParams(vmem_limit_bytes=VMEM_LIMIT),
        cost_estimate=pl.CostEstimate(flops=40 * moved, bytes_accessed=4 * moved, transcendentals=0),
    )(*pieces, *before)


def solution(mesh):
    num_dev = mesh.shape["dp"]
    hop = {"core": [(i, i ^ 1) for i in range(num_dev)], "x": [(i, i ^ 2) for i in range(num_dev)],
           "y": [(i, i ^ 4) for i in range(num_dev)]}

    def local_step(grad_row, master, mom_first, mom_second, decay_mask, learn_rate):
        shard_len = master.shape[0]
        rows = shard_len // LANES
        grains = rows // 4
        flat = lambda a: a.reshape(rows, LANES)

        def send(a, along):
            return lax.ppermute(a, "dp", hop[along])

        def put(pieces, spots, whole, direct=False):
            return (store(pieces, spots, whole, num_dev, grains, direct),)

        v, mask = flat(mom_second), flat(decay_mask)
        g, w, m, packed, norm = reduce_scatter(
            learn_rate, grad_row, flat(master), flat(mom_first), v, mask, num_dev)
        packs = {0: packed}
        state = ()
        whole = ()
        firsts = [sum(PARTS[:p]) for p in range(len(PARTS))]
        for p in (*range(1, len(PARTS)), 0):
            *state, packed, grad_norm = adamw(firsts[p], PARTS[p], learn_rate, norm, g, w, m, v, mask, state)
            packs.setdefault(p, packed)
        arrived = [(packs[p], send(packs[p], "x"), send(packs[p], "y"),
                    send(packs[p], "core")) for p in range(len(PARTS))]
        starts = [first * ADAM_ROWS // 4 for first in firsts]
        far = []
        for p, (packed, from_x, from_y, from_core) in enumerate(arrived):
            far.append(send(from_x, "y") if p % 2 == 0 else send(from_y, "x"))
            pieces = [packed, from_x, from_y, from_core, send(from_x, "core"), send(from_y, "core")]
            whole = put(pieces, [(k, starts[p]) for k in (0, 1, 2, 4, 5, 6)], whole)
        for p in range(0, len(PARTS), 2):
            pieces, spots = [], []
            for q in (p, p + 1):
                pieces += [far[q], send(far[q], "core")]
                spots += [(3, starts[q]), (7, starts[q])]
            whole = put(pieces, spots, whole, p + 2 == len(PARTS))
        new_w, new_m, new_v = state
        params = whole[0].reshape(num_dev * shard_len)
        return (params, new_w.reshape(shard_len), new_m.reshape(shard_len), new_v.reshape(shard_len),
                grad_norm)

    return jax.shard_map(
        local_step, mesh=mesh,
        in_specs=(P("dp", None), P("dp"), P("dp"), P("dp"), P("dp"), P()),
        out_specs=(P(), P("dp"), P("dp"), P("dp"), P()), check_vma=False)
```

```python
import functools

import jax
import jax.numpy as jnp
from jax import lax
from jax.experimental import pallas as pl
from jax.experimental.pallas import tpu as pltpu
from jax.sharding import PartitionSpec as P


BETA_FIRST = 0.9
BETA_SECOND = 0.95
ADAM_EPS = 1e-8
CLIP_EPS = 1e-6
WEIGHT_DECAY = 0.1
ADAM_STEP = 10

MESH = pl.DeviceIdType.MESH
LANES = 128
CHUNK_ROWS = 384
HALF_ROWS = CHUNK_ROWS // 2
SLOTS = 4
VMEM_LIMIT = 20 << 20
ADAM_ROWS = 960
PARTS = (2, 3, 4, 4, 4, 4, 2, 1, 1, 1)
TILE_ROWS = 120


def places():
    me = lax.axis_index("dp")
    core = me % 2
    part = me + 1 - 2 * core
    along_x = me + 2 - 4 * ((me // 2) % 2)
    along_y = me + 4 - 8 * (me // 4)
    return me, part, along_x, along_y


def stay(array):
    return pltpu.with_memory_space_constraint(array, pltpu.VMEM)


def remote(src, dst, send_sem, recv_sem, device):
    return pltpu.make_async_remote_copy(
        src_ref=src, dst_ref=dst, send_sem=send_sem, recv_sem=recv_sem,
        device_id=(device,), device_id_type=MESH)


def adamw_tile(g, w, m, v, mask, coef, rate):
    h = g * coef
    first = BETA_FIRST * m + (1.0 - BETA_FIRST) * h
    second = BETA_SECOND * v + (1.0 - BETA_SECOND) * h * h
    step_dir = (first * (1.0 / (1.0 - BETA_FIRST ** ADAM_STEP))) / (
        jnp.sqrt(second * (1.0 / (1.0 - BETA_SECOND ** ADAM_STEP))) + ADAM_EPS)
    new = w - rate * (step_dir + WEIGHT_DECAY * mask.astype(jnp.float32) * w)
    return new, first, second


def pack_tile(packed, t, new):
    grains = TILE_ROWS // 4
    packed[pl.ds(pl.multiple_of(t * grains, 2), grains)] = new.reshape(grains, 4, LANES).astype(packed.dtype)


def reduce_kernel(shard_rows, lr, grad, w, m, v, mask, g_out, w_out, m_out, packed, norm_out,
                  own, other, x_send, y_send, x_keep, y_keep, mine, x_recv, y_recv, acc, norm_recv,
                  own_sem, part_ssem, part_rsem, x_ssem, x_rsem, y_ssem, y_rsem, n_ssem, n_rsem,
                  v_part, mask_part, fetch_sem, head, head_sem):
    me, part, along_x, along_y = places()
    diag = along_x + along_y - me
    shift = part - me
    blocks = (me, along_x, along_y, diag)
    shard_len = shard_rows * LANES
    full = CHUNK_ROWS * LANES
    chunks = -(-shard_rows // CHUNK_ROWS)
    tail = (shard_rows - (chunks - 1) * CHUNK_ROWS) * LANES
    num_dev = grad.shape[1] // shard_len
    others = [(me + k) % num_dev for k in range(1, num_dev)]
    ahead = v_part.shape[0]
    fetches = [pltpu.make_async_copy(src, dst, fetch_sem.at[k]) for k, (src, dst) in enumerate((
        (w, w_out.at[pl.ds(0, shard_rows)]), (m, m_out.at[pl.ds(0, shard_rows)]),
        (v.at[pl.ds(0, ahead)], v_part), (mask.at[pl.ds(0, ahead)], mask_part)))]

    barrier = pltpu.get_barrier_semaphore()
    acc[...] = jnp.zeros_like(acc)

    def loads(i, size):
        slot = i % SLOTS
        out = []
        for b, block in enumerate(blocks):
            src = pl.multiple_of(block * shard_len + i * full, LANES)
            out.append(pltpu.make_async_copy(
                grad.at[:, pl.ds(src, size)], own.at[slot, b, :, pl.ds(0, size)], own_sem.at[slot, b]))
        return out

    def swaps(i, size):
        slot = i % SLOTS
        out = []
        for b, block in enumerate(blocks):
            src = pl.multiple_of((block + shift) * shard_len + i * full, LANES)
            out.append(remote(
                grad.at[:, pl.ds(src, size)], other.at[slot, b, :, pl.ds(0, size)],
                part_ssem.at[slot, b], part_rsem.at[slot, b], part))
        return out

    def for_size(i, do):
        @pl.when(i < chunks - 1)
        def _():
            do(full)

        @pl.when(i == chunks - 1)
        def _():
            do(tail)

    def hops(q, planes):
        slot = q % SLOTS
        return (remote(x_send.at[slot, planes], x_recv.at[slot, planes], x_ssem.at[slot], x_rsem.at[slot], along_x),
                remote(y_send.at[slot, planes], y_recv.at[slot, planes], y_ssem.at[slot], y_rsem.at[slot], along_y))

    def for_planes(q, do):
        @pl.when((q >= 1) & (q < 3))
        def _():
            do(pl.ds(0, 2))

        @pl.when((q >= 3) & (q <= chunks))
        def _():
            do(pl.ds(0, 3))

        @pl.when((q > chunks) & (q <= chunks + 2))
        def _():
            do(pl.ds(2, 1))

    staged = []
    for b, block in enumerate(blocks):
        src = pl.multiple_of((block + shift) * shard_len, LANES)
        staged.append(pltpu.make_async_copy(grad.at[:, pl.ds(src, full)], head.at[b], head_sem.at[b]))
    for cp in staged + loads(0, full):
        cp.start()
    for peer in (part, along_x, along_y):
        pl.semaphore_signal(barrier, inc=1, device_id=(peer,), device_id_type=MESH)
    for cp in staged:
        cp.wait()
    pl.semaphore_wait(barrier, 3)
    for b in range(len(blocks)):
        remote(head.at[b], other.at[0, b], part_ssem.at[0, b], part_rsem.at[0, b], part).start()

    def begin(i):
        def do(size):
            for cp in swaps(i, size) + loads(i, size):
                cp.start()

        for_size(i, do)

    def pair_sums(j):
        def do(size):
            for cp in loads(j, size) + swaps(j, size):
                cp.wait()

        for_size(j, do)
        slot = j % SLOTS
        out = (j + 1) % SLOTS
        kept = j % (SLOTS + 1)

        def tile(t, carry):
            for half in range(2):
                row = pl.multiple_of(t * 8, 8)
                col = pl.multiple_of((t + half * (HALF_ROWS // 8)) * 8 * LANES, 8 * LANES)

                def pair(b):
                    a = own[slot, b, :, pl.ds(col, 8 * LANES)].astype(jnp.float32)
                    o = other[slot, b, :, pl.ds(col, 8 * LANES)].astype(jnp.float32)
                    return (a + o).reshape(8, LANES)

                mine[kept, half, pl.ds(row, 8)] = pair(0)
                if half == 0:
                    x_send[out, 0, pl.ds(row, 8)] = pair(1)
                    y_keep[slot, pl.ds(row, 8)] = pair(2)
                    x_send[out, 1, pl.ds(row, 8)] = pair(3)
                else:
                    x_keep[slot, pl.ds(row, 8)] = pair(1)
                    y_send[out, 0, pl.ds(row, 8)] = pair(2)
                    y_send[out, 1, pl.ds(row, 8)] = pair(3)
            return carry

        lax.fori_loop(0, HALF_ROWS // 8, tile, 0)

    def wait_for(q):
        def do(planes):
            for cp in hops(q, planes):
                cp.wait()

        for_planes(q, do)

    def relay(j):
        slot = j % SLOTS
        got = (j + 1) % SLOTS
        out = (j + 3) % SLOTS
        kept = j % (SLOTS + 1)
        x_send[out, 2] = x_keep[slot] + y_recv[got, 1]
        y_send[out, 2] = y_keep[slot] + x_recv[got, 1]
        mine[kept, 0] = mine[kept, 0] + x_recv[got, 0]
        mine[kept, 1] = mine[kept, 1] + y_recv[got, 0]

    def finish(j):
        got = (j + 3) % SLOTS
        kept = j % (SLOTS + 1)
        base = j * CHUNK_ROWS
        left = shard_rows - j * CHUNK_ROWS
        rows = lax.broadcasted_iota(jnp.int32, (8, LANES), 0)

        def tile(t, total):
            row = pl.multiple_of(t * 8, 8)
            top = (mine[kept, 0, pl.ds(row, 8)] + y_recv[got, 2, pl.ds(row, 8)]) * 0.125
            low = (mine[kept, 1, pl.ds(row, 8)] + x_recv[got, 2, pl.ds(row, 8)]) * 0.125
            g_out[pl.ds(pl.multiple_of(base + t * 8, 8), 8)] = top
            g_out[pl.ds(pl.multiple_of(base + HALF_ROWS + t * 8, 8), 8)] = low
            total = total + jnp.where(rows + t * 8 < left, top * top, 0.0)
            return total + jnp.where(rows + (HALF_ROWS + t * 8) < left, low * low, 0.0)

        acc[...] += lax.fori_loop(0, HALF_ROWS // 8, tile, jnp.zeros((8, LANES), jnp.float32))

    def step(i, carry):
        @pl.when((i >= 1) & (i < chunks))
        def _():
            begin(i)

        @pl.when((i >= 1) & (i <= chunks))
        def _():
            pair_sums(i - 1)

        wait_for(i - 2)

        @pl.when((i >= 3) & (i <= chunks + 2))
        def _():
            relay(i - 3)

        @pl.when(i >= 5)
        def _():
            finish(i - 5)

        def go(planes):
            for cp in hops(i, planes):
                cp.start()

        for_planes(i, go)

        @pl.when(i == 4)
        def _():
            for cp in fetches:
                cp.start()

        return carry

    lax.fori_loop(0, chunks + 5, step, 0)
    norm_recv[me] = acc[...]

    def shares(peer, k):
        return remote(acc, norm_recv.at[me], n_ssem.at[k], n_rsem.at[me], peer)

    for k, peer in enumerate(others):
        shares(peer, k).start()
    for cp in fetches:
        cp.wait()
    for k, peer in enumerate(others):
        shares(peer, k).wait_send()
        remote(acc, norm_recv.at[peer], n_ssem.at[k], n_rsem.at[peer], peer).wait_recv()
    total = norm_recv[0]
    for k in range(1, num_dev):
        total = total + norm_recv[k]
    norm = jnp.broadcast_to(jnp.sqrt(jnp.sum(total, keepdims=True)), norm_out.shape)
    norm_out[...] = norm
    coef = jnp.minimum(1.0, 1.0 / (norm[0:1] + CLIP_EPS))
    rate = lr[0]

    def part_tile(t, carry):
        at = pl.ds(pl.multiple_of(t * TILE_ROWS, 8), TILE_ROWS)
        new, _, _ = adamw_tile(g_out[at], w_out[at], m_out[at], v_part[at], mask_part[at], coef, rate)
        pack_tile(packed, t, new)
        return carry

    lax.fori_loop(0, ahead // TILE_ROWS, part_tile, 0)


def reduce_scatter(lr, grad_row, w, m, v, mask, num_dev):
    f32, bf16 = jnp.float32, jnp.bfloat16
    shard_rows = w.shape[0]
    chunks = -(-shard_rows // CHUNK_ROWS)
    ahead = PARTS[0] * ADAM_ROWS
    vm, dma = pltpu.VMEM, pltpu.SemaphoreType.DMA
    three = (SLOTS, 3, HALF_ROWS, LANES)
    one = (SLOTS, HALF_ROWS, LANES)
    raw = (SLOTS, 4, 1, CHUNK_ROWS * LANES)
    state = vm((chunks * CHUNK_ROWS, LANES), f32)
    return pl.pallas_call(
        functools.partial(reduce_kernel, shard_rows),
        out_shape=(state, state, state, vm((ahead // 4, 4, LANES), bf16), jax.ShapeDtypeStruct((8, LANES), f32)),
        in_specs=[pl.BlockSpec(memory_space=pltpu.SMEM)] + [pl.BlockSpec(memory_space=pltpu.HBM)] * 5,
        out_specs=(pl.BlockSpec(memory_space=vm),) * 5,
        scratch_shapes=[
            vm(raw, bf16), vm(raw, bf16), vm(three, f32), vm(three, f32), vm(one, f32), vm(one, f32),
            vm((SLOTS + 1, 2, HALF_ROWS, LANES), f32), vm(three, f32), vm(three, f32), vm((8, LANES), f32),
            vm((num_dev, 8, LANES), f32),
            dma((SLOTS, 4)), dma((SLOTS, 4)), dma((SLOTS, 4)),
            dma((SLOTS,)), dma((SLOTS,)), dma((SLOTS,)), dma((SLOTS,)),
            dma((num_dev - 1,)), dma((num_dev,)),
            vm((ahead, LANES), f32), vm((ahead, LANES), jnp.int32), dma((4,)),
            vm(raw[1:], bf16), dma((4,))],
        compiler_params=pltpu.CompilerParams(collective_id=0, has_side_effects=True,
                                             vmem_limit_bytes=VMEM_LIMIT),
    )(lr, grad_row, w, m, v, mask)


def adamw_kernel(lr, norm, g, w, m, v, mask, *rest):
    w_out, m_out, v_out, packed, norm_out = rest[-5:]
    norm_out[0] = norm[0, 0]
    coef = jnp.minimum(1.0, 1.0 / (norm[0:1] + CLIP_EPS))
    rate = lr[0]

    def tile(t, carry):
        at = pl.ds(pl.multiple_of(t * TILE_ROWS, 8), TILE_ROWS)
        w_out[at], m_out[at], v_out[at] = new, first, second = adamw_tile(
            g[at], w[at], m[at], v[at], mask[at], coef, rate)
        pack_tile(packed, t, new)
        return carry

    lax.fori_loop(0, ADAM_ROWS // TILE_ROWS, tile, 0)


def adamw(first, steps, lr, norm, g, w, m, v, mask, before):
    rows = v.shape[0]
    part_rows = steps * ADAM_ROWS
    block = pl.BlockSpec((ADAM_ROWS, LANES), lambda i: (i + first, 0))
    state = jax.ShapeDtypeStruct((rows, LANES), jnp.float32)
    blind = [pl.BlockSpec(memory_space=pl.ANY)] * len(before)
    return pl.pallas_call(
        adamw_kernel,
        grid=(steps,),
        out_shape=(state, state, state, jax.ShapeDtypeStruct((part_rows // 4, 4, LANES), jnp.bfloat16),
                   jax.ShapeDtypeStruct((1,), jnp.float32)),
        in_specs=[pl.BlockSpec(memory_space=pltpu.SMEM),
                  pl.BlockSpec((8, LANES), lambda i: (0, 0)),
                  block, block, block, block, block] + blind,
        out_specs=(block, block, block, pl.BlockSpec((ADAM_ROWS // 4, 4, LANES), lambda i: (i, 0, 0)),
                   pl.BlockSpec(memory_space=pltpu.SMEM)),
        input_output_aliases={7 + k: k for k in range(len(before))},
        compiler_params=pltpu.CompilerParams(vmem_limit_bytes=VMEM_LIMIT),
        cost_estimate=pl.CostEstimate(flops=30 * part_rows * LANES * 40, bytes_accessed=20 * part_rows * LANES, transcendentals=0),
    )(lr, norm, stay(g), stay(w), stay(m), v, mask, *before)


def store_kernel(spots, direct, *refs):
    count = len(spots)
    pieces = refs[:count]
    params, buf, in_sem, out_sem = refs[-4:]
    me, part, along_x, along_y = places()
    diag = along_x + along_y - me
    shift = part - me
    blocks = (me, along_x, along_y, diag, me + shift, along_x + shift, along_y + shift, diag + shift)
    loads, stores = [], []
    for k, (which, start, size, grains) in enumerate(spots):
        dst = params.at[pl.ds(blocks[which] * grains + start, size)]
        src = pieces[k].at[pl.ds(0, size)]
        if not direct:
            loads.append(pltpu.make_async_copy(src, buf.at[k, pl.ds(0, size)], in_sem.at[k]))
            src = buf.at[k, pl.ds(0, size)]
        stores.append(pltpu.make_async_copy(src, dst, out_sem.at[k]))
    for cp in loads:
        cp.start()
    for k, out in enumerate(stores):
        if not direct:
            loads[k].wait()
        out.start()
    for out in stores:
        out.wait()


def store(pieces, spots, before, num_dev, grains, direct):
    count = len(pieces)
    if direct:
        pieces = [stay(p) for p in pieces]
    hbm = pl.BlockSpec(memory_space=pltpu.HBM)
    room = max(p.shape[0] for p in pieces)
    moved = sum(p.size for p in pieces)
    return pl.pallas_call(
        functools.partial(store_kernel, [(which, start, min(p.shape[0], grains - start), grains)
                                         for p, (which, start) in zip(pieces, spots)], direct),
        out_shape=jax.ShapeDtypeStruct((num_dev * grains, 4, LANES), jnp.bfloat16),
        in_specs=[pl.BlockSpec(memory_space=pltpu.VMEM) if direct else hbm] * count + [hbm] * len(before),
        out_specs=hbm,
        input_output_aliases={count: 0} if before else {},
        scratch_shapes=[pltpu.VMEM((1, 2, 4, LANES) if direct else (count, room, 4, LANES), jnp.bfloat16),
                        pltpu.SemaphoreType.DMA((count,)), pltpu.SemaphoreType.DMA((count,))],
        compiler_params=pltpu.CompilerParams(vmem_limit_bytes=VMEM_LIMIT),
        cost_estimate=pl.CostEstimate(flops=40 * moved, bytes_accessed=4 * moved, transcendentals=0),
    )(*pieces, *before)


def solution(mesh):
    num_dev = mesh.shape["dp"]
    hop = {"core": [(i, i ^ 1) for i in range(num_dev)], "x": [(i, i ^ 2) for i in range(num_dev)],
           "y": [(i, i ^ 4) for i in range(num_dev)]}

    def local_step(grad_row, master, mom_first, mom_second, decay_mask, learn_rate):
        shard_len = master.shape[0]
        rows = shard_len // LANES
        grains = rows // 4
        flat = lambda a: a.reshape(rows, LANES)

        def send(a, along):
            return lax.ppermute(a, "dp", hop[along])

        def put(pieces, spots, whole, direct=False):
            return (store(pieces, spots, whole, num_dev, grains, direct),)

        v, mask = flat(mom_second), flat(decay_mask)
        g, w, m, packed, norm = reduce_scatter(
            learn_rate, grad_row, flat(master), flat(mom_first), v, mask, num_dev)
        packs = {0: packed}
        state = ()
        whole = ()
        firsts = [sum(PARTS[:p]) for p in range(len(PARTS))]
        for p in (*range(1, len(PARTS)), 0):
            *state, packed, grad_norm = adamw(firsts[p], PARTS[p], learn_rate, norm, g, w, m, v, mask, state)
            packs.setdefault(p, packed)
        arrived = [(packs[p], send(packs[p], "x"), send(packs[p], "y"),
                    send(packs[p], "core")) for p in range(len(PARTS))]
        starts = [first * ADAM_ROWS // 4 for first in firsts]
        far = []
        for p, (packed, from_x, from_y, from_core) in enumerate(arrived):
            far.append(send(from_x, "y") if p % 2 == 0 else send(from_y, "x"))
            pieces = [packed, from_x, from_y, from_core, send(from_x, "core"), send(from_y, "core")]
            whole = put(pieces, [(k, starts[p]) for k in (0, 1, 2, 4, 5, 6)], whole)
        for p in range(0, len(PARTS), 2):
            pieces, spots = [], []
            for q in (p, p + 1):
                pieces += [far[q], send(far[q], "core")]
                spots += [(3, starts[q]), (7, starts[q])]
            whole = put(pieces, spots, whole, p + 2 == len(PARTS))
        new_w, new_m, new_v = state
        params = whole[0].reshape(num_dev * shard_len)
        return (params, new_w.reshape(shard_len), new_m.reshape(shard_len), new_v.reshape(shard_len),
                grad_norm)

    return jax.shard_map(
        local_step, mesh=mesh,
        in_specs=(P("dp", None), P("dp"), P("dp"), P("dp"), P("dp"), P()),
        out_specs=(P(), P("dp"), P("dp"), P("dp"), P()), check_vma=False)
```

```python
import functools

import jax
import jax.numpy as jnp
from jax import lax
from jax.experimental import pallas as pl
from jax.experimental.pallas import tpu as pltpu
from jax.sharding import PartitionSpec as P


BETA_FIRST = 0.9
BETA_SECOND = 0.95
ADAM_EPS = 1e-8
CLIP_EPS = 1e-6
WEIGHT_DECAY = 0.1
ADAM_STEP = 10

MESH = pl.DeviceIdType.MESH
LANES = 128
CHUNK_ROWS = 384
HALF_ROWS = CHUNK_ROWS // 2
SLOTS = 4
VMEM_LIMIT = 20 << 20
ADAM_ROWS = 960
PARTS = (2, 3, 4, 4, 4, 4, 2, 1, 1, 1)
TILE_ROWS = 120


def places():
    me = lax.axis_index("dp")
    core = me % 2
    part = me + 1 - 2 * core
    along_x = me + 2 - 4 * ((me // 2) % 2)
    along_y = me + 4 - 8 * (me // 4)
    return me, part, along_x, along_y


def stay(array):
    return pltpu.with_memory_space_constraint(array, pltpu.VMEM)


def remote(src, dst, send_sem, recv_sem, device):
    return pltpu.make_async_remote_copy(
        src_ref=src, dst_ref=dst, send_sem=send_sem, recv_sem=recv_sem,
        device_id=(device,), device_id_type=MESH)


def adamw_tile(g, w, m, v, mask, coef, rate):
    h = g * coef
    first = BETA_FIRST * m + (1.0 - BETA_FIRST) * h
    second = BETA_SECOND * v + (1.0 - BETA_SECOND) * h * h
    step_dir = (first * (1.0 / (1.0 - BETA_FIRST ** ADAM_STEP))) / (
        jnp.sqrt(second * (1.0 / (1.0 - BETA_SECOND ** ADAM_STEP))) + ADAM_EPS)
    new = w - rate * (step_dir + WEIGHT_DECAY * mask.astype(jnp.float32) * w)
    return new, first, second


def pack_tile(packed, t, new):
    grains = TILE_ROWS // 4
    packed[pl.ds(pl.multiple_of(t * grains, 2), grains)] = new.reshape(grains, 4, LANES).astype(packed.dtype)


def reduce_kernel(shard_rows, lr, grad, w, m, v, mask, g_out, w_out, m_out, packed, norm_out,
                  own, other, x_send, y_send, x_keep, y_keep, mine, x_recv, y_recv, acc, norm_recv,
                  own_sem, part_ssem, part_rsem, x_ssem, x_rsem, y_ssem, y_rsem, n_ssem, n_rsem,
                  v_part, mask_part, fetch_sem, head, head_sem):
    me, part, along_x, along_y = places()
    diag = along_x + along_y - me
    shift = part - me
    blocks = (me, along_x, along_y, diag)
    shard_len = shard_rows * LANES
    full = CHUNK_ROWS * LANES
    chunks = -(-shard_rows // CHUNK_ROWS)
    tail = (shard_rows - (chunks - 1) * CHUNK_ROWS) * LANES
    num_dev = grad.shape[1] // shard_len
    others = [(me + k) % num_dev for k in range(1, num_dev)]
    ahead = v_part.shape[0]
    fetches = [pltpu.make_async_copy(src, dst, fetch_sem.at[k]) for k, (src, dst) in enumerate((
        (w, w_out.at[pl.ds(0, shard_rows)]), (m, m_out.at[pl.ds(0, shard_rows)]),
        (v.at[pl.ds(0, ahead)], v_part), (mask.at[pl.ds(0, ahead)], mask_part)))]

    def fetch(i, size):
        at = pl.ds(pl.multiple_of(i * CHUNK_ROWS, 8), size // LANES)
        return [pltpu.make_async_copy(src.at[at], dst.at[at], fetch_sem.at[k])
                for k, (src, dst) in enumerate(((w, w_out), (m, m_out)))]

    barrier = pltpu.get_barrier_semaphore()
    acc[...] = jnp.zeros_like(acc)

    def loads(i, size):
        slot = i % SLOTS
        out = []
        for b, block in enumerate(blocks):
            src = pl.multiple_of(block * shard_len + i * full, LANES)
            out.append(pltpu.make_async_copy(
                grad.at[:, pl.ds(src, size)], own.at[slot, b, :, pl.ds(0, size)], own_sem.at[slot, b]))
        return out

    def swaps(i, size):
        slot = i % SLOTS
        out = []
        for b, block in enumerate(blocks):
            src = pl.multiple_of((block + shift) * shard_len + i * full, LANES)
            out.append(remote(
                grad.at[:, pl.ds(src, size)], other.at[slot, b, :, pl.ds(0, size)],
                part_ssem.at[slot, b], part_rsem.at[slot, b], part))
        return out

    def for_size(i, do):
        @pl.when(i < chunks - 1)
        def _():
            do(full)

        @pl.when(i == chunks - 1)
        def _():
            do(tail)

    def hops(q, planes):
        slot = q % SLOTS
        return (remote(x_send.at[slot, planes], x_recv.at[slot, planes], x_ssem.at[slot], x_rsem.at[slot], along_x),
                remote(y_send.at[slot, planes], y_recv.at[slot, planes], y_ssem.at[slot], y_rsem.at[slot], along_y))

    def for_planes(q, do):
        @pl.when((q >= 1) & (q < 3))
        def _():
            do(pl.ds(0, 2))

        @pl.when((q >= 3) & (q <= chunks))
        def _():
            do(pl.ds(0, 3))

        @pl.when((q > chunks) & (q <= chunks + 2))
        def _():
            do(pl.ds(2, 1))

    staged = []
    for b, block in enumerate(blocks):
        src = pl.multiple_of((block + shift) * shard_len, LANES)
        staged.append(pltpu.make_async_copy(grad.at[:, pl.ds(src, full)], head.at[b], head_sem.at[b]))
    for cp in staged + loads(0, full):
        cp.start()
    for peer in (part, along_x, along_y):
        pl.semaphore_signal(barrier, inc=1, device_id=(peer,), device_id_type=MESH)
    for cp in staged:
        cp.wait()
    pl.semaphore_wait(barrier, 3)
    for b in range(len(blocks)):
        remote(head.at[b], other.at[0, b], part_ssem.at[0, b], part_rsem.at[0, b], part).start()

    def begin(i):
        def do(size):
            for cp in swaps(i, size) + loads(i, size) + fetch(i, size):
                cp.start()

        for_size(i, do)

    def pair_sums(j):
        def do(size):
            for cp in loads(j, size) + swaps(j, size):
                cp.wait()

        for_size(j, do)
        slot = j % SLOTS
        out = (j + 1) % SLOTS
        kept = j % (SLOTS + 1)

        def tile(t, carry):
            for half in range(2):
                row = pl.multiple_of(t * 8, 8)
                col = pl.multiple_of((t + half * (HALF_ROWS // 8)) * 8 * LANES, 8 * LANES)

                def pair(b):
                    a = own[slot, b, :, pl.ds(col, 8 * LANES)].astype(jnp.float32)
                    o = other[slot, b, :, pl.ds(col, 8 * LANES)].astype(jnp.float32)
                    return (a + o).reshape(8, LANES)

                mine[kept, half, pl.ds(row, 8)] = pair(0)
                if half == 0:
                    x_send[out, 0, pl.ds(row, 8)] = pair(1)
                    y_keep[slot, pl.ds(row, 8)] = pair(2)
                    x_send[out, 1, pl.ds(row, 8)] = pair(3)
                else:
                    x_keep[slot, pl.ds(row, 8)] = pair(1)
                    y_send[out, 0, pl.ds(row, 8)] = pair(2)
                    y_send[out, 1, pl.ds(row, 8)] = pair(3)
            return carry

        lax.fori_loop(0, HALF_ROWS // 8, tile, 0)

    def wait_for(q):
        def do(planes):
            for cp in hops(q, planes):
                cp.wait()

        for_planes(q, do)

    def relay(j):
        slot = j % SLOTS
        got = (j + 1) % SLOTS
        out = (j + 3) % SLOTS
        kept = j % (SLOTS + 1)
        x_send[out, 2] = x_keep[slot] + y_recv[got, 1]
        y_send[out, 2] = y_keep[slot] + x_recv[got, 1]
        mine[kept, 0] = mine[kept, 0] + x_recv[got, 0]
        mine[kept, 1] = mine[kept, 1] + y_recv[got, 0]

    def finish(j):
        got = (j + 3) % SLOTS
        kept = j % (SLOTS + 1)
        base = j * CHUNK_ROWS
        left = shard_rows - j * CHUNK_ROWS
        rows = lax.broadcasted_iota(jnp.int32, (8, LANES), 0)

        def tile(t, total):
            row = pl.multiple_of(t * 8, 8)
            top = (mine[kept, 0, pl.ds(row, 8)] + y_recv[got, 2, pl.ds(row, 8)]) * 0.125
            low = (mine[kept, 1, pl.ds(row, 8)] + x_recv[got, 2, pl.ds(row, 8)]) * 0.125
            g_out[pl.ds(pl.multiple_of(base + t * 8, 8), 8)] = top
            g_out[pl.ds(pl.multiple_of(base + HALF_ROWS + t * 8, 8), 8)] = low
            total = total + jnp.where(rows + t * 8 < left, top * top, 0.0)
            return total + jnp.where(rows + (HALF_ROWS + t * 8) < left, low * low, 0.0)

        acc[...] += lax.fori_loop(0, HALF_ROWS // 8, tile, jnp.zeros((8, LANES), jnp.float32))

    def step(i, carry):
        @pl.when((i >= 1) & (i < chunks))
        def _():
            begin(i)

        @pl.when((i >= 1) & (i <= chunks))
        def _():
            pair_sums(i - 1)

        wait_for(i - 2)

        @pl.when((i >= 3) & (i <= chunks + 2))
        def _():
            relay(i - 3)

        @pl.when(i >= 5)
        def _():
            finish(i - 5)

        def go(planes):
            for cp in hops(i, planes):
                cp.start()

        for_planes(i, go)

        @pl.when(i == 4)
        def _():
            for cp in fetches[2:] + fetch(0, full):
                cp.start()

        return carry

    lax.fori_loop(0, chunks + 5, step, 0)
    norm_recv[me] = acc[...]

    def shares(peer, k):
        return remote(acc, norm_recv.at[me], n_ssem.at[k], n_rsem.at[me], peer)

    for k, peer in enumerate(others):
        shares(peer, k).start()
    for cp in fetches:
        cp.wait()
    for k, peer in enumerate(others):
        shares(peer, k).wait_send()
        remote(acc, norm_recv.at[peer], n_ssem.at[k], n_rsem.at[peer], peer).wait_recv()
    total = norm_recv[0]
    for k in range(1, num_dev):
        total = total + norm_recv[k]
    norm = jnp.broadcast_to(jnp.sqrt(jnp.sum(total, keepdims=True)), norm_out.shape)
    norm_out[...] = norm
    coef = jnp.minimum(1.0, 1.0 / (norm[0:1] + CLIP_EPS))
    rate = lr[0]

    def part_tile(t, carry):
        at = pl.ds(pl.multiple_of(t * TILE_ROWS, 8), TILE_ROWS)
        new, _, _ = adamw_tile(g_out[at], w_out[at], m_out[at], v_part[at], mask_part[at], coef, rate)
        pack_tile(packed, t, new)
        return carry

    lax.fori_loop(0, ahead // TILE_ROWS, part_tile, 0)


def reduce_scatter(lr, grad_row, w, m, v, mask, num_dev):
    f32, bf16 = jnp.float32, jnp.bfloat16
    shard_rows = w.shape[0]
    chunks = -(-shard_rows // CHUNK_ROWS)
    ahead = PARTS[0] * ADAM_ROWS
    vm, dma = pltpu.VMEM, pltpu.SemaphoreType.DMA
    three = (SLOTS, 3, HALF_ROWS, LANES)
    one = (SLOTS, HALF_ROWS, LANES)
    raw = (SLOTS, 4, 1, CHUNK_ROWS * LANES)
    state = vm((chunks * CHUNK_ROWS, LANES), f32)
    return pl.pallas_call(
        functools.partial(reduce_kernel, shard_rows),
        out_shape=(state, state, state, vm((ahead // 4, 4, LANES), bf16), jax.ShapeDtypeStruct((8, LANES), f32)),
        in_specs=[pl.BlockSpec(memory_space=pltpu.SMEM)] + [pl.BlockSpec(memory_space=pltpu.HBM)] * 5,
        out_specs=(pl.BlockSpec(memory_space=vm),) * 5,
        scratch_shapes=[
            vm(raw, bf16), vm(raw, bf16), vm(three, f32), vm(three, f32), vm(one, f32), vm(one, f32),
            vm((SLOTS + 1, 2, HALF_ROWS, LANES), f32), vm(three, f32), vm(three, f32), vm((8, LANES), f32),
            vm((num_dev, 8, LANES), f32),
            dma((SLOTS, 4)), dma((SLOTS, 4)), dma((SLOTS, 4)),
            dma((SLOTS,)), dma((SLOTS,)), dma((SLOTS,)), dma((SLOTS,)),
            dma((num_dev - 1,)), dma((num_dev,)),
            vm((ahead, LANES), f32), vm((ahead, LANES), jnp.int32), dma((4,)),
            vm(raw[1:], bf16), dma((4,))],
        compiler_params=pltpu.CompilerParams(collective_id=0, has_side_effects=True,
                                             vmem_limit_bytes=VMEM_LIMIT),
    )(lr, grad_row, w, m, v, mask)


def adamw_kernel(lr, norm, g, w, m, v, mask, *rest):
    w_out, m_out, v_out, packed, norm_out = rest[-5:]
    norm_out[0] = norm[0, 0]
    coef = jnp.minimum(1.0, 1.0 / (norm[0:1] + CLIP_EPS))
    rate = lr[0]

    def tile(t, carry):
        at = pl.ds(pl.multiple_of(t * TILE_ROWS, 8), TILE_ROWS)
        w_out[at], m_out[at], v_out[at] = new, first, second = adamw_tile(
            g[at], w[at], m[at], v[at], mask[at], coef, rate)
        pack_tile(packed, t, new)
        return carry

    lax.fori_loop(0, ADAM_ROWS // TILE_ROWS, tile, 0)


def adamw(first, steps, lr, norm, g, w, m, v, mask, before):
    rows = v.shape[0]
    part_rows = steps * ADAM_ROWS
    block = pl.BlockSpec((ADAM_ROWS, LANES), lambda i: (i + first, 0))
    state = jax.ShapeDtypeStruct((rows, LANES), jnp.float32)
    blind = [pl.BlockSpec(memory_space=pl.ANY)] * len(before)
    return pl.pallas_call(
        adamw_kernel,
        grid=(steps,),
        out_shape=(state, state, state, jax.ShapeDtypeStruct((part_rows // 4, 4, LANES), jnp.bfloat16),
                   jax.ShapeDtypeStruct((1,), jnp.float32)),
        in_specs=[pl.BlockSpec(memory_space=pltpu.SMEM),
                  pl.BlockSpec((8, LANES), lambda i: (0, 0)),
                  block, block, block, block, block] + blind,
        out_specs=(block, block, block, pl.BlockSpec((ADAM_ROWS // 4, 4, LANES), lambda i: (i, 0, 0)),
                   pl.BlockSpec(memory_space=pltpu.SMEM)),
        input_output_aliases={7 + k: k for k in range(len(before))},
        compiler_params=pltpu.CompilerParams(vmem_limit_bytes=VMEM_LIMIT),
        cost_estimate=pl.CostEstimate(flops=30 * part_rows * LANES * 40, bytes_accessed=20 * part_rows * LANES, transcendentals=0),
    )(lr, norm, stay(g), stay(w), stay(m), v, mask, *before)


def store_kernel(spots, direct, *refs):
    count = len(spots)
    pieces = refs[:count]
    params, buf, in_sem, out_sem = refs[-4:]
    me, part, along_x, along_y = places()
    diag = along_x + along_y - me
    shift = part - me
    blocks = (me, along_x, along_y, diag, me + shift, along_x + shift, along_y + shift, diag + shift)
    loads, stores = [], []
    for k, (which, start, size, grains) in enumerate(spots):
        dst = params.at[pl.ds(blocks[which] * grains + start, size)]
        src = pieces[k].at[pl.ds(0, size)]
        if not direct:
            loads.append(pltpu.make_async_copy(src, buf.at[k, pl.ds(0, size)], in_sem.at[k]))
            src = buf.at[k, pl.ds(0, size)]
        stores.append(pltpu.make_async_copy(src, dst, out_sem.at[k]))
    for cp in loads:
        cp.start()
    for k, out in enumerate(stores):
        if not direct:
            loads[k].wait()
        out.start()
    for out in stores:
        out.wait()


def store(pieces, spots, before, num_dev, grains, direct):
    count = len(pieces)
    if direct:
        pieces = [stay(p) for p in pieces]
    hbm = pl.BlockSpec(memory_space=pltpu.HBM)
    room = max(p.shape[0] for p in pieces)
    moved = sum(p.size for p in pieces)
    return pl.pallas_call(
        functools.partial(store_kernel, [(which, start, min(p.shape[0], grains - start), grains)
                                         for p, (which, start) in zip(pieces, spots)], direct),
        out_shape=jax.ShapeDtypeStruct((num_dev * grains, 4, LANES), jnp.bfloat16),
        in_specs=[pl.BlockSpec(memory_space=pltpu.VMEM) if direct else hbm] * count + [hbm] * len(before),
        out_specs=hbm,
        input_output_aliases={count: 0} if before else {},
        scratch_shapes=[pltpu.VMEM((1, 2, 4, LANES) if direct else (count, room, 4, LANES), jnp.bfloat16),
                        pltpu.SemaphoreType.DMA((count,)), pltpu.SemaphoreType.DMA((count,))],
        compiler_params=pltpu.CompilerParams(vmem_limit_bytes=VMEM_LIMIT),
        cost_estimate=pl.CostEstimate(flops=40 * moved, bytes_accessed=4 * moved, transcendentals=0),
    )(*pieces, *before)


def solution(mesh):
    num_dev = mesh.shape["dp"]
    hop = {"core": [(i, i ^ 1) for i in range(num_dev)], "x": [(i, i ^ 2) for i in range(num_dev)],
           "y": [(i, i ^ 4) for i in range(num_dev)]}

    def local_step(grad_row, master, mom_first, mom_second, decay_mask, learn_rate):
        shard_len = master.shape[0]
        rows = shard_len // LANES
        grains = rows // 4
        flat = lambda a: a.reshape(rows, LANES)

        def send(a, along):
            return lax.ppermute(a, "dp", hop[along])

        def put(pieces, spots, whole, direct=False):
            return (store(pieces, spots, whole, num_dev, grains, direct),)

        v, mask = flat(mom_second), flat(decay_mask)
        g, w, m, packed, norm = reduce_scatter(
            learn_rate, grad_row, flat(master), flat(mom_first), v, mask, num_dev)
        packs = {0: packed}
        state = ()
        whole = ()
        firsts = [sum(PARTS[:p]) for p in range(len(PARTS))]
        for p in (*range(1, len(PARTS)), 0):
            *state, packed, grad_norm = adamw(firsts[p], PARTS[p], learn_rate, norm, g, w, m, v, mask, state)
            packs.setdefault(p, packed)
        arrived = [(packs[p], send(packs[p], "x"), send(packs[p], "y"),
                    send(packs[p], "core")) for p in range(len(PARTS))]
        starts = [first * ADAM_ROWS // 4 for first in firsts]
        far = []
        for p, (packed, from_x, from_y, from_core) in enumerate(arrived):
            far.append(send(from_x, "y") if p % 2 == 0 else send(from_y, "x"))
            pieces = [packed, from_x, from_y, from_core, send(from_x, "core"), send(from_y, "core")]
            whole = put(pieces, [(k, starts[p]) for k in (0, 1, 2, 4, 5, 6)], whole)
        for p in range(0, len(PARTS), 2):
            pieces, spots = [], []
            for q in (p, p + 1):
                pieces += [far[q], send(far[q], "core")]
                spots += [(3, starts[q]), (7, starts[q])]
            whole = put(pieces, spots, whole, p + 2 == len(PARTS))
        new_w, new_m, new_v = state
        params = whole[0].reshape(num_dev * shard_len)
        return (params, new_w.reshape(shard_len), new_m.reshape(shard_len), new_v.reshape(shard_len),
                grad_norm)

    return jax.shard_map(
        local_step, mesh=mesh,
        in_specs=(P("dp", None), P("dp"), P("dp"), P("dp"), P("dp"), P()),
        out_specs=(P(), P("dp"), P("dp"), P("dp"), P()), check_vma=False)
```

```python
import functools

import jax
import jax.numpy as jnp
from jax import lax
from jax.experimental import pallas as pl
from jax.experimental.pallas import tpu as pltpu
from jax.sharding import PartitionSpec as P


BETA_FIRST = 0.9
BETA_SECOND = 0.95
ADAM_EPS = 1e-8
CLIP_EPS = 1e-6
WEIGHT_DECAY = 0.1
ADAM_STEP = 10

MESH = pl.DeviceIdType.MESH
LANES = 128
CHUNK_ROWS = 384
HALF_ROWS = CHUNK_ROWS // 2
SLOTS = 4
VMEM_LIMIT = 20 << 20
ADAM_ROWS = 960
PARTS = (2, 3, 4, 4, 4, 4, 2, 1, 1, 1)
TILE_ROWS = 120


def places():
    me = lax.axis_index("dp")
    core = me % 2
    part = me + 1 - 2 * core
    along_x = me + 2 - 4 * ((me // 2) % 2)
    along_y = me + 4 - 8 * (me // 4)
    return me, part, along_x, along_y


def stay(array):
    return pltpu.with_memory_space_constraint(array, pltpu.VMEM)


def remote(src, dst, send_sem, recv_sem, device):
    return pltpu.make_async_remote_copy(
        src_ref=src, dst_ref=dst, send_sem=send_sem, recv_sem=recv_sem,
        device_id=(device,), device_id_type=MESH)


def adamw_tile(g, w, m, v, mask, coef, rate):
    h = g * coef
    first = BETA_FIRST * m + (1.0 - BETA_FIRST) * h
    second = BETA_SECOND * v + (1.0 - BETA_SECOND) * h * h
    step_dir = (first * (1.0 / (1.0 - BETA_FIRST ** ADAM_STEP))) / (
        jnp.sqrt(second * (1.0 / (1.0 - BETA_SECOND ** ADAM_STEP))) + ADAM_EPS)
    new = w - rate * (step_dir + WEIGHT_DECAY * mask.astype(jnp.float32) * w)
    return new, first, second


def chunk_count(shard_rows):
    return 1 + -(-shard_rows // CHUNK_ROWS)


def pack_tile(packed, t, new):
    grains = TILE_ROWS // 4
    packed[pl.ds(pl.multiple_of(t * grains, 2), grains)] = new.reshape(grains, 4, LANES).astype(packed.dtype)


def reduce_kernel(shard_rows, lr, grad, w, m, v, mask, g_out, w_out, m_out, packed, norm_out,
                  own, other, x_send, y_send, x_keep, y_keep, mine, x_recv, y_recv, acc, norm_recv,
                  own_sem, part_ssem, part_rsem, x_ssem, x_rsem, y_ssem, y_rsem, n_ssem, n_rsem,
                  v_part, mask_part, fetch_sem):
    me, part, along_x, along_y = places()
    diag = along_x + along_y - me
    shift = part - me
    blocks = (me, along_x, along_y, diag)
    shard_len = shard_rows * LANES
    full = CHUNK_ROWS * LANES
    edge = full // 2
    chunks = chunk_count(shard_rows)
    tail = shard_rows * LANES - edge - (chunks - 2) * full
    num_dev = grad.shape[1] // shard_len
    others = [(me + k) % num_dev for k in range(1, num_dev)]
    ahead = v_part.shape[0]
    fetches = [pltpu.make_async_copy(src, dst, fetch_sem.at[k]) for k, (src, dst) in enumerate((
        (w, w_out.at[pl.ds(0, shard_rows)]), (m, m_out.at[pl.ds(0, shard_rows)]),
        (v.at[pl.ds(0, ahead)], v_part), (mask.at[pl.ds(0, ahead)], mask_part)))]

    barrier = pltpu.get_barrier_semaphore()
    acc[...] = jnp.zeros_like(acc)

    def row_of(i):
        return jnp.maximum(i * CHUNK_ROWS - HALF_ROWS, 0)

    def half_of(i):
        return jnp.where((i == 0) | (i == chunks - 1), HALF_ROWS // 2, HALF_ROWS)

    def loads(i, size):
        slot = i % SLOTS
        out = []
        for b, block in enumerate(blocks):
            src = pl.multiple_of(block * shard_len + row_of(i) * LANES, LANES)
            out.append(pltpu.make_async_copy(
                grad.at[:, pl.ds(src, size)], own.at[slot, b, :, pl.ds(0, size)], own_sem.at[slot, b]))
        return out

    def swaps(i, size):
        slot = i % SLOTS
        out = []
        for b, block in enumerate(blocks):
            src = pl.multiple_of((block + shift) * shard_len + row_of(i) * LANES, LANES)
            out.append(remote(
                grad.at[:, pl.ds(src, size)], other.at[slot, b, :, pl.ds(0, size)],
                part_ssem.at[slot, b], part_rsem.at[slot, b], part))
        return out

    def for_size(i, do):
        @pl.when(i == 0)
        def _():
            do(edge)

        @pl.when((i >= 1) & (i < chunks - 1))
        def _():
            do(full)

        @pl.when(i == chunks - 1)
        def _():
            do(tail)

    def hops(q, pieces):
        slot = q % SLOTS
        out = []
        for k, (plane, planes, rows) in enumerate(pieces):
            at = (slot, pl.ds(plane, planes), pl.ds(0, rows))
            out.append(remote(x_send.at[at], x_recv.at[at], x_ssem.at[slot, k], x_rsem.at[slot, k], along_x))
            out.append(remote(y_send.at[at], y_recv.at[at], y_ssem.at[slot, k], y_rsem.at[slot, k], along_y))
        return out

    short = HALF_ROWS // 2

    def for_pieces(q, do):
        for test, pieces in (
                (q == 1, [(0, 2, short)]),
                (q == 2, [(0, 2, HALF_ROWS)]),
                (q == 3, [(0, 2, HALF_ROWS), (2, 1, short)]),
                ((q > 3) & (q < chunks), [(0, 3, HALF_ROWS)]),
                (q == chunks, [(0, 2, short), (2, 1, HALF_ROWS)]),
                (q == chunks + 1, [(2, 1, HALF_ROWS)]),
                (q == chunks + 2, [(2, 1, short)])):
            pl.when(test)(functools.partial(do, pieces))

    for cp in loads(0, edge):
        cp.start()
    for peer in (part, along_x, along_y):
        pl.semaphore_signal(barrier, inc=1, device_id=(peer,), device_id_type=MESH)
    pl.semaphore_wait(barrier, 3)
    for cp in swaps(0, edge):
        cp.start()

    def begin(i):
        def do(size):
            for cp in swaps(i, size) + loads(i, size):
                cp.start()

        for_size(i, do)

    def pair_sums(j):
        def do(size):
            for cp in loads(j, size) + swaps(j, size):
                cp.wait()

        for_size(j, do)
        slot = j % SLOTS
        out = (j + 1) % SLOTS
        kept = j % (SLOTS + 1)
        tiles = half_of(j) // 8

        def tile(t, carry):
            for half in range(2):
                row = pl.multiple_of(t * 8, 8)
                col = pl.multiple_of((t + half * tiles) * 8 * LANES, 8 * LANES)

                def pair(b):
                    a = own[slot, b, :, pl.ds(col, 8 * LANES)].astype(jnp.float32)
                    o = other[slot, b, :, pl.ds(col, 8 * LANES)].astype(jnp.float32)
                    return (a + o).reshape(8, LANES)

                mine[kept, half, pl.ds(row, 8)] = pair(0)
                if half == 0:
                    x_send[out, 0, pl.ds(row, 8)] = pair(1)
                    y_keep[slot, pl.ds(row, 8)] = pair(2)
                    x_send[out, 1, pl.ds(row, 8)] = pair(3)
                else:
                    x_keep[slot, pl.ds(row, 8)] = pair(1)
                    y_send[out, 0, pl.ds(row, 8)] = pair(2)
                    y_send[out, 1, pl.ds(row, 8)] = pair(3)
            return carry

        lax.fori_loop(0, tiles, tile, 0)

    def wait_for(q):
        def do(pieces):
            for cp in hops(q, pieces):
                cp.wait()

        for_pieces(q, do)

    def relay(j):
        slot = j % SLOTS
        got = (j + 1) % SLOTS
        out = (j + 3) % SLOTS
        kept = j % (SLOTS + 1)
        x_send[out, 2] = x_keep[slot] + y_recv[got, 1]
        y_send[out, 2] = y_keep[slot] + x_recv[got, 1]
        mine[kept, 0] = mine[kept, 0] + x_recv[got, 0]
        mine[kept, 1] = mine[kept, 1] + y_recv[got, 0]

    def finish(j):
        got = (j + 3) % SLOTS
        kept = j % (SLOTS + 1)
        base = row_of(j)
        half = half_of(j)
        left = shard_rows - base
        rows = lax.broadcasted_iota(jnp.int32, (8, LANES), 0)

        def tile(t, total):
            row = pl.multiple_of(t * 8, 8)
            top = (mine[kept, 0, pl.ds(row, 8)] + y_recv[got, 2, pl.ds(row, 8)]) * 0.125
            low = (mine[kept, 1, pl.ds(row, 8)] + x_recv[got, 2, pl.ds(row, 8)]) * 0.125
            g_out[pl.ds(pl.multiple_of(base + t * 8, 8), 8)] = top
            g_out[pl.ds(pl.multiple_of(base + half + t * 8, 8), 8)] = low
            total = total + jnp.where(rows + t * 8 < left, top * top, 0.0)
            return total + jnp.where(rows + (half + t * 8) < left, low * low, 0.0)

        acc[...] += lax.fori_loop(0, half // 8, tile, jnp.zeros((8, LANES), jnp.float32))

    def step(i, carry):
        @pl.when((i >= 1) & (i < chunks))
        def _():
            begin(i)

        @pl.when((i >= 1) & (i <= chunks))
        def _():
            pair_sums(i - 1)

        wait_for(i - 2)

        @pl.when((i >= 3) & (i <= chunks + 2))
        def _():
            relay(i - 3)

        @pl.when(i >= 5)
        def _():
            finish(i - 5)

        def go(pieces):
            for cp in hops(i, pieces):
                cp.start()

        for_pieces(i, go)

        @pl.when(i == 4)
        def _():
            for cp in fetches:
                cp.start()

        return carry

    lax.fori_loop(0, chunks + 5, step, 0)
    norm_recv[me] = acc[...]

    def shares(peer, k):
        return remote(acc, norm_recv.at[me], n_ssem.at[k], n_rsem.at[me], peer)

    for k, peer in enumerate(others):
        shares(peer, k).start()
    for cp in fetches:
        cp.wait()
    for k, peer in enumerate(others):
        shares(peer, k).wait_send()
        remote(acc, norm_recv.at[peer], n_ssem.at[k], n_rsem.at[peer], peer).wait_recv()
    total = norm_recv[0]
    for k in range(1, num_dev):
        total = total + norm_recv[k]
    norm = jnp.broadcast_to(jnp.sqrt(jnp.sum(total, keepdims=True)), norm_out.shape)
    norm_out[...] = norm
    coef = jnp.minimum(1.0, 1.0 / (norm[0:1] + CLIP_EPS))
    rate = lr[0]

    def part_tile(t, carry):
        at = pl.ds(pl.multiple_of(t * TILE_ROWS, 8), TILE_ROWS)
        new, _, _ = adamw_tile(g_out[at], w_out[at], m_out[at], v_part[at], mask_part[at], coef, rate)
        pack_tile(packed, t, new)
        return carry

    lax.fori_loop(0, ahead // TILE_ROWS, part_tile, 0)


def reduce_scatter(lr, grad_row, w, m, v, mask, num_dev):
    f32, bf16 = jnp.float32, jnp.bfloat16
    shard_rows = w.shape[0]
    padded = (chunk_count(shard_rows) - 1) * CHUNK_ROWS
    ahead = PARTS[0] * ADAM_ROWS
    vm, dma = pltpu.VMEM, pltpu.SemaphoreType.DMA
    three = (SLOTS, 3, HALF_ROWS, LANES)
    one = (SLOTS, HALF_ROWS, LANES)
    raw = (SLOTS, 4, 1, CHUNK_ROWS * LANES)
    state = vm((padded, LANES), f32)
    return pl.pallas_call(
        functools.partial(reduce_kernel, shard_rows),
        out_shape=(state, state, state, vm((ahead // 4, 4, LANES), bf16), jax.ShapeDtypeStruct((8, LANES), f32)),
        in_specs=[pl.BlockSpec(memory_space=pltpu.SMEM)] + [pl.BlockSpec(memory_space=pltpu.HBM)] * 5,
        out_specs=(pl.BlockSpec(memory_space=vm),) * 5,
        scratch_shapes=[
            vm(raw, bf16), vm(raw, bf16), vm(three, f32), vm(three, f32), vm(one, f32), vm(one, f32),
            vm((SLOTS + 1, 2, HALF_ROWS, LANES), f32), vm(three, f32), vm(three, f32), vm((8, LANES), f32),
            vm((num_dev, 8, LANES), f32),
            dma((SLOTS, 4)), dma((SLOTS, 4)), dma((SLOTS, 4)),
            dma((SLOTS, 2)), dma((SLOTS, 2)), dma((SLOTS, 2)), dma((SLOTS, 2)),
            dma((num_dev - 1,)), dma((num_dev,)),
            vm((ahead, LANES), f32), vm((ahead, LANES), jnp.int32), dma((4,))],
        compiler_params=pltpu.CompilerParams(collective_id=0, has_side_effects=True,
                                             vmem_limit_bytes=VMEM_LIMIT),
    )(lr, grad_row, w, m, v, mask)


def adamw_kernel(lr, norm, g, w, m, v, mask, *rest):
    w_out, m_out, v_out, packed, norm_out = rest[-5:]
    norm_out[0] = norm[0, 0]
    coef = jnp.minimum(1.0, 1.0 / (norm[0:1] + CLIP_EPS))
    rate = lr[0]

    def tile(t, carry):
        at = pl.ds(pl.multiple_of(t * TILE_ROWS, 8), TILE_ROWS)
        w_out[at], m_out[at], v_out[at] = new, first, second = adamw_tile(
            g[at], w[at], m[at], v[at], mask[at], coef, rate)
        pack_tile(packed, t, new)
        return carry

    lax.fori_loop(0, ADAM_ROWS // TILE_ROWS, tile, 0)


def adamw(first, steps, lr, norm, g, w, m, v, mask, before):
    rows = v.shape[0]
    part_rows = steps * ADAM_ROWS
    block = pl.BlockSpec((ADAM_ROWS, LANES), lambda i: (i + first, 0))
    state = jax.ShapeDtypeStruct((rows, LANES), jnp.float32)
    blind = [pl.BlockSpec(memory_space=pl.ANY)] * len(before)
    return pl.pallas_call(
        adamw_kernel,
        grid=(steps,),
        out_shape=(state, state, state, jax.ShapeDtypeStruct((part_rows // 4, 4, LANES), jnp.bfloat16),
                   jax.ShapeDtypeStruct((1,), jnp.float32)),
        in_specs=[pl.BlockSpec(memory_space=pltpu.SMEM),
                  pl.BlockSpec((8, LANES), lambda i: (0, 0)),
                  block, block, block, block, block] + blind,
        out_specs=(block, block, block, pl.BlockSpec((ADAM_ROWS // 4, 4, LANES), lambda i: (i, 0, 0)),
                   pl.BlockSpec(memory_space=pltpu.SMEM)),
        input_output_aliases={7 + k: k for k in range(len(before))},
        compiler_params=pltpu.CompilerParams(vmem_limit_bytes=VMEM_LIMIT),
        cost_estimate=pl.CostEstimate(flops=30 * part_rows * LANES * 40, bytes_accessed=20 * part_rows * LANES, transcendentals=0),
    )(lr, norm, stay(g), stay(w), stay(m), v, mask, *before)


def store_kernel(spots, direct, *refs):
    count = len(spots)
    pieces = refs[:count]
    params, buf, in_sem, out_sem = refs[-4:]
    me, part, along_x, along_y = places()
    diag = along_x + along_y - me
    shift = part - me
    blocks = (me, along_x, along_y, diag, me + shift, along_x + shift, along_y + shift, diag + shift)
    loads, stores = [], []
    for k, (which, start, size, grains) in enumerate(spots):
        dst = params.at[pl.ds(blocks[which] * grains + start, size)]
        src = pieces[k].at[pl.ds(0, size)]
        if not direct:
            loads.append(pltpu.make_async_copy(src, buf.at[k, pl.ds(0, size)], in_sem.at[k]))
            src = buf.at[k, pl.ds(0, size)]
        stores.append(pltpu.make_async_copy(src, dst, out_sem.at[k]))
    for cp in loads:
        cp.start()
    for k, out in enumerate(stores):
        if not direct:
            loads[k].wait()
        out.start()
    for out in stores:
        out.wait()


def store(pieces, spots, before, num_dev, grains, direct):
    count = len(pieces)
    if direct:
        pieces = [stay(p) for p in pieces]
    hbm = pl.BlockSpec(memory_space=pltpu.HBM)
    room = max(p.shape[0] for p in pieces)
    moved = sum(p.size for p in pieces)
    return pl.pallas_call(
        functools.partial(store_kernel, [(which, start, min(p.shape[0], grains - start), grains)
                                         for p, (which, start) in zip(pieces, spots)], direct),
        out_shape=jax.ShapeDtypeStruct((num_dev * grains, 4, LANES), jnp.bfloat16),
        in_specs=[pl.BlockSpec(memory_space=pltpu.VMEM) if direct else hbm] * count + [hbm] * len(before),
        out_specs=hbm,
        input_output_aliases={count: 0} if before else {},
        scratch_shapes=[pltpu.VMEM((1, 2, 4, LANES) if direct else (count, room, 4, LANES), jnp.bfloat16),
                        pltpu.SemaphoreType.DMA((count,)), pltpu.SemaphoreType.DMA((count,))],
        compiler_params=pltpu.CompilerParams(vmem_limit_bytes=VMEM_LIMIT),
        cost_estimate=pl.CostEstimate(flops=40 * moved, bytes_accessed=4 * moved, transcendentals=0),
    )(*pieces, *before)


def solution(mesh):
    num_dev = mesh.shape["dp"]
    hop = {"core": [(i, i ^ 1) for i in range(num_dev)], "x": [(i, i ^ 2) for i in range(num_dev)],
           "y": [(i, i ^ 4) for i in range(num_dev)]}

    def local_step(grad_row, master, mom_first, mom_second, decay_mask, learn_rate):
        shard_len = master.shape[0]
        rows = shard_len // LANES
        grains = rows // 4
        flat = lambda a: a.reshape(rows, LANES)

        def send(a, along):
            return lax.ppermute(a, "dp", hop[along])

        def put(pieces, spots, whole, direct=False):
            return (store(pieces, spots, whole, num_dev, grains, direct),)

        v, mask = flat(mom_second), flat(decay_mask)
        g, w, m, packed, norm = reduce_scatter(
            learn_rate, grad_row, flat(master), flat(mom_first), v, mask, num_dev)
        packs = {0: packed}
        state = ()
        whole = ()
        firsts = [sum(PARTS[:p]) for p in range(len(PARTS))]
        for p in (*range(1, len(PARTS)), 0):
            *state, packed, grad_norm = adamw(firsts[p], PARTS[p], learn_rate, norm, g, w, m, v, mask, state)
            packs.setdefault(p, packed)
        arrived = [(packs[p], send(packs[p], "x"), send(packs[p], "y"),
                    send(packs[p], "core")) for p in range(len(PARTS))]
        starts = [first * ADAM_ROWS // 4 for first in firsts]
        far = []
        for p, (packed, from_x, from_y, from_core) in enumerate(arrived):
            far.append(send(from_x, "y") if p % 2 == 0 else send(from_y, "x"))
            pieces = [packed, from_x, from_y, from_core, send(from_x, "core"), send(from_y, "core")]
            whole = put(pieces, [(k, starts[p]) for k in (0, 1, 2, 4, 5, 6)], whole)
        pieces, spots = [], []
        for p in range(0, len(PARTS), 2):
            for q in (p, p + 1):
                pieces += [far[q], send(far[q], "core")]
                spots += [(3, starts[q]), (7, starts[q])]
            if p + 4 != len(PARTS):
                whole = put(pieces, spots, whole, p + 2 == len(PARTS))
                pieces, spots = [], []
        new_w, new_m, new_v = state
        params = whole[0].reshape(num_dev * shard_len)
        return (params, new_w.reshape(shard_len), new_m.reshape(shard_len), new_v.reshape(shard_len),
                grad_norm)

    return jax.shard_map(
        local_step, mesh=mesh,
        in_specs=(P("dp", None), P("dp"), P("dp"), P("dp"), P("dp"), P()),
        out_specs=(P(), P("dp"), P("dp"), P("dp"), P()), check_vma=False)
```

```python
import functools

import jax
import jax.numpy as jnp
from jax import lax
from jax.experimental import pallas as pl
from jax.experimental.pallas import tpu as pltpu
from jax.sharding import PartitionSpec as P


BETA_FIRST = 0.9
BETA_SECOND = 0.95
ADAM_EPS = 1e-8
CLIP_EPS = 1e-6
WEIGHT_DECAY = 0.1
ADAM_STEP = 10

MESH = pl.DeviceIdType.MESH
LANES = 128
CHUNK_ROWS = 480
HALF_ROWS = CHUNK_ROWS // 2
SLOTS = 4
VMEM_LIMIT = 20 << 20
ADAM_ROWS = 480
PARTS = (3, 5, 8, 8, 8, 7, 4, 3, 3, 3)
TILE_ROWS = 120


def places():
    me = lax.axis_index("dp")
    core = me % 2
    part = me + 1 - 2 * core
    along_x = me + 2 - 4 * ((me // 2) % 2)
    along_y = me + 4 - 8 * (me // 4)
    return me, part, along_x, along_y


def stay(array):
    return pltpu.with_memory_space_constraint(array, pltpu.VMEM)


def remote(src, dst, send_sem, recv_sem, device):
    return pltpu.make_async_remote_copy(
        src_ref=src, dst_ref=dst, send_sem=send_sem, recv_sem=recv_sem,
        device_id=(device,), device_id_type=MESH)


def adamw_tile(g, w, m, v, mask, coef, rate):
    h = g * coef
    first = BETA_FIRST * m + (1.0 - BETA_FIRST) * h
    second = BETA_SECOND * v + (1.0 - BETA_SECOND) * h * h
    step_dir = (first * (1.0 / (1.0 - BETA_FIRST ** ADAM_STEP))) / (
        jnp.sqrt(second * (1.0 / (1.0 - BETA_SECOND ** ADAM_STEP))) + ADAM_EPS)
    new = w - rate * (step_dir + WEIGHT_DECAY * mask.astype(jnp.float32) * w)
    return new, first, second


def chunk_count(shard_rows):
    return 1 + -(-shard_rows // CHUNK_ROWS)


def pack_tile(packed, t, new):
    grains = TILE_ROWS // 4
    packed[pl.ds(pl.multiple_of(t * grains, 2), grains)] = new.reshape(grains, 4, LANES).astype(packed.dtype)


def reduce_kernel(shard_rows, lr, grad, w, m, v, mask, g_out, w_out, m_out, packed, norm_out,
                  own, other, x_send, y_send, x_keep, y_keep, mine, x_recv, y_recv, acc, norm_recv,
                  own_sem, part_ssem, part_rsem, x_ssem, x_rsem, y_ssem, y_rsem, n_ssem, n_rsem,
                  v_part, mask_part, fetch_sem):
    me, part, along_x, along_y = places()
    diag = along_x + along_y - me
    shift = part - me
    blocks = (me, along_x, along_y, diag)
    shard_len = shard_rows * LANES
    full = CHUNK_ROWS * LANES
    edge = full // 2
    chunks = chunk_count(shard_rows)
    tail = shard_rows * LANES - edge - (chunks - 2) * full
    num_dev = grad.shape[1] // shard_len
    others = [(me + k) % num_dev for k in range(1, num_dev)]
    ahead = v_part.shape[0]
    fetches = [pltpu.make_async_copy(src, dst, fetch_sem.at[k]) for k, (src, dst) in enumerate((
        (w, w_out.at[pl.ds(0, shard_rows)]), (m, m_out.at[pl.ds(0, shard_rows)]),
        (v.at[pl.ds(0, ahead)], v_part), (mask.at[pl.ds(0, ahead)], mask_part)))]

    barrier = pltpu.get_barrier_semaphore()
    acc[...] = jnp.zeros_like(acc)

    def row_of(i):
        return jnp.maximum(i * CHUNK_ROWS - HALF_ROWS, 0)

    def half_of(i):
        return jnp.where((i == 0) | (i == chunks - 1), HALF_ROWS // 2, HALF_ROWS)

    def loads(i, size):
        slot = i % SLOTS
        out = []
        for b, block in enumerate(blocks):
            src = pl.multiple_of(block * shard_len + row_of(i) * LANES, LANES)
            out.append(pltpu.make_async_copy(
                grad.at[:, pl.ds(src, size)], own.at[slot, b, :, pl.ds(0, size)], own_sem.at[slot, b]))
        return out

    def swaps(i, size):
        slot = i % SLOTS
        out = []
        for b, block in enumerate(blocks):
            src = pl.multiple_of((block + shift) * shard_len + row_of(i) * LANES, LANES)
            out.append(remote(
                grad.at[:, pl.ds(src, size)], other.at[slot, b, :, pl.ds(0, size)],
                part_ssem.at[slot, b], part_rsem.at[slot, b], part))
        return out

    def for_size(i, do):
        @pl.when(i == 0)
        def _():
            do(edge)

        @pl.when((i >= 1) & (i < chunks - 1))
        def _():
            do(full)

        @pl.when(i == chunks - 1)
        def _():
            do(tail)

    def hops(q, pieces):
        slot = q % SLOTS
        out = []
        for k, (plane, planes, rows) in enumerate(pieces):
            at = (slot, pl.ds(plane, planes), pl.ds(0, rows))
            out.append(remote(x_send.at[at], x_recv.at[at], x_ssem.at[slot, k], x_rsem.at[slot, k], along_x))
            out.append(remote(y_send.at[at], y_recv.at[at], y_ssem.at[slot, k], y_rsem.at[slot, k], along_y))
        return out

    short = HALF_ROWS // 2

    def for_pieces(q, do):
        for test, pieces in (
                (q == 1, [(0, 2, short)]),
                (q == 2, [(0, 2, HALF_ROWS)]),
                (q == 3, [(0, 2, HALF_ROWS), (2, 1, short)]),
                ((q > 3) & (q < chunks), [(0, 3, HALF_ROWS)]),
                (q == chunks, [(0, 2, short), (2, 1, HALF_ROWS)]),
                (q == chunks + 1, [(2, 1, HALF_ROWS)]),
                (q == chunks + 2, [(2, 1, short)])):
            pl.when(test)(functools.partial(do, pieces))

    for cp in loads(0, edge):
        cp.start()
    for peer in (part, along_x, along_y):
        pl.semaphore_signal(barrier, inc=1, device_id=(peer,), device_id_type=MESH)
    pl.semaphore_wait(barrier, 3)
    for cp in swaps(0, edge):
        cp.start()

    def begin(i):
        def do(size):
            for cp in swaps(i, size) + loads(i, size):
                cp.start()

        for_size(i, do)

    def pair_sums(j):
        def do(size):
            for cp in loads(j, size) + swaps(j, size):
                cp.wait()

        for_size(j, do)
        slot = j % SLOTS
        out = (j + 1) % SLOTS
        kept = j % (SLOTS + 1)
        tiles = half_of(j) // 8

        def tile(t, carry):
            for half in range(2):
                row = pl.multiple_of(t * 8, 8)
                col = pl.multiple_of((t + half * tiles) * 8 * LANES, 8 * LANES)

                def pair(b):
                    a = own[slot, b, :, pl.ds(col, 8 * LANES)].astype(jnp.float32)
                    o = other[slot, b, :, pl.ds(col, 8 * LANES)].astype(jnp.float32)
                    return (a + o).reshape(8, LANES)

                mine[kept, half, pl.ds(row, 8)] = pair(0)
                if half == 0:
                    x_send[out, 0, pl.ds(row, 8)] = pair(1)
                    y_keep[slot, pl.ds(row, 8)] = pair(2)
                    x_send[out, 1, pl.ds(row, 8)] = pair(3)
                else:
                    x_keep[slot, pl.ds(row, 8)] = pair(1)
                    y_send[out, 0, pl.ds(row, 8)] = pair(2)
                    y_send[out, 1, pl.ds(row, 8)] = pair(3)
            return carry

        lax.fori_loop(0, tiles, tile, 0)

    def wait_for(q):
        def do(pieces):
            for cp in hops(q, pieces):
                cp.wait()

        for_pieces(q, do)

    def relay(j):
        slot = j % SLOTS
        got = (j + 1) % SLOTS
        out = (j + 3) % SLOTS
        kept = j % (SLOTS + 1)
        x_send[out, 2] = x_keep[slot] + y_recv[got, 1]
        y_send[out, 2] = y_keep[slot] + x_recv[got, 1]
        mine[kept, 0] = mine[kept, 0] + x_recv[got, 0]
        mine[kept, 1] = mine[kept, 1] + y_recv[got, 0]

    def finish(j):
        got = (j + 3) % SLOTS
        kept = j % (SLOTS + 1)
        base = row_of(j)
        half = half_of(j)
        left = shard_rows - base
        rows = lax.broadcasted_iota(jnp.int32, (8, LANES), 0)

        def tile(t, total):
            row = pl.multiple_of(t * 8, 8)
            top = (mine[kept, 0, pl.ds(row, 8)] + y_recv[got, 2, pl.ds(row, 8)]) * 0.125
            low = (mine[kept, 1, pl.ds(row, 8)] + x_recv[got, 2, pl.ds(row, 8)]) * 0.125
            g_out[pl.ds(pl.multiple_of(base + t * 8, 8), 8)] = top
            g_out[pl.ds(pl.multiple_of(base + half + t * 8, 8), 8)] = low
            total = total + jnp.where(rows + t * 8 < left, top * top, 0.0)
            return total + jnp.where(rows + (half + t * 8) < left, low * low, 0.0)

        acc[...] += lax.fori_loop(0, half // 8, tile, jnp.zeros((8, LANES), jnp.float32))

    def step(i, carry):
        @pl.when((i >= 1) & (i < chunks))
        def _():
            begin(i)

        @pl.when((i >= 1) & (i <= chunks))
        def _():
            pair_sums(i - 1)

        wait_for(i - 2)

        @pl.when((i >= 3) & (i <= chunks + 2))
        def _():
            relay(i - 3)

        @pl.when(i >= 5)
        def _():
            finish(i - 5)

        def go(pieces):
            for cp in hops(i, pieces):
                cp.start()

        for_pieces(i, go)

        @pl.when(i == 4)
        def _():
            for cp in fetches:
                cp.start()

        return carry

    lax.fori_loop(0, chunks + 5, step, 0)
    norm_recv[me] = acc[...]

    def shares(peer, k):
        return remote(acc, norm_recv.at[me], n_ssem.at[k], n_rsem.at[me], peer)

    for k, peer in enumerate(others):
        shares(peer, k).start()
    for cp in fetches:
        cp.wait()
    for k, peer in enumerate(others):
        shares(peer, k).wait_send()
        remote(acc, norm_recv.at[peer], n_ssem.at[k], n_rsem.at[peer], peer).wait_recv()
    total = norm_recv[0]
    for k in range(1, num_dev):
        total = total + norm_recv[k]
    norm = jnp.broadcast_to(jnp.sqrt(jnp.sum(total, keepdims=True)), norm_out.shape)
    norm_out[...] = norm
    coef = jnp.minimum(1.0, 1.0 / (norm[0:1] + CLIP_EPS))
    rate = lr[0]

    def part_tile(t, carry):
        at = pl.ds(pl.multiple_of(t * TILE_ROWS, 8), TILE_ROWS)
        new, _, _ = adamw_tile(g_out[at], w_out[at], m_out[at], v_part[at], mask_part[at], coef, rate)
        pack_tile(packed, t, new)
        return carry

    lax.fori_loop(0, ahead // TILE_ROWS, part_tile, 0)


def reduce_scatter(lr, grad_row, w, m, v, mask, num_dev):
    f32, bf16 = jnp.float32, jnp.bfloat16
    shard_rows = w.shape[0]
    padded = (chunk_count(shard_rows) - 1) * CHUNK_ROWS
    ahead = PARTS[0] * ADAM_ROWS
    vm, dma = pltpu.VMEM, pltpu.SemaphoreType.DMA
    three = (SLOTS, 3, HALF_ROWS, LANES)
    one = (SLOTS, HALF_ROWS, LANES)
    raw = (SLOTS, 4, 1, CHUNK_ROWS * LANES)
    state = vm((padded, LANES), f32)
    return pl.pallas_call(
        functools.partial(reduce_kernel, shard_rows),
        out_shape=(state, state, state, vm((ahead // 4, 4, LANES), bf16), jax.ShapeDtypeStruct((8, LANES), f32)),
        in_specs=[pl.BlockSpec(memory_space=pltpu.SMEM)] + [pl.BlockSpec(memory_space=pltpu.HBM)] * 5,
        out_specs=(pl.BlockSpec(memory_space=vm),) * 5,
        scratch_shapes=[
            vm(raw, bf16), vm(raw, bf16), vm(three, f32), vm(three, f32), vm(one, f32), vm(one, f32),
            vm((SLOTS + 1, 2, HALF_ROWS, LANES), f32), vm(three, f32), vm(three, f32), vm((8, LANES), f32),
            vm((num_dev, 8, LANES), f32),
            dma((SLOTS, 4)), dma((SLOTS, 4)), dma((SLOTS, 4)),
            dma((SLOTS, 2)), dma((SLOTS, 2)), dma((SLOTS, 2)), dma((SLOTS, 2)),
            dma((num_dev - 1,)), dma((num_dev,)),
            vm((ahead, LANES), f32), vm((ahead, LANES), jnp.int32), dma((4,))],
        compiler_params=pltpu.CompilerParams(collective_id=0, has_side_effects=True,
                                             vmem_limit_bytes=VMEM_LIMIT),
    )(lr, grad_row, w, m, v, mask)


def adamw_kernel(lr, norm, g, w, m, v, mask, *rest):
    w_out, m_out, v_out, packed, norm_out = rest[-5:]
    norm_out[0] = norm[0, 0]
    coef = jnp.minimum(1.0, 1.0 / (norm[0:1] + CLIP_EPS))
    rate = lr[0]

    def tile(t, carry):
        at = pl.ds(pl.multiple_of(t * TILE_ROWS, 8), TILE_ROWS)
        w_out[at], m_out[at], v_out[at] = new, first, second = adamw_tile(
            g[at], w[at], m[at], v[at], mask[at], coef, rate)
        pack_tile(packed, t, new)
        return carry

    lax.fori_loop(0, ADAM_ROWS // TILE_ROWS, tile, 0)


def adamw(first, steps, lr, norm, g, w, m, v, mask, before):
    rows = v.shape[0]
    part_rows = steps * ADAM_ROWS
    block = pl.BlockSpec((ADAM_ROWS, LANES), lambda i: (i + first, 0))
    state = jax.ShapeDtypeStruct((rows, LANES), jnp.float32)
    blind = [pl.BlockSpec(memory_space=pl.ANY)] * len(before)
    return pl.pallas_call(
        adamw_kernel,
        grid=(steps,),
        out_shape=(state, state, state, jax.ShapeDtypeStruct((part_rows // 4, 4, LANES), jnp.bfloat16),
                   jax.ShapeDtypeStruct((1,), jnp.float32)),
        in_specs=[pl.BlockSpec(memory_space=pltpu.SMEM),
                  pl.BlockSpec((8, LANES), lambda i: (0, 0)),
                  block, block, block, block, block] + blind,
        out_specs=(block, block, block, pl.BlockSpec((ADAM_ROWS // 4, 4, LANES), lambda i: (i, 0, 0)),
                   pl.BlockSpec(memory_space=pltpu.SMEM)),
        input_output_aliases={7 + k: k for k in range(len(before))},
        compiler_params=pltpu.CompilerParams(vmem_limit_bytes=VMEM_LIMIT),
        cost_estimate=pl.CostEstimate(flops=30 * part_rows * LANES * 40, bytes_accessed=20 * part_rows * LANES, transcendentals=0),
    )(lr, norm, stay(g), stay(w), stay(m), v, mask, *before)


def store_kernel(spots, direct, *refs):
    count = len(spots)
    pieces = refs[:count]
    params, buf, in_sem, out_sem = refs[-4:]
    me, part, along_x, along_y = places()
    diag = along_x + along_y - me
    shift = part - me
    blocks = (me, along_x, along_y, diag, me + shift, along_x + shift, along_y + shift, diag + shift)
    loads, stores = [], []
    for k, (which, start, size, grains) in enumerate(spots):
        dst = params.at[pl.ds(blocks[which] * grains + start, size)]
        src = pieces[k].at[pl.ds(0, size)]
        if not direct:
            loads.append(pltpu.make_async_copy(src, buf.at[k, pl.ds(0, size)], in_sem.at[k]))
            src = buf.at[k, pl.ds(0, size)]
        stores.append(pltpu.make_async_copy(src, dst, out_sem.at[k]))
    for cp in loads:
        cp.start()
    for k, out in enumerate(stores):
        if not direct:
            loads[k].wait()
        out.start()
    for out in stores:
        out.wait()


def store(pieces, spots, before, num_dev, grains, direct):
    count = len(pieces)
    if direct:
        pieces = [stay(p) for p in pieces]
    hbm = pl.BlockSpec(memory_space=pltpu.HBM)
    room = max(p.shape[0] for p in pieces)
    moved = sum(p.size for p in pieces)
    return pl.pallas_call(
        functools.partial(store_kernel, [(which, start, min(p.shape[0], grains - start), grains)
                                         for p, (which, start) in zip(pieces, spots)], direct),
        out_shape=jax.ShapeDtypeStruct((num_dev * grains, 4, LANES), jnp.bfloat16),
        in_specs=[pl.BlockSpec(memory_space=pltpu.VMEM) if direct else hbm] * count + [hbm] * len(before),
        out_specs=hbm,
        input_output_aliases={count: 0} if before else {},
        scratch_shapes=[pltpu.VMEM((1, 2, 4, LANES) if direct else (count, room, 4, LANES), jnp.bfloat16),
                        pltpu.SemaphoreType.DMA((count,)), pltpu.SemaphoreType.DMA((count,))],
        compiler_params=pltpu.CompilerParams(vmem_limit_bytes=VMEM_LIMIT),
        cost_estimate=pl.CostEstimate(flops=40 * moved, bytes_accessed=4 * moved, transcendentals=0),
    )(*pieces, *before)


def solution(mesh):
    num_dev = mesh.shape["dp"]
    hop = {"core": [(i, i ^ 1) for i in range(num_dev)], "x": [(i, i ^ 2) for i in range(num_dev)],
           "y": [(i, i ^ 4) for i in range(num_dev)]}

    def local_step(grad_row, master, mom_first, mom_second, decay_mask, learn_rate):
        shard_len = master.shape[0]
        rows = shard_len // LANES
        grains = rows // 4
        flat = lambda a: a.reshape(rows, LANES)

        def send(a, along):
            return lax.ppermute(a, "dp", hop[along])

        def put(pieces, spots, whole, direct=False):
            return (store(pieces, spots, whole, num_dev, grains, direct),)

        v, mask = flat(mom_second), flat(decay_mask)
        g, w, m, packed, norm = reduce_scatter(
            learn_rate, grad_row, flat(master), flat(mom_first), v, mask, num_dev)
        packs = {0: packed}
        state = ()
        whole = ()
        firsts = [sum(PARTS[:p]) for p in range(len(PARTS))]
        for p in (*range(1, len(PARTS)), 0):
            *state, packed, grad_norm = adamw(firsts[p], PARTS[p], learn_rate, norm, g, w, m, v, mask, state)
            packs.setdefault(p, packed)
        arrived = [(packs[p], send(packs[p], "x"), send(packs[p], "y"),
                    send(packs[p], "core")) for p in range(len(PARTS))]
        starts = [first * ADAM_ROWS // 4 for first in firsts]
        far = []
        for p, (packed, from_x, from_y, from_core) in enumerate(arrived):
            far.append(send(from_x, "y") if p % 2 == 0 else send(from_y, "x"))
            pieces = [packed, from_x, from_y, from_core, send(from_x, "core"), send(from_y, "core")]
            whole = put(pieces, [(k, starts[p]) for k in (0, 1, 2, 4, 5, 6)], whole)
        for p in range(0, len(PARTS), 2):
            pieces, spots = [], []
            for q in (p, p + 1):
                pieces += [far[q], send(far[q], "core")]
                spots += [(3, starts[q]), (7, starts[q])]
            whole = put(pieces, spots, whole, p + 2 == len(PARTS))
        new_w, new_m, new_v = state
        params = whole[0].reshape(num_dev * shard_len)
        return (params, new_w.reshape(shard_len), new_m.reshape(shard_len), new_v.reshape(shard_len),
                grad_norm)

    return jax.shard_map(
        local_step, mesh=mesh,
        in_specs=(P("dp", None), P("dp"), P("dp"), P("dp"), P("dp"), P()),
        out_specs=(P(), P("dp"), P("dp"), P("dp"), P()), check_vma=False)
```
